8 devices in a mesh: dp: 1 (over z), tp: 8 (over y, x, core).
Axes of the slice: x: 2, y: 2, z: 1, core: 2. Of those that a mesh axis runs over, the one named last changes fastest.
Arguments:
- x_steps: bfloat16 [32, 64, 2048], P(None, 'dp')
- cur_len: int32 [64], P('dp')
- k_cache: bfloat16 [2, 64, 128, 16, 128], P(None, 'dp', None, 'tp')
- v_cache: bfloat16 [2, 64, 128, 16, 128], P(None, 'dp', None, 'tp')
- ln_gain: bfloat16 [2, 2048], replicated
- ln_bias: bfloat16 [2, 2048], replicated
- w_q: bfloat16 [2, 2048, 2048], P(None, None, 'tp')
- w_k: bfloat16 [2, 2048, 2048], P(None, None, 'tp')
- w_v: bfloat16 [2, 2048, 2048], P(None, None, 'tp')
- w_o: bfloat16 [2, 2048, 2048], P(None, 'tp')
- w_in: bfloat16 [2, 2048, 8192], P(None, None, 'tp')
- b_in: bfloat16 [2, 8192], P(None, 'tp')
- w_out: bfloat16 [2, 8192, 2048], P(None, 'tp')
- b_out: bfloat16 [2, 2048], replicated
Outputs:
- output 1: bfloat16 [32, 64, 2048], P(None, 'dp')
- output 2: bfloat16 [2, 64, 128, 16, 128], P(None, 'dp', None, 'tp')
- output 3: bfloat16 [2, 64, 128, 16, 128], P(None, 'dp', None, 'tp')
All inputs are finite; a program needn't handle non-finite values.
Results may differ from the reference program's by a relative error of at most 0.0160624.
Values are sent between devices in bfloat16 or wider.
A program may use at most 1 GiB of HBM per device.

```python
import jax
import jax.numpy as jnp
from jax import lax

D_MODEL = 2048
N_HEADS = 16
HEAD_DIM = 128
ROT_DIM = 64
FF_DIM = 8192
BATCH_PART = 64
CACHE_LEN = 128
N_STEPS = 32
N_LAYERS = 2
LN_EPS = 1e-5
QUERY_GAIN = 2.5


def setup_inputs(seed: int = 0, part: int = 0) -> dict:
    base_key = jax.random.key(seed)
    shared_keys = jax.random.split(base_key, 10)
    part_keys = jax.random.split(jax.random.fold_in(base_key, part), 6)
    scale_model = D_MODEL ** -0.5
    scale_ff = FF_DIM ** -0.5
    cache_shape = (N_LAYERS, BATCH_PART, CACHE_LEN, N_HEADS, HEAD_DIM)

    def gaussian(key, shape, scale):
        return jax.random.normal(key, shape, jnp.float32) * scale

    top_len = CACHE_LEN - N_STEPS
    raw_span = jax.random.randint(part_keys[1], (BATCH_PART,), 0, top_len)
    shift_bits = jax.random.randint(part_keys[2], (BATCH_PART,), 0, 8)
    full_row = jax.random.randint(part_keys[3], (), 0, BATCH_PART)
    cur_len = 1 + jnp.right_shift(raw_span, shift_bits)
    cur_len = jnp.where(jnp.arange(BATCH_PART) == full_row, top_len, cur_len).astype(jnp.int32)
    return {
        "x_steps": gaussian(part_keys[0], (N_STEPS, BATCH_PART, D_MODEL), 1.0).astype(jnp.bfloat16),
        "cur_len": cur_len,
        "k_cache": gaussian(part_keys[4], cache_shape, 1.0).astype(jnp.bfloat16),
        "v_cache": gaussian(part_keys[5], cache_shape, 1.0).astype(jnp.bfloat16),
        "ln_gain": (1.0 + gaussian(shared_keys[0], (N_LAYERS, D_MODEL), 0.2)).astype(jnp.bfloat16),
        "ln_bias": gaussian(shared_keys[1], (N_LAYERS, D_MODEL), 0.2).astype(jnp.bfloat16),
        "w_q": gaussian(shared_keys[2], (N_LAYERS, D_MODEL, D_MODEL), QUERY_GAIN * scale_model).astype(jnp.bfloat16),
        "w_k": gaussian(shared_keys[3], (N_LAYERS, D_MODEL, D_MODEL), scale_model).astype(jnp.bfloat16),
        "w_v": gaussian(shared_keys[4], (N_LAYERS, D_MODEL, D_MODEL), scale_model).astype(jnp.bfloat16),
        "w_o": gaussian(shared_keys[5], (N_LAYERS, D_MODEL, D_MODEL), scale_model).astype(jnp.bfloat16),
        "w_in": gaussian(shared_keys[6], (N_LAYERS, D_MODEL, FF_DIM), scale_model).astype(jnp.bfloat16),
        "b_in": gaussian(shared_keys[7], (N_LAYERS, FF_DIM), 0.5).astype(jnp.bfloat16),
        "w_out": gaussian(shared_keys[8], (N_LAYERS, FF_DIM, D_MODEL), scale_ff).astype(jnp.bfloat16),
        "b_out": gaussian(shared_keys[9], (N_LAYERS, D_MODEL), 0.3).astype(jnp.bfloat16),
    }


def layer_norm(hidden, gain, bias):
    hid_f32 = hidden.astype(jnp.float32)
    row_mean = jnp.mean(hid_f32, axis=-1, keepdims=True)
    centered = hid_f32 - row_mean
    row_var = jnp.mean(centered * centered, axis=-1, keepdims=True)
    normed = centered / jnp.sqrt(row_var + LN_EPS)
    return (normed * gain.astype(jnp.float32) + bias.astype(jnp.float32)).astype(jnp.bfloat16)


def rotary_tables(positions):
    inv_freq = 1.0 / (10000.0 ** (jnp.arange(0, ROT_DIM, 2).astype(jnp.float32) / ROT_DIM))
    angles = positions.astype(jnp.float32)[:, None] * inv_freq[None, :]
    return jnp.cos(angles)[:, None, :], jnp.sin(angles)[:, None, :]


def apply_rotary(vectors, cos_tab, sin_tab):
    lead_shape = vectors.shape[:-1]
    pairs = vectors[..., :ROT_DIM].reshape(lead_shape + (ROT_DIM // 2, 2))
    even_part = pairs[..., 0]
    odd_part = pairs[..., 1]
    rotated = jnp.stack([even_part * cos_tab - odd_part * sin_tab, odd_part * cos_tab + even_part * sin_tab], axis=-1)
    return jnp.concatenate([rotated.reshape(lead_shape + (ROT_DIM,)), vectors[..., ROT_DIM:]], axis=-1)


def decoder_layer(hidden, new_pos, layer):
    (k_layer, v_layer, gain, bias, q_weight, k_weight, v_weight, o_weight,
     in_weight, in_bias, out_weight, out_bias) = layer
    batch = hidden.shape[0]
    head_shape = (batch, N_HEADS, HEAD_DIM)
    normed = layer_norm(hidden, gain, bias)
    query = jnp.dot(normed, q_weight, preferred_element_type=jnp.float32).reshape(head_shape)
    key_new = jnp.dot(normed, k_weight, preferred_element_type=jnp.float32).reshape(head_shape)
    value_new = jnp.dot(normed, v_weight, preferred_element_type=jnp.float32).reshape(head_shape).astype(jnp.bfloat16)
    cos_tab, sin_tab = rotary_tables(new_pos)
    query = apply_rotary(query, cos_tab, sin_tab).astype(jnp.bfloat16)
    key_new = apply_rotary(key_new, cos_tab, sin_tab).astype(jnp.bfloat16)
    slot_ids = jnp.arange(CACHE_LEN)
    written = (slot_ids[None, :] == new_pos[:, None])[:, :, None, None]
    k_layer = jnp.where(written, key_new[:, None], k_layer)
    v_layer = jnp.where(written, value_new[:, None], v_layer)
    scores = jnp.einsum("bhe,bshe->bhs", query.astype(jnp.float32), k_layer.astype(jnp.float32)) * (HEAD_DIM ** -0.5)
    visible = (slot_ids[None, :] <= new_pos[:, None])[:, None, :]
    scores = jnp.where(visible, scores, -jnp.inf)
    exp_scores = jnp.exp(scores - jnp.max(scores, axis=-1, keepdims=True))
    attn_probs = (exp_scores / jnp.sum(exp_scores, axis=-1, keepdims=True)).astype(jnp.bfloat16)
    context = jnp.einsum("bhs,bshe->bhe", attn_probs.astype(jnp.float32), v_layer.astype(jnp.float32))
    context = context.astype(jnp.bfloat16).reshape(batch, N_HEADS * HEAD_DIM)
    attn_out = jnp.dot(context, o_weight, preferred_element_type=jnp.float32)
    pre_act = jnp.dot(normed, in_weight, preferred_element_type=jnp.float32) + in_bias.astype(jnp.float32)
    gelu_act = jax.nn.gelu(pre_act, approximate=True).astype(jnp.bfloat16)
    mlp_out = jnp.dot(gelu_act, out_weight, preferred_element_type=jnp.float32)
    new_hidden = (hidden.astype(jnp.float32) + attn_out + mlp_out + out_bias.astype(jnp.float32)).astype(jnp.bfloat16)
    return new_hidden, (k_layer, v_layer)


def reference(x_steps, cur_len, k_cache, v_cache, ln_gain, ln_bias, w_q, w_k, w_v, w_o, w_in, b_in, w_out, b_out):
    def one_step(caches, step_in):
        x_now, step_idx = step_in
        new_pos = cur_len + step_idx

        def layer_step(hidden, layer):
            return decoder_layer(hidden, new_pos, layer)

        layers = (caches[0], caches[1], ln_gain, ln_bias, w_q, w_k, w_v, w_o, w_in, b_in, w_out, b_out)
        last_hidden, new_caches = lax.scan(layer_step, x_now, layers)
        return new_caches, last_hidden

    final_caches, hidden_out = lax.scan(one_step, (k_cache, v_cache), (x_steps, jnp.arange(N_STEPS, dtype=jnp.int32)))
    return hidden_out, final_caches[0], final_caches[1]
```

```python
import jax
import jax.numpy as jnp
from jax import lax
from jax.sharding import PartitionSpec as P

ROT_DIM = 64
LN_EPS = 1e-5
CHUNKS = 2


def layer_norm(hidden, gain, bias):
    hid_f32 = hidden.astype(jnp.float32)
    row_mean = jnp.mean(hid_f32, axis=-1, keepdims=True)
    centered = hid_f32 - row_mean
    row_var = jnp.mean(centered * centered, axis=-1, keepdims=True)
    normed = centered * lax.rsqrt(row_var + LN_EPS)
    return (normed * gain.astype(jnp.float32) + bias.astype(jnp.float32)).astype(jnp.bfloat16)


def rotary_tables(positions):
    lane = jnp.arange(128)
    inv_freq = 1.0 / (10000.0 ** ((lane // 2 * 2).astype(jnp.float32) / ROT_DIM))
    angles = positions.astype(jnp.float32)[..., None] * inv_freq
    inside = lane < ROT_DIM
    cos_tab = jnp.where(inside, jnp.cos(angles), 1.0)
    sin_tab = jnp.where(inside, jnp.where(lane % 2 == 0, -jnp.sin(angles), jnp.sin(angles)), 0.0)
    return cos_tab, sin_tab


def apply_rotary(vectors, cos_tab, sin_tab):
    even_lane = jnp.arange(vectors.shape[-1]) % 2 == 0
    swapped = jnp.where(even_lane, jnp.roll(vectors, -1, axis=-1), jnp.roll(vectors, 1, axis=-1))
    return vectors * cos_tab + swapped * sin_tab


def chunk_layer(hidden, rotary, slot_of, visible, k_cache, v_cache, weights):
    cos_tab, sin_tab = rotary
    gain, bias, q_weight, k_weight, v_weight, o_weight, in_weight, in_bias, out_weight = weights
    steps, n_seq, d_model = hidden.shape
    n_heads, head_dim = k_cache.shape[2:]
    normed = layer_norm(hidden, gain, bias).reshape(steps * n_seq, d_model)
    head_shape = (steps, n_seq, n_heads, head_dim)
    query = jnp.dot(normed, q_weight, preferred_element_type=jnp.float32).reshape(head_shape)
    key_new = jnp.dot(normed, k_weight, preferred_element_type=jnp.float32).reshape(head_shape)
    value_new = jnp.dot(normed, v_weight, preferred_element_type=jnp.float32).astype(jnp.bfloat16).reshape(head_shape)
    query = apply_rotary(query, cos_tab, sin_tab).astype(jnp.bfloat16)
    key_new = apply_rotary(key_new, cos_tab, sin_tab).astype(jnp.bfloat16)
    rows = jnp.arange(n_seq)[None, :]
    k_cache = k_cache.at[rows, slot_of].set(key_new)
    v_cache = v_cache.at[rows, slot_of].set(value_new)
    scores = jnp.einsum("tbhe,bshe->bhts", query, k_cache, preferred_element_type=jnp.float32) * (head_dim ** -0.5)
    scores = jnp.where(visible, scores, -jnp.inf)
    exp_scores = jnp.exp(scores - jnp.max(scores, axis=-1, keepdims=True))
    probs = (exp_scores / jnp.sum(exp_scores, axis=-1, keepdims=True)).astype(jnp.bfloat16)
    context = jnp.einsum("bhts,bshe->tbhe", probs, v_cache, preferred_element_type=jnp.float32).astype(jnp.bfloat16)
    context = context.reshape(steps * n_seq, n_heads * head_dim)
    pre_act = jnp.dot(normed, in_weight, preferred_element_type=jnp.float32) + in_bias.astype(jnp.float32)
    gelu_act = jax.nn.gelu(pre_act, approximate=True).astype(jnp.bfloat16)
    part = jnp.dot(context, o_weight, preferred_element_type=jnp.float32) + jnp.dot(gelu_act, out_weight, preferred_element_type=jnp.float32)
    return part.reshape(hidden.shape), k_cache, v_cache


def decode_shard(x_steps, cur_len, k_cache, v_cache, ln_gain, ln_bias, w_q, w_k, w_v, w_o, w_in, b_in, w_out, b_out):
    n_layers, batch, cache_len = k_cache.shape[:3]
    steps = x_steps.shape[0]
    size = batch // CHUNKS
    hiddens, k_parts, v_parts = [], [], []
    for chunk in range(CHUNKS):
        part = slice(chunk * size, (chunk + 1) * size)
        lens = cur_len[part]
        slot_of = lens[None, :] + jnp.arange(steps)[:, None]
        cos_tab, sin_tab = rotary_tables(slot_of)
        rotary = (cos_tab[:, :, None, :], sin_tab[:, :, None, :])
        visible = (jnp.arange(cache_len)[None, None, :] <= slot_of.T[:, :, None])[:, None]
        hidden = x_steps[:, part]
        ks, vs = [], []
        for layer in range(n_layers):
            weights = (ln_gain[layer], ln_bias[layer], w_q[layer], w_k[layer], w_v[layer], w_o[layer], w_in[layer], b_in[layer], w_out[layer])
            update, k_new, v_new = chunk_layer(hidden, rotary, slot_of, visible, k_cache[layer, part], v_cache[layer, part], weights)
            total = lax.psum(update.astype(jnp.bfloat16), "tp")
            hidden = (hidden.astype(jnp.float32) + total.astype(jnp.float32) + b_out[layer].astype(jnp.float32)).astype(jnp.bfloat16)
            ks.append(k_new)
            vs.append(v_new)
        hiddens.append(hidden)
        k_parts.append(jnp.stack(ks))
        v_parts.append(jnp.stack(vs))
    return jnp.concatenate(hiddens, axis=1), jnp.concatenate(k_parts, axis=1), jnp.concatenate(v_parts, axis=1)


def solution(mesh):
    cache_spec = P(None, "dp", None, "tp", None)
    in_specs = (P(None, "dp", None), P("dp"), cache_spec, cache_spec, P(None, None), P(None, None),
                P(None, None, "tp"), P(None, None, "tp"), P(None, None, "tp"), P(None, "tp", None),
                P(None, None, "tp"), P(None, "tp"), P(None, "tp", None), P(None, None))
    out_specs = (P(None, "dp", None), cache_spec, cache_spec)
    return jax.shard_map(decode_shard, mesh=mesh, in_specs=in_specs, out_specs=out_specs, check_vma=False)
```

```python
import functools

import jax
import jax.numpy as jnp
from jax import lax
from jax.experimental import pallas as pl
from jax.experimental.pallas import tpu as pltpu
from jax.sharding import PartitionSpec as P

ROT_DIM = 64
LN_EPS = 1e-5
MESH = pl.DeviceIdType.MESH
F32 = jnp.float32
BF16 = jnp.bfloat16
SEQS = 8
OLD = 96


def decode_kernel(n_chunks, n_stages, x_hbm, k_hbm, v_hbm, wq_hbm, wk_hbm, wv_hbm, wo_hbm, win_hbm, wout_hbm,
                  cos_c, sin_c, cos_t, sin_t, old_mask, gain, bias, b_in, b_out,
                  out_hbm, rec_k, rec_v,
                  wq, wk, wv, wo, win, wout, hid, part, recv0, sum0, recv1, sum1, recv2,
                  normed, qf, kf, vf, cf, ctx, act, inter, scores, kbuf, vbuf,
                  w_sem, x_sem, kv_sem, rec_sem, out_sem, send_sem, recv_sem):
    steps = x_hbm.shape[0]
    rows = steps * SEQS
    half, quarter, eighth = steps // 2, steps // 4, steps // 8
    d_model = x_hbm.shape[2]
    me = lax.axis_index("tp")
    core = lax.rem(me, 2)
    px = lax.rem(lax.div(me, 2), 2)
    py = lax.div(me, 4)
    partner = me + 1 - 2 * core
    x_peer = me + 2 * (1 - 2 * px)
    y_peer = me + 4 * (1 - 2 * py)
    first = (1 - core) * x_peer + core * y_peer
    second = (1 - core) * y_peer + core * x_peer
    pos1 = (1 - core) * px + core * py
    pos2 = (1 - core) * py + core * px
    base0 = half * core
    base1 = base0 + quarter * pos1
    base2 = base1 + eighth * pos2

    weight_pairs = ((wq_hbm, wq), (wk_hbm, wk), (wv_hbm, wv), (win_hbm, win), (wo_hbm, wo), (wout_hbm, wout))

    def weight_copy(layer, j):
        src, dst = weight_pairs[j]
        return pltpu.make_async_copy(src.at[layer], dst.at[layer], w_sem.at[layer, j])

    def x_copy(chunk):
        return pltpu.make_async_copy(x_hbm.at[:, pl.ds(pl.multiple_of(chunk * SEQS, SEQS), SEQS), :], hid.at[chunk], x_sem.at[chunk])

    def out_copy(chunk):
        return pltpu.make_async_copy(hid.at[chunk], out_hbm.at[:, pl.ds(pl.multiple_of(chunk * SEQS, SEQS), SEQS), :], out_sem.at[chunk])

    def kv_copies(stage):
        layer, chunk, slot = lax.div(stage, n_chunks), lax.rem(stage, n_chunks), lax.rem(stage, 2)
        seqs = pl.ds(chunk * SEQS, SEQS)
        return (pltpu.make_async_copy(k_hbm.at[layer, seqs], kbuf.at[slot], kv_sem.at[0, slot]),
                pltpu.make_async_copy(v_hbm.at[layer, seqs], vbuf.at[slot], kv_sem.at[1, slot]))

    def rec_copies(stage):
        layer, chunk, slot = lax.div(stage, n_chunks), lax.rem(stage, n_chunks), lax.rem(stage, 2)
        seqs = pl.ds(chunk * SEQS, SEQS)
        new = pl.ds(2 * OLD, 2 * steps)
        return (pltpu.make_async_copy(kbuf.at[slot, :, new, :], rec_k.at[layer, seqs], rec_sem.at[0, slot]),
                pltpu.make_async_copy(vbuf.at[slot, :, new, :], rec_v.at[layer, seqs], rec_sem.at[1, slot]))

    def remote(phase, stage, src, dst, peer):
        slot = lax.rem(stage, 2)
        return pltpu.make_async_remote_copy(src_ref=src, dst_ref=dst, send_sem=send_sem.at[phase, slot], recv_sem=recv_sem.at[phase, lax.rem(stage, 4)],
                                            device_id={"tp": peer}, device_id_type=MESH)

    def phase0(stage):
        return remote(0, stage, part.at[pl.ds(half - base0, half)], recv0.at[lax.rem(stage, 2)], partner)

    def phase1(stage):
        return remote(1, stage, sum0.at[pl.ds(quarter * (1 - pos1), quarter)], recv1.at[lax.rem(stage, 2)], first)

    def phase2(stage):
        return remote(2, stage, sum1.at[pl.ds(eighth * (1 - pos2), eighth)], recv2.at[lax.rem(stage, 2)], second)

    def gather(phase, stage, start, size, peer):
        block = hid.at[lax.rem(stage, n_chunks), pl.ds(start, size)]
        return remote(phase, stage, block, block, peer)

    def phase3(stage):
        return gather(3, stage, base2, eighth, second)

    def phase4(stage):
        return gather(4, stage, base1, quarter, first)

    def phase5(stage):
        return gather(5, stage, base0, half, partner)

    barrier = pltpu.get_barrier_semaphore()
    for peer in (partner, x_peer, y_peer):
        pl.semaphore_signal(barrier, inc=1, device_id={"tp": peer}, device_id_type=MESH)
    x_copy(0).start()
    for j in range(3):
        weight_copy(0, j).start()
    for copy in kv_copies(0):
        copy.start()
    for j in range(3, 6):
        weight_copy(0, j).start()
    for chunk in range(1, n_chunks):
        x_copy(chunk).start()
    for j in range(6):
        weight_copy(1, j).start()
    pl.semaphore_wait(barrier, 3)

    def norm_and_project(stage, layer, chunk):
        @pl.when(layer == 0)
        def _():
            x_copy(chunk).wait()

        group = 8

        @pl.loop(0, steps // group)
        def _(g):
            x = hid[chunk, pl.ds(g * group, group)].astype(F32)
            mean = jnp.mean(x, axis=-1, keepdims=True)
            centered = x - mean
            var = jnp.mean(centered * centered, axis=-1, keepdims=True)
            y = centered * lax.rsqrt(var + LN_EPS) * gain[layer][None] + bias[layer][None]
            normed[pl.ds(pl.multiple_of(g * group * SEQS, group * SEQS), group * SEQS), :] = y.reshape(group * SEQS, d_model).astype(BF16)

        @pl.when(chunk == 0)
        def _():
            for j in range(3):
                weight_copy(layer, j).wait()

        here = pl.ds(pl.multiple_of(chunk * SEQS, SEQS), SEQS)
        cc, sc = cos_c[here, :][None], sin_c[here, :][None]
        ct, st = cos_t[...], sin_t[...]
        cos = (cc * ct - sc * st).reshape(rows, 128)
        sin = (sc * ct + cc * st).reshape(rows, 128)
        even = lax.rem(lax.broadcasted_iota(jnp.int32, (rows, 128), 1), 2) == 0

        for weight, dst, rotate in ((wq, qf, True), (wk, kf, True), (wv, vf, False)):
            vec = jnp.dot(normed[...], weight[layer], preferred_element_type=F32)
            for h in range(2):
                piece = vec[:, h * 128:(h + 1) * 128]
                if rotate:
                    swapped = jnp.where(even, pltpu.roll(piece, 127, 1), pltpu.roll(piece, 1, 1))
                    piece = piece * cos + swapped * sin
                dst[h] = piece

    def attend(stage, layer, chunk):
        slot = lax.rem(stage, 2)
        for copy in kv_copies(stage):
            copy.wait()
        shape = (2 * steps, 2 * (OLD + steps))
        row, col = lax.broadcasted_iota(jnp.int32, shape, 0), lax.broadcasted_iota(jnp.int32, shape, 1)
        col_slot, col_head = lax.shift_right_logical(col, 1), lax.bitwise_and(col, 1)
        row_head, row_step = lax.div(row, steps), lax.rem(row, steps)
        same = row_head == col_head
        fresh = jnp.where(col_slot - OLD <= row_step, 2.0, 0.0)
        kind = jnp.where(same, jnp.where(col_slot >= OLD, fresh, 1.0), 0.0)
        here = pl.ds(pl.multiple_of(chunk * SEQS, SEQS), SEQS)
        old = old_mask[here, :]
        for b in range(SEQS):
            mine = pl.ds(b, steps, stride=SEQS)
            for src, buf, j in ((kf, kbuf, 0), (vf, vbuf, 1)):
                for h in range(2):
                    inter[b, j, pl.ds(h, steps, stride=2), :] = src[h, mine, :]
                buf[slot, b, pl.ds(2 * OLD, 2 * steps), :] = inter[b, j].astype(BF16)
        for copy in rec_copies(stage):
            copy.start()
        for b in range(SEQS):
            mine = pl.ds(b, steps, stride=SEQS)
            query = jnp.concatenate([qf[0, mine, :], qf[1, mine, :]], axis=0).astype(BF16)
            s = lax.dot_general(query, kbuf[slot, b], (((1,), (1,)), ((), ())), preferred_element_type=F32) * (128 ** -0.5)
            scores[b] = jnp.where(kind + old[b:b + 1, :] > 1.5, s, -jnp.inf)
        for b in range(SEQS):
            s = scores[b]
            e = jnp.exp(s - jnp.max(s, axis=-1, keepdims=True))
            probs = (e * (1.0 / jnp.sum(e, axis=-1, keepdims=True))).astype(BF16)
            context = jnp.dot(probs, vbuf[slot, b], preferred_element_type=F32)
            for h in range(2):
                cf[h, pl.ds(b, steps, stride=SEQS), :] = context[h * steps:(h + 1) * steps]

    def feed_forward(layer, chunk):
        @pl.when(chunk == 0)
        def _():
            for j in range(3, 6):
                weight_copy(layer, j).wait()

        @pl.loop(0, act.shape[1] // 256)
        def _(n):
            cols = pl.ds(pl.multiple_of(n * 256, 256), 256)
            pre = jnp.dot(normed[...], win[layer, :, cols], preferred_element_type=F32) + b_in[layer, :, cols]
            act[:, cols] = jax.nn.gelu(pre, approximate=True).astype(BF16)

    def project_out(stage, layer):
        for h in range(2):
            ctx[:, h * 128:(h + 1) * 128] = cf[h].astype(BF16)

        @pl.loop(0, d_model // 256)
        def _(n):
            cols = pl.ds(pl.multiple_of(n * 256, 256), 256)
            total = jnp.dot(ctx[...], wo[layer, :, cols], preferred_element_type=F32)
            total += jnp.dot(act[...], wout[layer, :, cols], preferred_element_type=F32)
            part[:, :, cols] = total.reshape(steps, SEQS, 256).astype(BF16)

    @pl.loop(0, n_stages + 4)
    def _(i):
        layer, chunk = lax.div(i, n_chunks), lax.rem(i, n_chunks)
        live = i < n_stages

        @pl.when(jnp.logical_and(i >= 1, i <= n_stages))
        def _():
            s = i - 1
            phase0(s).wait()

            @pl.loop(0, half // 4)
            def _(g):
                ts = pl.ds(g * 4, 4)
                sum0[ts] = part[pl.ds(base0 + g * 4, 4)] + recv0[lax.rem(s, 2), ts]

            phase1(s).start()

        @pl.when(live)
        def _():
            norm_and_project(i, layer, chunk)

        @pl.when(jnp.logical_and(i >= 2, i <= n_stages + 1))
        def _():
            s = i - 2
            where = lax.rem(s, n_chunks)
            phase2(s).wait()
            own = pl.ds(base2, eighth)
            total = sum1[pl.ds(eighth * pos2, eighth)].astype(F32) + recv2[lax.rem(s, 2)].astype(F32)
            total = total + hid[where, own].astype(F32) + b_out[lax.div(s, n_chunks)][None]
            hid[where, own] = total.astype(BF16)
            phase3(s).start()

        @pl.when(jnp.logical_and(i >= 3, i <= n_stages + 2))
        def _():
            phase4(i - 3).wait()
            phase5(i - 3).start()

        @pl.when(i >= 4)
        def _():
            s = i - 4
            phase5(s).wait()

            @pl.when(s >= n_stages - n_chunks)
            def _():
                out_copy(lax.rem(s, n_chunks)).start()

        @pl.when(live)
        def _():
            @pl.when(i >= 1)
            def _():
                for copy in rec_copies(i - 1):
                    copy.wait()

            @pl.when(i + 1 < n_stages)
            def _():
                for copy in kv_copies(i + 1):
                    copy.start()

            attend(i, layer, chunk)

        @pl.when(jnp.logical_and(i >= 1, i <= n_stages))
        def _():
            s = i - 1
            phase1(s).wait()

            @pl.loop(0, quarter // 4)
            def _(g):
                ts = pl.ds(g * 4, 4)
                sum1[ts] = sum0[pl.ds(quarter * pos1 + g * 4, 4)] + recv1[lax.rem(s, 2), ts]

            phase2(s).start()

        @pl.when(live)
        def _():
            feed_forward(layer, chunk)

        @pl.when(jnp.logical_and(i >= 2, i <= n_stages + 1))
        def _():
            phase3(i - 2).wait()
            phase4(i - 2).start()

        @pl.when(live)
        def _():
            project_out(i, layer)
            phase0(i).start()

    for copy in rec_copies(n_stages - 1):
        copy.wait()
    for chunk in range(n_chunks):
        out_copy(chunk).wait()


def merge_kernel(n_blocks, lens, k_hbm, v_hbm, rec_k, rec_v, k_out, v_out, kbuf, vbuf, rk, rv, in_sem, out_sem):
    size = kbuf.shape[1]
    steps = rk.shape[2]

    def loads(i):
        slot, here = lax.rem(i, 2), pl.ds(i * size, size)
        return [pltpu.make_async_copy(src.at[here], dst.at[slot], in_sem.at[j, slot])
                for j, (src, dst) in enumerate(((k_hbm, kbuf), (v_hbm, vbuf), (rec_k, rk), (rec_v, rv)))]

    def stores(i):
        slot, here = lax.rem(i, 2), pl.ds(i * size, size)
        return [pltpu.make_async_copy(src.at[slot], dst.at[here], out_sem.at[j, slot])
                for j, (src, dst) in enumerate(((kbuf, k_out), (vbuf, v_out)))]

    for copy in loads(0):
        copy.start()

    @pl.loop(0, n_blocks)
    def _(i):
        slot = lax.rem(i, 2)

        @pl.when(i >= 1)
        def _():
            for copy in stores(i - 1):
                copy.wait()

        @pl.when(i + 1 < n_blocks)
        def _():
            for copy in loads(i + 1):
                copy.start()

        for copy in loads(i):
            copy.wait()
        for b in range(size):
            at = lens[lax.rem(i * size + b, lens.shape[0])]
            kbuf[slot, b, pl.ds(at, steps)] = rk[slot, b]
            vbuf[slot, b, pl.ds(at, steps)] = rv[slot, b]
        for copy in stores(i):
            copy.start()

    for copy in stores(n_blocks - 1):
        copy.wait()


def angle_tables(positions):
    lane = jnp.arange(128)
    inv_freq = jnp.where(lane < ROT_DIM, 1.0 / (10000.0 ** ((lane // 2 * 2).astype(F32) / ROT_DIM)), 0.0)
    angles = positions.astype(F32)[:, None] * inv_freq[None, :]
    return jnp.cos(angles), jnp.where(lane % 2 == 0, -jnp.sin(angles), jnp.sin(angles))


def decode_shard(x_steps, cur_len, k_cache, v_cache, ln_gain, ln_bias, w_q, w_k, w_v, w_o, w_in, b_in, w_out, b_out):
    n_layers, batch, cache_len, n_heads, head_dim = k_cache.shape
    steps, _, d_model = x_steps.shape
    ff = w_in.shape[2]
    n_chunks = batch // SEQS
    n_stages = n_layers * n_chunks
    rows = steps * SEQS
    flat = (n_layers, batch, cache_len * n_heads, head_dim)
    cos_c, sin_c = angle_tables(cur_len)
    cos_t, sin_t = (jnp.broadcast_to(tab[:, None, :], (steps, SEQS, 128)) for tab in angle_tables(jnp.arange(steps)))
    col_slot = jnp.arange(cache_len * n_heads) // n_heads
    old_mask = jnp.where((col_slot[None, :] < cur_len[:, None]) & (col_slot[None, :] < OLD), 1.0, 0.0).astype(F32)
    vecs = [v.astype(F32)[:, None, :] for v in (ln_gain, ln_bias, b_in, b_out)]
    any_spec, vmem = pl.BlockSpec(memory_space=pl.ANY), pl.BlockSpec(memory_space=pltpu.VMEM)
    dma = pltpu.SemaphoreType.DMA
    block = (steps, SEQS, d_model)
    hidden, rec_k, rec_v = pl.pallas_call(
        functools.partial(decode_kernel, n_chunks, n_stages),
        out_shape=(jax.ShapeDtypeStruct(x_steps.shape, BF16),
                   jax.ShapeDtypeStruct((n_layers, batch, steps * n_heads, head_dim), BF16),
                   jax.ShapeDtypeStruct((n_layers, batch, steps * n_heads, head_dim), BF16)),
        in_specs=[any_spec] * 9 + [vmem] * 9,
        out_specs=(any_spec,) * 3,
        scratch_shapes=[
            pltpu.VMEM(w_q.shape, BF16), pltpu.VMEM(w_k.shape, BF16), pltpu.VMEM(w_v.shape, BF16), pltpu.VMEM(w_o.shape, BF16),
            pltpu.VMEM(w_in.shape, BF16), pltpu.VMEM(w_out.shape, BF16),
            pltpu.VMEM((n_chunks,) + block, BF16), pltpu.VMEM(block, BF16),
            pltpu.VMEM((2, steps // 2, SEQS, d_model), BF16), pltpu.VMEM((steps // 2, SEQS, d_model), BF16),
            pltpu.VMEM((2, steps // 4, SEQS, d_model), BF16), pltpu.VMEM((steps // 4, SEQS, d_model), BF16),
            pltpu.VMEM((2, steps // 8, SEQS, d_model), BF16),
            pltpu.VMEM((rows, d_model), BF16),
            pltpu.VMEM((2, rows, 128), F32), pltpu.VMEM((2, rows, 128), F32), pltpu.VMEM((2, rows, 128), F32), pltpu.VMEM((2, rows, 128), F32),
            pltpu.VMEM((rows, 256), BF16), pltpu.VMEM((rows, ff), BF16),
            pltpu.VMEM((SEQS, 2, 2 * steps, 128), F32), pltpu.VMEM((SEQS, 2 * steps, 256), F32),
            pltpu.VMEM((2, SEQS, 256, 128), BF16), pltpu.VMEM((2, SEQS, 256, 128), BF16),
            dma((n_layers, 6)), dma((n_chunks,)), dma((2, 2)), dma((2, 2)), dma((n_chunks,)), dma((6, 2)), dma((6, 4)),
        ],
        compiler_params=pltpu.CompilerParams(collective_id=0, has_side_effects=True, vmem_limit_bytes=60 * 1024 * 1024),
        name="decode",
    )(x_steps, k_cache.reshape(flat), v_cache.reshape(flat), w_q, w_k, w_v, w_o, w_in, w_out,
      cos_c, sin_c, cos_t, sin_t, old_mask, *vecs)

    pairs = n_layers * batch
    size = 16
    lines = (pairs, cache_len, n_heads, head_dim)
    new = (pairs, steps, n_heads, head_dim)
    k_out, v_out = pl.pallas_call(
        functools.partial(merge_kernel, pairs // size),
        out_shape=(jax.ShapeDtypeStruct(lines, BF16),) * 2,
        in_specs=[pl.BlockSpec(memory_space=pltpu.SMEM)] + [any_spec] * 4,
        out_specs=(any_spec,) * 2,
        scratch_shapes=[pltpu.VMEM((2, size) + lines[1:], BF16), pltpu.VMEM((2, size) + lines[1:], BF16),
                        pltpu.VMEM((2, size) + new[1:], BF16), pltpu.VMEM((2, size) + new[1:], BF16), dma((4, 2)), dma((2, 2))],
        name="merge",
    )(cur_len, k_cache.reshape(lines), v_cache.reshape(lines), rec_k.reshape(new), rec_v.reshape(new))
    return hidden, k_out.reshape(k_cache.shape), v_out.reshape(v_cache.shape)


def solution(mesh):
    cache_spec = P(None, "dp", None, "tp", None)
    in_specs = (P(None, "dp", None), P("dp"), cache_spec, cache_spec, P(None, None), P(None, None),
                P(None, None, "tp"), P(None, None, "tp"), P(None, None, "tp"), P(None, "tp", None),
                P(None, None, "tp"), P(None, "tp"), P(None, "tp", None), P(None, None))
    out_specs = (P(None, "dp", None), cache_spec, cache_spec)
    return jax.shard_map(decode_shard, mesh=mesh, in_specs=in_specs, out_specs=out_specs, check_vma=False)
```

```python
import functools

import jax
import jax.numpy as jnp
import numpy as np
from jax import lax
from jax.experimental import pallas as pl
from jax.experimental.pallas import tpu as pltpu
from jax.sharding import PartitionSpec as P

ROT_DIM = 64
LN_EPS = 1e-5
MESH = pl.DeviceIdType.MESH
F32 = jnp.float32
BF16 = jnp.bfloat16
SEQS = 8
OLD = 96


def decode_kernel(n_chunks, n_stages, x_hbm, k_hbm, v_hbm, wq_hbm, wk_hbm, wv_hbm, wo_hbm, win_hbm, wout_hbm,
                  lens, inv_freq, cos_t, sin_t, gain_in, bias_in, b_in_in, b_out_in,
                  out_hbm, rec_k, rec_v,
                  wq, wk, wv, wo, win, wout, hid, part, recv0, sum0, recv1, sum1, recv2,
                  normed, qf, kf, vf, cf, ctx, act, inter, scores, kbuf, vbuf,
                  cos_c, sin_c, gain, bias, b_in, b_out,
                  w_sem, x_sem, kv_sem, rec_sem, out_sem, send_sem, recv_sem):
    steps = x_hbm.shape[0]
    rows = steps * SEQS
    half, quarter, eighth = steps // 2, steps // 4, steps // 8
    d_model = x_hbm.shape[2]
    me = lax.axis_index("tp")
    core = lax.rem(me, 2)
    px = lax.rem(lax.div(me, 2), 2)
    py = lax.div(me, 4)
    partner = me + 1 - 2 * core
    x_peer = me + 2 * (1 - 2 * px)
    y_peer = me + 4 * (1 - 2 * py)
    first = (1 - core) * x_peer + core * y_peer
    second = (1 - core) * y_peer + core * x_peer
    pos1 = (1 - core) * px + core * py
    pos2 = (1 - core) * py + core * px
    base0 = half * core
    base1 = base0 + quarter * pos1
    base2 = base1 + eighth * pos2

    weight_pairs = ((wq_hbm, wq), (wk_hbm, wk), (wv_hbm, wv), (win_hbm, win), (wo_hbm, wo), (wout_hbm, wout))

    def weight_copy(layer, j):
        src, dst = weight_pairs[j]
        return pltpu.make_async_copy(src.at[layer], dst.at[layer], w_sem.at[layer, j])

    def x_copy(chunk):
        return pltpu.make_async_copy(x_hbm.at[:, pl.ds(pl.multiple_of(chunk * SEQS, SEQS), SEQS), :], hid.at[chunk], x_sem.at[chunk])

    def out_copy(chunk):
        return pltpu.make_async_copy(hid.at[chunk], out_hbm.at[:, pl.ds(pl.multiple_of(chunk * SEQS, SEQS), SEQS), :], out_sem.at[chunk])

    def kv_copies(stage):
        layer, chunk, slot = lax.div(stage, n_chunks), lax.rem(stage, n_chunks), lax.rem(stage, 2)
        seqs = pl.ds(chunk * SEQS, SEQS)
        return (pltpu.make_async_copy(k_hbm.at[layer, seqs], kbuf.at[slot], kv_sem.at[0, slot]),
                pltpu.make_async_copy(v_hbm.at[layer, seqs], vbuf.at[slot], kv_sem.at[1, slot]))

    def rec_copies(stage):
        layer, chunk, slot = lax.div(stage, n_chunks), lax.rem(stage, n_chunks), lax.rem(stage, 2)
        seqs = pl.ds(chunk * SEQS, SEQS)
        new = pl.ds(2 * OLD, 2 * steps)
        return (pltpu.make_async_copy(kbuf.at[slot, :, new, :], rec_k.at[layer, seqs], rec_sem.at[0, slot]),
                pltpu.make_async_copy(vbuf.at[slot, :, new, :], rec_v.at[layer, seqs], rec_sem.at[1, slot]))

    def remote(phase, stage, src, dst, peer):
        slot = lax.rem(stage, 2)
        return pltpu.make_async_remote_copy(src_ref=src, dst_ref=dst, send_sem=send_sem.at[phase, slot], recv_sem=recv_sem.at[phase, lax.rem(stage, 4)],
                                            device_id={"tp": peer}, device_id_type=MESH)

    def phase0(stage):
        return remote(0, stage, part.at[pl.ds(half - base0, half)], recv0.at[lax.rem(stage, 2)], partner)

    def phase1(stage):
        return remote(1, stage, sum0.at[lax.rem(stage, 2), pl.ds(quarter * (1 - pos1), quarter)], recv1.at[lax.rem(stage, 4)], first)

    def phase2(stage):
        return remote(2, stage, sum1.at[pl.ds(eighth * (1 - pos2), eighth)], recv2.at[lax.rem(stage, 2)], second)

    def gather(phase, stage, start, size, peer):
        block = hid.at[lax.rem(stage, n_chunks), pl.ds(start, size)]
        return remote(phase, stage, block, block, peer)

    def phase3(stage):
        return gather(3, stage, base2, eighth, second)

    def phase4(stage):
        return gather(4, stage, base1, quarter, first)

    def phase5(stage):
        return gather(5, stage, base0, half, partner)

    barrier = pltpu.get_barrier_semaphore()
    for peer in (partner, x_peer, y_peer):
        pl.semaphore_signal(barrier, inc=1, device_id={"tp": peer}, device_id_type=MESH)
    x_copy(0).start()
    for j in range(3):
        weight_copy(0, j).start()
    for copy in kv_copies(0):
        copy.start()
    for j in range(3, 6):
        weight_copy(0, j).start()
    for chunk in range(1, n_chunks):
        x_copy(chunk).start()
    for j in range(6):
        weight_copy(1, j).start()
    angles = lens[:, 0:128].astype(F32) * inv_freq[...]
    odd = lax.rem(lax.broadcasted_iota(jnp.int32, angles.shape, 1), 2) == 1
    cos_c[...] = jnp.cos(angles)
    sin_c[...] = jnp.where(odd, jnp.sin(angles), -jnp.sin(angles))
    for src, dst in ((gain_in, gain), (bias_in, bias), (b_in_in, b_in), (b_out_in, b_out)):
        for layer in range(src.shape[0]):
            dst[layer] = src[layer:layer + 1, :].astype(F32)
    pl.semaphore_wait(barrier, 3)

    def norm_and_project(stage, layer, chunk):
        @pl.when(layer == 0)
        def _():
            x_copy(chunk).wait()

        group = 8

        @pl.loop(0, steps // group)
        def _(g):
            x = hid[chunk, pl.ds(g * group, group)].astype(F32)
            mean = jnp.mean(x, axis=-1, keepdims=True)
            centered = x - mean
            var = jnp.mean(centered * centered, axis=-1, keepdims=True)
            y = centered * lax.rsqrt(var + LN_EPS) * gain[layer][None] + bias[layer][None]
            normed[pl.ds(pl.multiple_of(g * group * SEQS, group * SEQS), group * SEQS), :] = y.reshape(group * SEQS, d_model).astype(BF16)

        @pl.when(chunk == 0)
        def _():
            for j in range(3):
                weight_copy(layer, j).wait()

        here = pl.ds(pl.multiple_of(chunk * SEQS, SEQS), SEQS)
        cc, sc = cos_c[here, :][None], sin_c[here, :][None]
        ct, st = cos_t[...], sin_t[...]
        cos = (cc * ct - sc * st).reshape(rows, 128)
        sin = (sc * ct + cc * st).reshape(rows, 128)
        even = lax.rem(lax.broadcasted_iota(jnp.int32, (rows, 128), 1), 2) == 0

        for weight, dst, rotate in ((wq, qf, True), (wk, kf, True), (wv, vf, False)):
            vec = jnp.dot(normed[...], weight[layer], preferred_element_type=F32)
            for h in range(2):
                piece = vec[:, h * 128:(h + 1) * 128]
                if rotate:
                    swapped = jnp.where(even, pltpu.roll(piece, 127, 1), pltpu.roll(piece, 1, 1))
                    piece = piece * cos + swapped * sin
                dst[h] = piece

    def attend(stage, layer, chunk):
        slot = lax.rem(stage, 2)
        for copy in kv_copies(stage):
            copy.wait()
        shape = (2 * steps, 2 * (OLD + steps))
        row, col = lax.broadcasted_iota(jnp.int32, shape, 0), lax.broadcasted_iota(jnp.int32, shape, 1)
        col_slot, col_head = lax.shift_right_logical(col, 1), lax.bitwise_and(col, 1)
        row_head, row_step = lax.div(row, steps), lax.rem(row, steps)
        never = 1 << 20
        fresh = jnp.where(col_slot - OLD <= row_step, -1, never)
        key = jnp.where(row_head == col_head, jnp.where(col_slot >= OLD, fresh, col_slot), never)
        here = pl.ds(pl.multiple_of(chunk * SEQS, SEQS), SEQS)
        limit = lens[here, :]
        for b in range(SEQS):
            mine = pl.ds(b, steps, stride=SEQS)
            for src, buf, j in ((kf, kbuf, 0), (vf, vbuf, 1)):
                for h in range(2):
                    inter[b, j, pl.ds(h, steps, stride=2), :] = src[h, mine, :]
                buf[slot, b, pl.ds(2 * OLD, 2 * steps), :] = inter[b, j].astype(BF16)
        for copy in rec_copies(stage):
            copy.start()
        for b in range(SEQS):
            mine = pl.ds(b, steps, stride=SEQS)
            query = jnp.concatenate([qf[0, mine, :], qf[1, mine, :]], axis=0).astype(BF16)
            s = lax.dot_general(query, kbuf[slot, b], (((1,), (1,)), ((), ())), preferred_element_type=F32) * (128 ** -0.5)
            scores[b] = jnp.where(key < limit[b:b + 1, :], s, -jnp.inf)
        for b in range(SEQS):
            s = scores[b]
            e = jnp.exp(s - jnp.max(s, axis=-1, keepdims=True))
            probs = (e * (1.0 / jnp.sum(e, axis=-1, keepdims=True))).astype(BF16)
            context = jnp.dot(probs, vbuf[slot, b], preferred_element_type=F32)
            for h in range(2):
                cf[h, pl.ds(b, steps, stride=SEQS), :] = context[h * steps:(h + 1) * steps]

    def feed_forward(layer, chunk):
        @pl.when(chunk == 0)
        def _():
            for j in range(3, 6):
                weight_copy(layer, j).wait()

        @pl.loop(0, act.shape[1] // 256)
        def _(n):
            cols = pl.ds(pl.multiple_of(n * 256, 256), 256)
            pre = jnp.dot(normed[...], win[layer, :, cols], preferred_element_type=F32) + b_in[layer, :, cols]
            act[:, cols] = jax.nn.gelu(pre, approximate=True).astype(BF16)

    def project_out(stage, layer):
        for h in range(2):
            ctx[:, h * 128:(h + 1) * 128] = cf[h].astype(BF16)

        @pl.loop(0, d_model // 256)
        def _(n):
            cols = pl.ds(pl.multiple_of(n * 256, 256), 256)
            total = jnp.dot(ctx[...], wo[layer, :, cols], preferred_element_type=F32)
            total += jnp.dot(act[...], wout[layer, :, cols], preferred_element_type=F32)
            part[:, :, cols] = total.reshape(steps, SEQS, 256).astype(BF16)

    def between(i, lag):
        return jnp.logical_and(i >= lag, i < n_stages + lag)

    @pl.loop(0, n_stages + 5)
    def _(i):
        layer, chunk = lax.div(i, n_chunks), lax.rem(i, n_chunks)
        live = i < n_stages

        @pl.when(live)
        def _():
            norm_and_project(i, layer, chunk)

            @pl.when(i >= 1)
            def _():
                for copy in rec_copies(i - 1):
                    copy.wait()

            @pl.when(i + 1 < n_stages)
            def _():
                for copy in kv_copies(i + 1):
                    copy.start()

            attend(i, layer, chunk)

        @pl.when(between(i, 1))
        def _():
            s = i - 1
            phase0(s).wait()

            @pl.loop(0, half // 4)
            def _(g):
                ts = pl.ds(g * 4, 4)
                sum0[lax.rem(s, 2), ts] = part[pl.ds(base0 + g * 4, 4)] + recv0[lax.rem(s, 2), ts]

            phase1(s).start()

        @pl.when(between(i, 3))
        def _():
            phase3(i - 3).wait()
            phase4(i - 3).start()

        @pl.when(between(i, 2))
        def _():
            s = i - 2
            phase1(s).wait()

            @pl.loop(0, quarter // 4)
            def _(g):
                ts = pl.ds(g * 4, 4)
                sum1[ts] = sum0[lax.rem(s, 2), pl.ds(quarter * pos1 + g * 4, 4)] + recv1[lax.rem(s, 4), ts]

            phase2(s).start()

        @pl.when(between(i, 4))
        def _():
            phase4(i - 4).wait()
            phase5(i - 4).start()

        @pl.when(live)
        def _():
            feed_forward(layer, chunk)
            project_out(i, layer)
            phase0(i).start()

        @pl.when(between(i, 2))
        def _():
            s = i - 2
            where = lax.rem(s, n_chunks)
            phase2(s).wait()
            own = pl.ds(base2, eighth)
            total = sum1[pl.ds(eighth * pos2, eighth)].astype(F32) + recv2[lax.rem(s, 2)].astype(F32)
            total = total + hid[where, own].astype(F32) + b_out[lax.div(s, n_chunks)][None]
            hid[where, own] = total.astype(BF16)
            phase3(s).start()

        @pl.when(between(i, 4))
        def _():
            s = i - 4
            phase5(s).wait()

            @pl.when(s >= n_stages - n_chunks)
            def _():
                out_copy(lax.rem(s, n_chunks)).start()

    for copy in rec_copies(n_stages - 1):
        copy.wait()
    for chunk in range(n_chunks):
        out_copy(chunk).wait()


def merge_kernel(n_blocks, lens, hid_in, k_hbm, v_hbm, rec_k, rec_v, hid_out, k_out, v_out, hbuf, kbuf, vbuf, rk, rv, in_sem, out_sem):
    depth, size = kbuf.shape[:2]
    steps = rk.shape[2]
    ahead = depth // 2

    def loads(i):
        slot = lax.rem(i, depth)
        pairs = ((hid_in, hbuf), (k_hbm, kbuf), (v_hbm, vbuf), (rec_k, rk), (rec_v, rv))
        return [pltpu.make_async_copy(src.at[pl.ds(i * dst.shape[1], dst.shape[1])], dst.at[slot], in_sem.at[j, slot]) for j, (src, dst) in enumerate(pairs)]

    def stores(i):
        slot = lax.rem(i, depth)
        pairs = ((hbuf, hid_out), (kbuf, k_out), (vbuf, v_out))
        return [pltpu.make_async_copy(src.at[slot], dst.at[pl.ds(i * src.shape[1], src.shape[1])], out_sem.at[j, slot]) for j, (src, dst) in enumerate(pairs)]

    for i in range(ahead):
        for copy in loads(i):
            copy.start()

    @pl.loop(0, n_blocks)
    def _(i):
        slot = lax.rem(i, depth)

        @pl.when(i >= depth - ahead)
        def _():
            for copy in stores(i - (depth - ahead)):
                copy.wait()

        @pl.when(i + ahead < n_blocks)
        def _():
            for copy in loads(i + ahead):
                copy.start()

        for copy in loads(i):
            copy.wait()
        for b in range(size):
            at = lens[lax.rem(i * size + b, lens.shape[0])]
            kbuf[slot, b, pl.ds(at, steps)] = rk[slot, b]
            vbuf[slot, b, pl.ds(at, steps)] = rv[slot, b]
        for copy in stores(i):
            copy.start()

    for i in range(n_blocks - (depth - ahead), n_blocks):
        for copy in stores(i):
            copy.wait()


def inverse_frequencies():
    lane = np.arange(128)
    return np.where(lane < ROT_DIM, 1.0 / (10000.0 ** ((lane // 2 * 2) / ROT_DIM)), 0.0)


def decode_shard(x_steps, cur_len, k_cache, v_cache, ln_gain, ln_bias, w_q, w_k, w_v, w_o, w_in, b_in, w_out, b_out):
    n_layers, batch, cache_len, n_heads, head_dim = k_cache.shape
    steps, _, d_model = x_steps.shape
    ff = w_in.shape[2]
    n_chunks = batch // SEQS
    n_stages = n_layers * n_chunks
    rows = steps * SEQS
    flat = (n_layers, batch, cache_len * n_heads, head_dim)
    step_angles = np.arange(steps)[:, None] * inverse_frequencies()[None, :]
    signed = np.where(np.arange(128) % 2 == 0, -1.0, 1.0)
    cos_t, sin_t = (np.repeat(tab.astype(np.float32)[:, None, :], SEQS, axis=1) for tab in (np.cos(step_angles), np.sin(step_angles) * signed))
    inv_freq = np.broadcast_to(inverse_frequencies().astype(np.float32), (batch, 128))
    lens = jnp.broadcast_to(cur_len[:, None], (batch, cache_len * n_heads))
    any_spec, vmem = pl.BlockSpec(memory_space=pl.ANY), pl.BlockSpec(memory_space=pltpu.VMEM)
    dma = pltpu.SemaphoreType.DMA
    block = (steps, SEQS, d_model)
    hidden, rec_k, rec_v = pl.pallas_call(
        functools.partial(decode_kernel, n_chunks, n_stages),
        out_shape=(jax.ShapeDtypeStruct(x_steps.shape, BF16),
                   jax.ShapeDtypeStruct((n_layers, batch, steps * n_heads, head_dim), BF16),
                   jax.ShapeDtypeStruct((n_layers, batch, steps * n_heads, head_dim), BF16)),
        in_specs=[any_spec] * 9 + [vmem] * 8,
        out_specs=(any_spec,) * 3,
        scratch_shapes=[
            pltpu.VMEM(w_q.shape, BF16), pltpu.VMEM(w_k.shape, BF16), pltpu.VMEM(w_v.shape, BF16), pltpu.VMEM(w_o.shape, BF16),
            pltpu.VMEM(w_in.shape, BF16), pltpu.VMEM(w_out.shape, BF16),
            pltpu.VMEM((n_chunks,) + block, BF16), pltpu.VMEM(block, BF16),
            pltpu.VMEM((2, steps // 2, SEQS, d_model), BF16), pltpu.VMEM((2, steps // 2, SEQS, d_model), BF16),
            pltpu.VMEM((4, steps // 4, SEQS, d_model), BF16), pltpu.VMEM((steps // 4, SEQS, d_model), BF16),
            pltpu.VMEM((2, steps // 8, SEQS, d_model), BF16),
            pltpu.VMEM((rows, d_model), BF16),
            pltpu.VMEM((2, rows, 128), F32), pltpu.VMEM((2, rows, 128), F32), pltpu.VMEM((2, rows, 128), F32), pltpu.VMEM((2, rows, 128), F32),
            pltpu.VMEM((rows, 256), BF16), pltpu.VMEM((rows, ff), BF16),
            pltpu.VMEM((SEQS, 2, 2 * steps, 128), F32), pltpu.VMEM((SEQS, 2 * steps, 256), F32),
            pltpu.VMEM((2, SEQS, 256, 128), BF16), pltpu.VMEM((2, SEQS, 256, 128), BF16),
            pltpu.VMEM((batch, 128), F32), pltpu.VMEM((batch, 128), F32),
            pltpu.VMEM((n_layers, 1, d_model), F32), pltpu.VMEM((n_layers, 1, d_model), F32),
            pltpu.VMEM((n_layers, 1, ff), F32), pltpu.VMEM((n_layers, 1, d_model), F32),
            dma((n_layers, 6)), dma((n_chunks,)), dma((2, 2)), dma((2, 2)), dma((n_chunks,)), dma((6, 2)), dma((6, 4)),
        ],
        compiler_params=pltpu.CompilerParams(collective_id=0, has_side_effects=True, vmem_limit_bytes=60 * 1024 * 1024),
        name="decode",
    )(x_steps, k_cache.reshape(flat), v_cache.reshape(flat), w_q, w_k, w_v, w_o, w_in, w_out,
      lens, inv_freq, cos_t, sin_t, ln_gain, ln_bias, b_in, b_out)

    pairs = n_layers * batch
    n_blocks, depth = 16, 4
    size = pairs // n_blocks
    lines = (pairs, cache_len, n_heads, head_dim)
    new = (pairs, steps, n_heads, head_dim)
    hidden, k_out, v_out = pl.pallas_call(
        functools.partial(merge_kernel, n_blocks),
        out_shape=(jax.ShapeDtypeStruct(x_steps.shape, BF16),) + (jax.ShapeDtypeStruct(lines, BF16),) * 2,
        in_specs=[pl.BlockSpec(memory_space=pltpu.SMEM)] + [any_spec] * 5,
        out_specs=(any_spec,) * 3,
        scratch_shapes=[pltpu.VMEM((depth, steps // n_blocks) + x_steps.shape[1:], BF16),
                        pltpu.VMEM((depth, size) + lines[1:], BF16), pltpu.VMEM((depth, size) + lines[1:], BF16),
                        pltpu.VMEM((depth, size) + new[1:], BF16), pltpu.VMEM((depth, size) + new[1:], BF16), dma((5, depth)), dma((3, depth))],
        name="merge",
    )(cur_len, hidden, k_cache.reshape(lines), v_cache.reshape(lines), rec_k.reshape(new), rec_v.reshape(new))
    return hidden, k_out.reshape(k_cache.shape), v_out.reshape(v_cache.shape)


def solution(mesh):
    cache_spec = P(None, "dp", None, "tp", None)
    in_specs = (P(None, "dp", None), P("dp"), cache_spec, cache_spec, P(None, None), P(None, None),
                P(None, None, "tp"), P(None, None, "tp"), P(None, None, "tp"), P(None, "tp", None),
                P(None, None, "tp"), P(None, "tp"), P(None, "tp", None), P(None, None))
    out_specs = (P(None, "dp", None), cache_spec, cache_spec)
    return jax.shard_map(decode_shard, mesh=mesh, in_specs=in_specs, out_specs=out_specs, check_vma=False)
```

```python
import functools

import jax
import jax.numpy as jnp
import numpy as np
from jax import lax
from jax.experimental import pallas as pl
from jax.experimental.pallas import tpu as pltpu
from jax.sharding import PartitionSpec as P

ROT_DIM = 64
LN_EPS = 1e-5
MESH = pl.DeviceIdType.MESH
F32 = jnp.float32
BF16 = jnp.bfloat16
SEQS = 8
OLD = 96


def decode_kernel(n_chunks, n_stages, x_hbm, k_hbm, v_hbm, wq_hbm, wk_hbm, wv_hbm, wo_hbm, win_hbm, wout_hbm,
                  lens, inv_freq, cos_t, sin_t, gain_in, bias_in, b_in_in, b_out_in,
                  out_hbm, rec_k, rec_v,
                  wq, wk, wv, wo, win, wout, hid, part, recv0, sum0, recv1, sum1, recv2,
                  normed, qf, kf, vf, cf, ctx, act, inter, scores, kbuf, vbuf,
                  cos_c, sin_c, gain, bias, b_in, b_out,
                  w_sem, x_sem, kv_sem, rec_sem, out_sem, send_sem, recv_sem):
    steps = x_hbm.shape[0]
    rows = steps * SEQS
    half, quarter, eighth = steps // 2, steps // 4, steps // 8
    d_model = x_hbm.shape[2]
    me = lax.axis_index("tp")
    core = lax.rem(me, 2)
    px = lax.rem(lax.div(me, 2), 2)
    py = lax.div(me, 4)
    partner = me + 1 - 2 * core
    x_peer = me + 2 * (1 - 2 * px)
    y_peer = me + 4 * (1 - 2 * py)
    first = (1 - core) * x_peer + core * y_peer
    second = (1 - core) * y_peer + core * x_peer
    pos1 = (1 - core) * px + core * py
    pos2 = (1 - core) * py + core * px
    base0 = half * core
    base1 = base0 + quarter * pos1
    base2 = base1 + eighth * pos2

    weight_pairs = ((wq_hbm, wq), (wk_hbm, wk), (wv_hbm, wv), (win_hbm, win), (wo_hbm, wo), (wout_hbm, wout))

    def weight_copy(layer, j):
        src, dst = weight_pairs[j]
        return pltpu.make_async_copy(src.at[layer], dst.at[layer], w_sem.at[layer, j])

    def x_copy(chunk):
        return pltpu.make_async_copy(x_hbm.at[:, pl.ds(pl.multiple_of(chunk * SEQS, SEQS), SEQS), :], hid.at[chunk], x_sem.at[chunk])

    def out_copy(chunk):
        return pltpu.make_async_copy(hid.at[chunk], out_hbm.at[:, pl.ds(pl.multiple_of(chunk * SEQS, SEQS), SEQS), :], out_sem.at[chunk])

    def kv_copies(stage):
        layer, chunk, slot = lax.div(stage, n_chunks), lax.rem(stage, n_chunks), lax.rem(stage, 2)
        seqs = pl.ds(chunk * SEQS, SEQS)
        return (pltpu.make_async_copy(k_hbm.at[layer, seqs], kbuf.at[slot], kv_sem.at[0, slot]),
                pltpu.make_async_copy(v_hbm.at[layer, seqs], vbuf.at[slot], kv_sem.at[1, slot]))

    def rec_copies(stage):
        layer, chunk, slot = lax.div(stage, n_chunks), lax.rem(stage, n_chunks), lax.rem(stage, 2)
        seqs = pl.ds(chunk * SEQS, SEQS)
        new = pl.ds(2 * OLD, 2 * steps)
        return (pltpu.make_async_copy(kbuf.at[slot, :, new, :], rec_k.at[layer, seqs], rec_sem.at[0, slot]),
                pltpu.make_async_copy(vbuf.at[slot, :, new, :], rec_v.at[layer, seqs], rec_sem.at[1, slot]))

    def remote(phase, stage, src, dst, peer):
        slot = lax.rem(stage, 2)
        return pltpu.make_async_remote_copy(src_ref=src, dst_ref=dst, send_sem=send_sem.at[phase, slot], recv_sem=recv_sem.at[phase, lax.rem(stage, 4)],
                                            device_id={"tp": peer}, device_id_type=MESH)

    def phase0(stage):
        return remote(0, stage, part.at[pl.ds(half - base0, half)], recv0.at[lax.rem(stage, 2)], partner)

    def phase1(stage):
        return remote(1, stage, sum0.at[lax.rem(stage, 2), pl.ds(quarter * (1 - pos1), quarter)], recv1.at[lax.rem(stage, 4)], first)

    def phase2(stage):
        return remote(2, stage, sum1.at[lax.rem(stage, 2), pl.ds(eighth * (1 - pos2), eighth)], recv2.at[lax.rem(stage, 4)], second)

    def gather(phase, stage, start, size, peer):
        block = hid.at[lax.rem(stage, n_chunks), pl.ds(start, size)]
        return remote(phase, stage, block, block, peer)

    def phase3(stage):
        return gather(3, stage, base2, eighth, second)

    def phase4(stage):
        return gather(4, stage, base1, quarter, first)

    def phase5(stage):
        return gather(5, stage, base0, half, partner)

    barrier = pltpu.get_barrier_semaphore()
    for peer in (partner, x_peer, y_peer):
        pl.semaphore_signal(barrier, inc=1, device_id={"tp": peer}, device_id_type=MESH)
    x_copy(0).start()
    for j in range(3):
        weight_copy(0, j).start()
    for copy in kv_copies(0):
        copy.start()
    for j in range(3, 6):
        weight_copy(0, j).start()
    for chunk in range(1, n_chunks):
        x_copy(chunk).start()
    for j in range(6):
        weight_copy(1, j).start()
    angles = lens[:, 0:128].astype(F32) * inv_freq[...]
    odd = lax.rem(lax.broadcasted_iota(jnp.int32, angles.shape, 1), 2) == 1
    cos_c[...] = jnp.cos(angles)
    sin_c[...] = jnp.where(odd, jnp.sin(angles), -jnp.sin(angles))
    for src, dst in ((gain_in, gain), (bias_in, bias), (b_in_in, b_in), (b_out_in, b_out)):
        for layer in range(src.shape[0]):
            dst[layer] = src[layer:layer + 1, :].astype(F32)
    pl.semaphore_wait(barrier, 3)

    def norm_and_project(stage, layer, chunk):
        @pl.when(layer == 0)
        def _():
            x_copy(chunk).wait()

        group = 8

        @pl.loop(0, steps // group)
        def _(g):
            x = hid[chunk, pl.ds(g * group, group)].astype(F32)
            mean = jnp.mean(x, axis=-1, keepdims=True)
            centered = x - mean
            var = jnp.mean(centered * centered, axis=-1, keepdims=True)
            y = centered * lax.rsqrt(var + LN_EPS) * gain[layer][None] + bias[layer][None]
            normed[pl.ds(pl.multiple_of(g * group * SEQS, group * SEQS), group * SEQS), :] = y.reshape(group * SEQS, d_model).astype(BF16)

        @pl.when(chunk == 0)
        def _():
            for j in range(3):
                weight_copy(layer, j).wait()

        here = pl.ds(pl.multiple_of(chunk * SEQS, SEQS), SEQS)
        cc, sc = cos_c[here, :][None], sin_c[here, :][None]
        ct, st = cos_t[...], sin_t[...]
        cos = (cc * ct - sc * st).reshape(rows, 128)
        sin = (sc * ct + cc * st).reshape(rows, 128)
        even = lax.rem(lax.broadcasted_iota(jnp.int32, (rows, 128), 1), 2) == 0

        for weight, dst, rotate in ((wq, qf, True), (wk, kf, True), (wv, vf, False)):
            vec = jnp.dot(normed[...], weight[layer], preferred_element_type=F32)
            for h in range(2):
                piece = vec[:, h * 128:(h + 1) * 128]
                if rotate:
                    swapped = jnp.where(even, pltpu.roll(piece, 127, 1), pltpu.roll(piece, 1, 1))
                    piece = piece * cos + swapped * sin
                dst[h] = piece

    def attend(stage, layer, chunk):
        slot = lax.rem(stage, 2)
        for copy in kv_copies(stage):
            copy.wait()
        shape = (2 * steps, 2 * (OLD + steps))
        row, col = lax.broadcasted_iota(jnp.int32, shape, 0), lax.broadcasted_iota(jnp.int32, shape, 1)
        col_slot, col_head = lax.shift_right_logical(col, 1), lax.bitwise_and(col, 1)
        row_head, row_step = lax.div(row, steps), lax.rem(row, steps)
        never = 1 << 20
        fresh = jnp.where(col_slot - OLD <= row_step, -1, never)
        key = jnp.where(row_head == col_head, jnp.where(col_slot >= OLD, fresh, col_slot), never)
        here = pl.ds(pl.multiple_of(chunk * SEQS, SEQS), SEQS)
        limit = lens[here, :]
        for b in range(SEQS):
            mine = pl.ds(b, steps, stride=SEQS)
            for src, buf, j in ((kf, kbuf, 0), (vf, vbuf, 1)):
                for h in range(2):
                    inter[b, j, pl.ds(h, steps, stride=2), :] = src[h, mine, :]
                buf[slot, b, pl.ds(2 * OLD, 2 * steps), :] = inter[b, j].astype(BF16)
        for copy in rec_copies(stage):
            copy.start()
        for b in range(SEQS):
            mine = pl.ds(b, steps, stride=SEQS)
            query = jnp.concatenate([qf[0, mine, :], qf[1, mine, :]], axis=0).astype(BF16)
            s = lax.dot_general(query, kbuf[slot, b], (((1,), (1,)), ((), ())), preferred_element_type=F32) * (128 ** -0.5)
            scores[b] = jnp.where(key < limit[b:b + 1, :], s, -jnp.inf)
        for b in range(SEQS):
            s = scores[b]
            e = jnp.exp(s - jnp.max(s, axis=-1, keepdims=True))
            probs = (e * (1.0 / jnp.sum(e, axis=-1, keepdims=True))).astype(BF16)
            context = jnp.dot(probs, vbuf[slot, b], preferred_element_type=F32)
            for h in range(2):
                cf[h, pl.ds(b, steps, stride=SEQS), :] = context[h * steps:(h + 1) * steps]

    def feed_forward(layer, chunk):
        @pl.when(chunk == 0)
        def _():
            for j in range(3, 6):
                weight_copy(layer, j).wait()

        @pl.loop(0, act.shape[1] // 256)
        def _(n):
            cols = pl.ds(pl.multiple_of(n * 256, 256), 256)
            pre = jnp.dot(normed[...], win[layer, :, cols], preferred_element_type=F32) + b_in[layer, :, cols]
            act[:, cols] = jax.nn.gelu(pre, approximate=True).astype(BF16)

    def project_out(stage, layer):
        for h in range(2):
            ctx[:, h * 128:(h + 1) * 128] = cf[h].astype(BF16)

        @pl.loop(0, d_model // 256)
        def _(n):
            cols = pl.ds(pl.multiple_of(n * 256, 256), 256)
            total = jnp.dot(ctx[...], wo[layer, :, cols], preferred_element_type=F32)
            total += jnp.dot(act[...], wout[layer, :, cols], preferred_element_type=F32)
            part[:, :, cols] = total.reshape(steps, SEQS, 256).astype(BF16)

    def between(i, lag):
        return jnp.logical_and(i >= lag, i < n_stages + lag)

    @pl.loop(0, n_stages + 6)
    def _(i):
        layer, chunk = lax.div(i, n_chunks), lax.rem(i, n_chunks)
        live = i < n_stages

        @pl.when(live)
        def _():
            norm_and_project(i, layer, chunk)

            @pl.when(i >= 1)
            def _():
                for copy in rec_copies(i - 1):
                    copy.wait()

            @pl.when(i + 1 < n_stages)
            def _():
                for copy in kv_copies(i + 1):
                    copy.start()

            attend(i, layer, chunk)

        @pl.when(between(i, 1))
        def _():
            s = i - 1
            phase0(s).wait()

            @pl.loop(0, half // 4)
            def _(g):
                ts = pl.ds(g * 4, 4)
                sum0[lax.rem(s, 2), ts] = part[pl.ds(base0 + g * 4, 4)] + recv0[lax.rem(s, 2), ts]

            phase1(s).start()

        @pl.when(between(i, 2))
        def _():
            s = i - 2
            phase1(s).wait()

            @pl.loop(0, quarter // 4)
            def _(g):
                ts = pl.ds(g * 4, 4)
                sum1[lax.rem(s, 2), ts] = sum0[lax.rem(s, 2), pl.ds(quarter * pos1 + g * 4, 4)] + recv1[lax.rem(s, 4), ts]

            phase2(s).start()

        @pl.when(between(i, 3))
        def _():
            s = i - 3
            where = lax.rem(s, n_chunks)
            phase2(s).wait()
            own = pl.ds(base2, eighth)
            total = sum1[lax.rem(s, 2), pl.ds(eighth * pos2, eighth)].astype(F32) + recv2[lax.rem(s, 4)].astype(F32)
            total = total + hid[where, own].astype(F32) + b_out[lax.div(s, n_chunks)][None]
            hid[where, own] = total.astype(BF16)
            phase3(s).start()

        @pl.when(between(i, 4))
        def _():
            phase3(i - 4).wait()
            phase4(i - 4).start()

        @pl.when(between(i, 5))
        def _():
            phase4(i - 5).wait()
            phase5(i - 5).start()

        @pl.when(live)
        def _():
            feed_forward(layer, chunk)
            project_out(i, layer)
            phase0(i).start()

        @pl.when(between(i, 5))
        def _():
            s = i - 5
            phase5(s).wait()

            @pl.when(s >= n_stages - n_chunks)
            def _():
                out_copy(lax.rem(s, n_chunks)).start()

    for copy in rec_copies(n_stages - 1):
        copy.wait()
    for chunk in range(n_chunks):
        out_copy(chunk).wait()


def merge_kernel(n_blocks, lens, hid_in, k_hbm, v_hbm, rec_k, rec_v, hid_out, k_out, v_out, hbuf, kbuf, vbuf, rk, rv, in_sem, out_sem):
    depth, size = kbuf.shape[:2]
    steps = rk.shape[2]
    ahead = depth // 2

    def loads(i):
        slot = lax.rem(i, depth)
        pairs = ((hid_in, hbuf), (k_hbm, kbuf), (v_hbm, vbuf), (rec_k, rk), (rec_v, rv))
        return [pltpu.make_async_copy(src.at[pl.ds(i * dst.shape[1], dst.shape[1])], dst.at[slot], in_sem.at[j, slot]) for j, (src, dst) in enumerate(pairs)]

    def stores(i):
        slot = lax.rem(i, depth)
        pairs = ((hbuf, hid_out), (kbuf, k_out), (vbuf, v_out))
        return [pltpu.make_async_copy(src.at[slot], dst.at[pl.ds(i * src.shape[1], src.shape[1])], out_sem.at[j, slot]) for j, (src, dst) in enumerate(pairs)]

    for i in range(ahead):
        for copy in loads(i):
            copy.start()

    @pl.loop(0, n_blocks)
    def _(i):
        slot = lax.rem(i, depth)

        @pl.when(i >= depth - ahead)
        def _():
            for copy in stores(i - (depth - ahead)):
                copy.wait()

        @pl.when(i + ahead < n_blocks)
        def _():
            for copy in loads(i + ahead):
                copy.start()

        for copy in loads(i):
            copy.wait()
        for b in range(size):
            at = lens[lax.rem(i * size + b, lens.shape[0])]
            kbuf[slot, b, pl.ds(at, steps)] = rk[slot, b]
            vbuf[slot, b, pl.ds(at, steps)] = rv[slot, b]
        for copy in stores(i):
            copy.start()

    for i in range(n_blocks - (depth - ahead), n_blocks):
        for copy in stores(i):
            copy.wait()


def inverse_frequencies():
    lane = np.arange(128)
    return np.where(lane < ROT_DIM, 1.0 / (10000.0 ** ((lane // 2 * 2) / ROT_DIM)), 0.0)


def decode_shard(x_steps, cur_len, k_cache, v_cache, ln_gain, ln_bias, w_q, w_k, w_v, w_o, w_in, b_in, w_out, b_out):
    n_layers, batch, cache_len, n_heads, head_dim = k_cache.shape
    steps, _, d_model = x_steps.shape
    ff = w_in.shape[2]
    n_chunks = batch // SEQS
    n_stages = n_layers * n_chunks
    rows = steps * SEQS
    flat = (n_layers, batch, cache_len * n_heads, head_dim)
    step_angles = np.arange(steps)[:, None] * inverse_frequencies()[None, :]
    signed = np.where(np.arange(128) % 2 == 0, -1.0, 1.0)
    cos_t, sin_t = (np.repeat(tab.astype(np.float32)[:, None, :], SEQS, axis=1) for tab in (np.cos(step_angles), np.sin(step_angles) * signed))
    inv_freq = np.broadcast_to(inverse_frequencies().astype(np.float32), (batch, 128))
    lens = jnp.broadcast_to(cur_len[:, None], (batch, cache_len * n_heads))
    any_spec, vmem = pl.BlockSpec(memory_space=pl.ANY), pl.BlockSpec(memory_space=pltpu.VMEM)
    dma = pltpu.SemaphoreType.DMA
    block = (steps, SEQS, d_model)
    hidden, rec_k, rec_v = pl.pallas_call(
        functools.partial(decode_kernel, n_chunks, n_stages),
        out_shape=(jax.ShapeDtypeStruct(x_steps.shape, BF16),
                   jax.ShapeDtypeStruct((n_layers, batch, steps * n_heads, head_dim), BF16),
                   jax.ShapeDtypeStruct((n_layers, batch, steps * n_heads, head_dim), BF16)),
        in_specs=[any_spec] * 9 + [vmem] * 8,
        out_specs=(any_spec,) * 3,
        scratch_shapes=[
            pltpu.VMEM(w_q.shape, BF16), pltpu.VMEM(w_k.shape, BF16), pltpu.VMEM(w_v.shape, BF16), pltpu.VMEM(w_o.shape, BF16),
            pltpu.VMEM(w_in.shape, BF16), pltpu.VMEM(w_out.shape, BF16),
            pltpu.VMEM((n_chunks,) + block, BF16), pltpu.VMEM(block, BF16),
            pltpu.VMEM((2, steps // 2, SEQS, d_model), BF16), pltpu.VMEM((2, steps // 2, SEQS, d_model), BF16),
            pltpu.VMEM((4, steps // 4, SEQS, d_model), BF16), pltpu.VMEM((2, steps // 4, SEQS, d_model), BF16),
            pltpu.VMEM((4, steps // 8, SEQS, d_model), BF16),
            pltpu.VMEM((rows, d_model), BF16),
            pltpu.VMEM((2, rows, 128), F32), pltpu.VMEM((2, rows, 128), F32), pltpu.VMEM((2, rows, 128), F32), pltpu.VMEM((2, rows, 128), F32),
            pltpu.VMEM((rows, 256), BF16), pltpu.VMEM((rows, ff), BF16),
            pltpu.VMEM((SEQS, 2, 2 * steps, 128), F32), pltpu.VMEM((SEQS, 2 * steps, 256), F32),
            pltpu.VMEM((2, SEQS, 256, 128), BF16), pltpu.VMEM((2, SEQS, 256, 128), BF16),
            pltpu.VMEM((batch, 128), F32), pltpu.VMEM((batch, 128), F32),
            pltpu.VMEM((n_layers, 1, d_model), F32), pltpu.VMEM((n_layers, 1, d_model), F32),
            pltpu.VMEM((n_layers, 1, ff), F32), pltpu.VMEM((n_layers, 1, d_model), F32),
            dma((n_layers, 6)), dma((n_chunks,)), dma((2, 2)), dma((2, 2)), dma((n_chunks,)), dma((6, 2)), dma((6, 4)),
        ],
        compiler_params=pltpu.CompilerParams(collective_id=0, has_side_effects=True, vmem_limit_bytes=60 * 1024 * 1024),
        name="decode",
    )(x_steps, k_cache.reshape(flat), v_cache.reshape(flat), w_q, w_k, w_v, w_o, w_in, w_out,
      lens, inv_freq, cos_t, sin_t, ln_gain, ln_bias, b_in, b_out)

    pairs = n_layers * batch
    n_blocks, depth = 16, 4
    size = pairs // n_blocks
    lines = (pairs, cache_len, n_heads, head_dim)
    new = (pairs, steps, n_heads, head_dim)
    hidden, k_out, v_out = pl.pallas_call(
        functools.partial(merge_kernel, n_blocks),
        out_shape=(jax.ShapeDtypeStruct(x_steps.shape, BF16),) + (jax.ShapeDtypeStruct(lines, BF16),) * 2,
        in_specs=[pl.BlockSpec(memory_space=pltpu.SMEM)] + [any_spec] * 5,
        out_specs=(any_spec,) * 3,
        scratch_shapes=[pltpu.VMEM((depth, steps // n_blocks) + x_steps.shape[1:], BF16),
                        pltpu.VMEM((depth, size) + lines[1:], BF16), pltpu.VMEM((depth, size) + lines[1:], BF16),
                        pltpu.VMEM((depth, size) + new[1:], BF16), pltpu.VMEM((depth, size) + new[1:], BF16), dma((5, depth)), dma((3, depth))],
        name="merge",
    )(cur_len, hidden, k_cache.reshape(lines), v_cache.reshape(lines), rec_k.reshape(new), rec_v.reshape(new))
    return hidden, k_out.reshape(k_cache.shape), v_out.reshape(v_cache.shape)


def solution(mesh):
    cache_spec = P(None, "dp", None, "tp", None)
    in_specs = (P(None, "dp", None), P("dp"), cache_spec, cache_spec, P(None, None), P(None, None),
                P(None, None, "tp"), P(None, None, "tp"), P(None, None, "tp"), P(None, "tp", None),
                P(None, None, "tp"), P(None, "tp"), P(None, "tp", None), P(None, None))
    out_specs = (P(None, "dp", None), cache_spec, cache_spec)
    return jax.shard_map(decode_shard, mesh=mesh, in_specs=in_specs, out_specs=out_specs, check_vma=False)
```

```python
import functools

import jax
import jax.numpy as jnp
import numpy as np
from jax import lax
from jax.experimental import pallas as pl
from jax.experimental.pallas import tpu as pltpu
from jax.sharding import PartitionSpec as P

ROT_DIM = 64
LN_EPS = 1e-5
MESH = pl.DeviceIdType.MESH
F32 = jnp.float32
BF16 = jnp.bfloat16
SEQS = 8
OLD = 96


def decode_kernel(n_chunks, n_stages, x_hbm, k_hbm, v_hbm, wq_hbm, wk_hbm, wv_hbm, wo_hbm, win_hbm, wout_hbm,
                  lens_in, inv_freq, cos_t, sin_t, gain_in, bias_in, b_in_in, b_out_in,
                  out_hbm, rec_k, rec_v,
                  wq, wk, wv, wo, win, wout, hid, part, recv0, sum0, recv1, sum1, recv2,
                  normed, qf, kf, vf, cf, ctx, act, inter, scores, kbuf, vbuf,
                  lens, cos_c, sin_c, gain, bias, b_in, b_out,
                  w_sem, x_sem, kv_sem, rec_sem, out_sem, send_sem, recv_sem):
    steps = x_hbm.shape[0]
    rows = steps * SEQS
    half, quarter, eighth = steps // 2, steps // 4, steps // 8
    d_model = x_hbm.shape[2]
    me = lax.axis_index("tp")
    core = lax.rem(me, 2)
    px = lax.rem(lax.div(me, 2), 2)
    py = lax.div(me, 4)
    partner = me + 1 - 2 * core
    x_peer = me + 2 * (1 - 2 * px)
    y_peer = me + 4 * (1 - 2 * py)
    first = (1 - core) * x_peer + core * y_peer
    second = (1 - core) * y_peer + core * x_peer
    pos1 = (1 - core) * px + core * py
    pos2 = (1 - core) * py + core * px
    base0 = half * core
    base1 = base0 + quarter * pos1
    base2 = base1 + eighth * pos2

    weight_pairs = ((wq_hbm, wq), (wk_hbm, wk), (wv_hbm, wv), (win_hbm, win), (wo_hbm, wo), (wout_hbm, wout))

    def weight_copy(layer, j):
        src, dst = weight_pairs[j]
        return pltpu.make_async_copy(src.at[layer], dst.at[layer], w_sem.at[layer, j])

    def x_copy(chunk):
        return pltpu.make_async_copy(x_hbm.at[:, pl.ds(pl.multiple_of(chunk * SEQS, SEQS), SEQS), :], hid.at[chunk], x_sem.at[chunk])

    def out_copy(chunk):
        return pltpu.make_async_copy(hid.at[chunk], out_hbm.at[:, pl.ds(pl.multiple_of(chunk * SEQS, SEQS), SEQS), :], out_sem.at[chunk])

    def kv_copies(stage):
        layer, chunk, slot = lax.div(stage, n_chunks), lax.rem(stage, n_chunks), lax.rem(stage, 2)
        seqs = pl.ds(chunk * SEQS, SEQS)
        return (pltpu.make_async_copy(k_hbm.at[layer, seqs], kbuf.at[slot], kv_sem.at[0, slot]),
                pltpu.make_async_copy(v_hbm.at[layer, seqs], vbuf.at[slot], kv_sem.at[1, slot]))

    def rec_copies(stage):
        layer, chunk, slot = lax.div(stage, n_chunks), lax.rem(stage, n_chunks), lax.rem(stage, 2)
        seqs = pl.ds(chunk * SEQS, SEQS)
        new = pl.ds(2 * OLD, 2 * steps)
        return (pltpu.make_async_copy(kbuf.at[slot, :, new, :], rec_k.at[layer, seqs], rec_sem.at[0, slot]),
                pltpu.make_async_copy(vbuf.at[slot, :, new, :], rec_v.at[layer, seqs], rec_sem.at[1, slot]))

    def remote(phase, stage, src, dst, peer):
        slot = lax.rem(stage, 2)
        return pltpu.make_async_remote_copy(src_ref=src, dst_ref=dst, send_sem=send_sem.at[phase, slot], recv_sem=recv_sem.at[phase, lax.rem(stage, 4)],
                                            device_id={"tp": peer}, device_id_type=MESH)

    def phase0(stage):
        return remote(0, stage, part.at[pl.ds(half - base0, half)], recv0.at[lax.rem(stage, 2)], partner)

    def phase1(stage):
        return remote(1, stage, sum0.at[lax.rem(stage, 2), pl.ds(quarter * (1 - pos1), quarter)], recv1.at[lax.rem(stage, 4)], first)

    def phase2(stage):
        return remote(2, stage, sum1.at[lax.rem(stage, 2), pl.ds(eighth * (1 - pos2), eighth)], recv2.at[lax.rem(stage, 4)], second)

    def gather(phase, stage, start, size, peer):
        block = hid.at[lax.rem(stage, n_chunks), pl.ds(start, size)]
        return remote(phase, stage, block, block, peer)

    def phase3(stage):
        return gather(3, stage, base2, eighth, second)

    def phase4(stage):
        return gather(4, stage, base1, quarter, first)

    def phase5(stage):
        return gather(5, stage, base0, half, partner)

    barrier = pltpu.get_barrier_semaphore()
    for peer in (partner, x_peer, y_peer):
        pl.semaphore_signal(barrier, inc=1, device_id={"tp": peer}, device_id_type=MESH)
    x_copy(0).start()
    for j in range(3):
        weight_copy(0, j).start()
    for copy in kv_copies(0):
        copy.start()
    for j in range(3, 6):
        weight_copy(0, j).start()
    for chunk in range(1, n_chunks):
        x_copy(chunk).start()
    for j in range(6):
        weight_copy(1, j).start()
    for b in range(lens.shape[0]):
        lens[b:b + 1, :] = jnp.full((1, lens.shape[1]), lens_in[b], jnp.int32)
    angles = lens[:, 0:128].astype(F32) * inv_freq[...]
    odd = lax.rem(lax.broadcasted_iota(jnp.int32, angles.shape, 1), 2) == 1
    cos_c[...] = jnp.cos(angles)
    sin_c[...] = jnp.where(odd, jnp.sin(angles), -jnp.sin(angles))
    for src, dst in ((gain_in, gain), (bias_in, bias), (b_in_in, b_in), (b_out_in, b_out)):
        for layer in range(src.shape[0]):
            dst[layer] = src[layer:layer + 1, :].astype(F32)
    pl.semaphore_wait(barrier, 3)

    def norm_and_project(stage, layer, chunk):
        @pl.when(layer == 0)
        def _():
            x_copy(chunk).wait()

        group = 8

        @pl.loop(0, steps // group)
        def _(g):
            x = hid[chunk, pl.ds(g * group, group)].astype(F32)
            mean = jnp.mean(x, axis=-1, keepdims=True)
            centered = x - mean
            var = jnp.mean(centered * centered, axis=-1, keepdims=True)
            y = centered * lax.rsqrt(var + LN_EPS) * gain[layer][None] + bias[layer][None]
            normed[pl.ds(pl.multiple_of(g * group * SEQS, group * SEQS), group * SEQS), :] = y.reshape(group * SEQS, d_model).astype(BF16)

        @pl.when(chunk == 0)
        def _():
            for j in range(3):
                weight_copy(layer, j).wait()

        here = pl.ds(pl.multiple_of(chunk * SEQS, SEQS), SEQS)
        cc, sc = cos_c[here, :][None], sin_c[here, :][None]
        ct, st = cos_t[...], sin_t[...]
        cos = (cc * ct - sc * st).reshape(rows, 128)
        sin = (sc * ct + cc * st).reshape(rows, 128)
        even = lax.rem(lax.broadcasted_iota(jnp.int32, (rows, 128), 1), 2) == 0

        for weight, dst, rotate in ((wq, qf, True), (wk, kf, True), (wv, vf, False)):
            vec = jnp.dot(normed[...], weight[layer], preferred_element_type=F32)
            for h in range(2):
                piece = vec[:, h * 128:(h + 1) * 128]
                if rotate:
                    swapped = jnp.where(even, pltpu.roll(piece, 127, 1), pltpu.roll(piece, 1, 1))
                    piece = piece * cos + swapped * sin
                dst[h] = piece

    def attend(stage, layer, chunk):
        slot = lax.rem(stage, 2)
        for copy in kv_copies(stage):
            copy.wait()
        shape = (2 * steps, 2 * (OLD + steps))
        row, col = lax.broadcasted_iota(jnp.int32, shape, 0), lax.broadcasted_iota(jnp.int32, shape, 1)
        col_slot, col_head = lax.shift_right_logical(col, 1), lax.bitwise_and(col, 1)
        row_head, row_step = lax.div(row, steps), lax.rem(row, steps)
        never = 1 << 20
        fresh = jnp.where(col_slot - OLD <= row_step, -1, never)
        key = jnp.where(row_head == col_head, jnp.where(col_slot >= OLD, fresh, col_slot), never)
        here = pl.ds(pl.multiple_of(chunk * SEQS, SEQS), SEQS)
        limit = lens[here, :]
        for b in range(SEQS):
            mine = pl.ds(b, steps, stride=SEQS)
            for src, buf, j in ((kf, kbuf, 0), (vf, vbuf, 1)):
                for h in range(2):
                    inter[b, j, pl.ds(h, steps, stride=2), :] = src[h, mine, :]
                buf[slot, b, pl.ds(2 * OLD, 2 * steps), :] = inter[b, j].astype(BF16)
        for copy in rec_copies(stage):
            copy.start()
        for b in range(SEQS):
            mine = pl.ds(b, steps, stride=SEQS)
            query = jnp.concatenate([qf[0, mine, :], qf[1, mine, :]], axis=0).astype(BF16)
            s = lax.dot_general(query, kbuf[slot, b], (((1,), (1,)), ((), ())), preferred_element_type=F32) * (128 ** -0.5)
            scores[b] = jnp.where(key < limit[b:b + 1, :], s, -jnp.inf)
        for b in range(SEQS):
            s = scores[b]
            e = jnp.exp(s - jnp.max(s, axis=-1, keepdims=True))
            probs = (e * (1.0 / jnp.sum(e, axis=-1, keepdims=True))).astype(BF16)
            context = jnp.dot(probs, vbuf[slot, b], preferred_element_type=F32)
            for h in range(2):
                cf[h, pl.ds(b, steps, stride=SEQS), :] = context[h * steps:(h + 1) * steps]

    def feed_forward(layer, chunk):
        @pl.when(chunk == 0)
        def _():
            for j in range(3, 6):
                weight_copy(layer, j).wait()

        @pl.loop(0, act.shape[1] // 256, unroll=2)
        def _(n):
            cols = pl.ds(pl.multiple_of(n * 256, 256), 256)
            pre = jnp.dot(normed[...], win[layer, :, cols], preferred_element_type=F32) + b_in[layer, :, cols]
            act[:, cols] = jax.nn.gelu(pre, approximate=True).astype(BF16)

    def project_out(stage, layer):
        for h in range(2):
            ctx[:, h * 128:(h + 1) * 128] = cf[h].astype(BF16)

        @pl.loop(0, d_model // 256, unroll=2)
        def _(n):
            cols = pl.ds(pl.multiple_of(n * 256, 256), 256)
            total = jnp.dot(ctx[...], wo[layer, :, cols], preferred_element_type=F32)
            total += jnp.dot(act[...], wout[layer, :, cols], preferred_element_type=F32)
            part[:, :, cols] = total.reshape(steps, SEQS, 256).astype(BF16)

    def between(i, lag):
        return jnp.logical_and(i >= lag, i < n_stages + lag)

    @pl.loop(0, n_stages + 6)
    def _(i):
        layer, chunk = lax.div(i, n_chunks), lax.rem(i, n_chunks)
        live = i < n_stages

        @pl.when(live)
        def _():
            norm_and_project(i, layer, chunk)

            @pl.when(i >= 1)
            def _():
                for copy in rec_copies(i - 1):
                    copy.wait()

            @pl.when(i + 1 < n_stages)
            def _():
                for copy in kv_copies(i + 1):
                    copy.start()

            attend(i, layer, chunk)

        @pl.when(between(i, 1))
        def _():
            s = i - 1
            phase0(s).wait()

            @pl.loop(0, half // 4)
            def _(g):
                ts = pl.ds(g * 4, 4)
                sum0[lax.rem(s, 2), ts] = part[pl.ds(base0 + g * 4, 4)] + recv0[lax.rem(s, 2), ts]

            phase1(s).start()

        @pl.when(between(i, 2))
        def _():
            s = i - 2
            phase1(s).wait()

            @pl.loop(0, quarter // 4)
            def _(g):
                ts = pl.ds(g * 4, 4)
                sum1[lax.rem(s, 2), ts] = sum0[lax.rem(s, 2), pl.ds(quarter * pos1 + g * 4, 4)] + recv1[lax.rem(s, 4), ts]

            phase2(s).start()

        @pl.when(between(i, 3))
        def _():
            s = i - 3
            where = lax.rem(s, n_chunks)
            phase2(s).wait()
            own = pl.ds(base2, eighth)
            total = sum1[lax.rem(s, 2), pl.ds(eighth * pos2, eighth)].astype(F32) + recv2[lax.rem(s, 4)].astype(F32)
            total = total + hid[where, own].astype(F32) + b_out[lax.div(s, n_chunks)][None]
            hid[where, own] = total.astype(BF16)
            phase3(s).start()

        @pl.when(between(i, 4))
        def _():
            phase3(i - 4).wait()
            phase4(i - 4).start()

        @pl.when(between(i, 5))
        def _():
            phase4(i - 5).wait()
            phase5(i - 5).start()

        @pl.when(live)
        def _():
            feed_forward(layer, chunk)
            project_out(i, layer)
            phase0(i).start()

        @pl.when(between(i, 5))
        def _():
            s = i - 5
            phase5(s).wait()

            @pl.when(s >= n_stages - n_chunks)
            def _():
                out_copy(lax.rem(s, n_chunks)).start()

    for copy in rec_copies(n_stages - 1):
        copy.wait()
    for chunk in range(n_chunks):
        out_copy(chunk).wait()


def merge_kernel(n_blocks, lens, hid_in, k_hbm, v_hbm, rec_k, rec_v, hid_out, k_out, v_out, hbuf, kbuf, vbuf, rk, rv, in_sem, out_sem):
    size = kbuf.shape[0] // n_blocks
    steps = rk.shape[1]

    def block(ref, i):
        rows = ref.shape[0] // n_blocks
        return ref.at[pl.ds(i * rows, rows)]

    def loads(i):
        pairs = ((k_hbm, kbuf), (v_hbm, vbuf), (rec_k, rk), (rec_v, rv), (hid_in, hbuf))
        return [pltpu.make_async_copy(block(src, i), block(dst, i), in_sem.at[j, i]) for j, (src, dst) in enumerate(pairs)]

    def stores(i):
        pairs = ((kbuf, k_out), (vbuf, v_out), (hbuf, hid_out))
        return [pltpu.make_async_copy(block(src, i), block(dst, i), out_sem.at[j, i]) for j, (src, dst) in enumerate(pairs)]

    for i in range(n_blocks):
        for copy in loads(i):
            copy.start()

    @pl.loop(0, n_blocks)
    def _(i):
        for copy in loads(i):
            copy.wait()
        for b in range(size):
            row = i * size + b
            at = lens[lax.rem(row, lens.shape[0])]
            kbuf[row, pl.ds(at, steps)] = rk[row]
            vbuf[row, pl.ds(at, steps)] = rv[row]
        for copy in stores(i):
            copy.start()

    for i in range(n_blocks):
        for copy in stores(i):
            copy.wait()


def inverse_frequencies():
    lane = np.arange(128)
    return np.where(lane < ROT_DIM, 1.0 / (10000.0 ** ((lane // 2 * 2) / ROT_DIM)), 0.0)


def decode_shard(x_steps, cur_len, k_cache, v_cache, ln_gain, ln_bias, w_q, w_k, w_v, w_o, w_in, b_in, w_out, b_out):
    n_layers, batch, cache_len, n_heads, head_dim = k_cache.shape
    steps, _, d_model = x_steps.shape
    ff = w_in.shape[2]
    n_chunks = batch // SEQS
    n_stages = n_layers * n_chunks
    rows = steps * SEQS
    flat = (n_layers, batch, cache_len * n_heads, head_dim)
    step_angles = np.arange(steps)[:, None] * inverse_frequencies()[None, :]
    signed = np.where(np.arange(128) % 2 == 0, -1.0, 1.0)
    cos_t, sin_t = (np.repeat(tab.astype(np.float32)[:, None, :], SEQS, axis=1) for tab in (np.cos(step_angles), np.sin(step_angles) * signed))
    inv_freq = inverse_frequencies().astype(np.float32)[None, :]
    any_spec, vmem = pl.BlockSpec(memory_space=pl.ANY), pl.BlockSpec(memory_space=pltpu.VMEM)
    dma = pltpu.SemaphoreType.DMA
    block = (steps, SEQS, d_model)
    hidden, rec_k, rec_v = pl.pallas_call(
        functools.partial(decode_kernel, n_chunks, n_stages),
        out_shape=(jax.ShapeDtypeStruct(x_steps.shape, BF16),
                   jax.ShapeDtypeStruct((n_layers, batch, steps * n_heads, head_dim), BF16),
                   jax.ShapeDtypeStruct((n_layers, batch, steps * n_heads, head_dim), BF16)),
        in_specs=[any_spec] * 9 + [pl.BlockSpec(memory_space=pltpu.SMEM)] + [vmem] * 7,
        out_specs=(any_spec,) * 3,
        scratch_shapes=[
            pltpu.VMEM(w_q.shape, BF16), pltpu.VMEM(w_k.shape, BF16), pltpu.VMEM(w_v.shape, BF16), pltpu.VMEM(w_o.shape, BF16),
            pltpu.VMEM(w_in.shape, BF16), pltpu.VMEM(w_out.shape, BF16),
            pltpu.VMEM((n_chunks,) + block, BF16), pltpu.VMEM(block, BF16),
            pltpu.VMEM((2, steps // 2, SEQS, d_model), BF16), pltpu.VMEM((2, steps // 2, SEQS, d_model), BF16),
            pltpu.VMEM((4, steps // 4, SEQS, d_model), BF16), pltpu.VMEM((2, steps // 4, SEQS, d_model), BF16),
            pltpu.VMEM((4, steps // 8, SEQS, d_model), BF16),
            pltpu.VMEM((rows, d_model), BF16),
            pltpu.VMEM((2, rows, 128), F32), pltpu.VMEM((2, rows, 128), F32), pltpu.VMEM((2, rows, 128), F32), pltpu.VMEM((2, rows, 128), F32),
            pltpu.VMEM((rows, 256), BF16), pltpu.VMEM((rows, ff), BF16),
            pltpu.VMEM((SEQS, 2, 2 * steps, 128), F32), pltpu.VMEM((SEQS, 2 * steps, 256), F32),
            pltpu.VMEM((2, SEQS, 256, 128), BF16), pltpu.VMEM((2, SEQS, 256, 128), BF16),
            pltpu.VMEM((batch, cache_len * n_heads), jnp.int32), pltpu.VMEM((batch, 128), F32), pltpu.VMEM((batch, 128), F32),
            pltpu.VMEM((n_layers, 1, d_model), F32), pltpu.VMEM((n_layers, 1, d_model), F32),
            pltpu.VMEM((n_layers, 1, ff), F32), pltpu.VMEM((n_layers, 1, d_model), F32),
            dma((n_layers, 6)), dma((n_chunks,)), dma((2, 2)), dma((2, 2)), dma((n_chunks,)), dma((6, 2)), dma((6, 4)),
        ],
        compiler_params=pltpu.CompilerParams(collective_id=0, has_side_effects=True, vmem_limit_bytes=60 * 1024 * 1024),
        name="decode",
    )(x_steps, k_cache.reshape(flat), v_cache.reshape(flat), w_q, w_k, w_v, w_o, w_in, w_out,
      cur_len, inv_freq, cos_t, sin_t, ln_gain, ln_bias, b_in, b_out)

    pairs = n_layers * batch
    n_blocks = 16
    lines = (pairs, cache_len, n_heads, head_dim)
    new = (pairs, steps, n_heads, head_dim)
    hidden, k_out, v_out = pl.pallas_call(
        functools.partial(merge_kernel, n_blocks),
        out_shape=(jax.ShapeDtypeStruct(x_steps.shape, BF16),) + (jax.ShapeDtypeStruct(lines, BF16),) * 2,
        in_specs=[pl.BlockSpec(memory_space=pltpu.SMEM)] + [any_spec] * 5,
        out_specs=(any_spec,) * 3,
        scratch_shapes=[pltpu.VMEM(x_steps.shape, BF16), pltpu.VMEM(lines, BF16), pltpu.VMEM(lines, BF16),
                        pltpu.VMEM(new, BF16), pltpu.VMEM(new, BF16), dma((5, n_blocks)), dma((3, n_blocks))],
        compiler_params=pltpu.CompilerParams(vmem_limit_bytes=62 * 1024 * 1024),
        name="merge",
    )(cur_len, hidden, k_cache.reshape(lines), v_cache.reshape(lines), rec_k.reshape(new), rec_v.reshape(new))
    return hidden, k_out.reshape(k_cache.shape), v_out.reshape(v_cache.shape)


def solution(mesh):
    cache_spec = P(None, "dp", None, "tp", None)
    in_specs = (P(None, "dp", None), P("dp"), cache_spec, cache_spec, P(None, None), P(None, None),
                P(None, None, "tp"), P(None, None, "tp"), P(None, None, "tp"), P(None, "tp", None),
                P(None, None, "tp"), P(None, "tp"), P(None, "tp", None), P(None, None))
    out_specs = (P(None, "dp", None), cache_spec, cache_spec)
    return jax.shard_map(decode_shard, mesh=mesh, in_specs=in_specs, out_specs=out_specs, check_vma=False)
```

```python
import functools

import jax
import jax.numpy as jnp
import numpy as np
from jax import lax
from jax.experimental import pallas as pl
from jax.experimental.pallas import tpu as pltpu
from jax.sharding import PartitionSpec as P

ROT_DIM = 64
LN_EPS = 1e-5
MESH = pl.DeviceIdType.MESH
F32 = jnp.float32
BF16 = jnp.bfloat16
SEQS = 8
OLD = 96


def decode_kernel(n_chunks, n_stages, x_hbm, k_hbm, v_hbm, wq_hbm, wk_hbm, wv_hbm, wo_hbm, win_hbm, wout_hbm,
                  lens_in, inv_freq, cos_t, sin_t, gain_in, bias_in, b_in_in, b_out_in,
                  out_hbm, rec_k, rec_v,
                  wq, wk, wv, wo, win, wout, hid, part, recv0, sum0, recv1, sum1, recv2,
                  normed, qf, kf, vf, cf, ctx, act, inter, scores, kbuf, vbuf,
                  lens, cos_c, sin_c, gain, bias, b_in, b_out,
                  w_sem, x_sem, kv_sem, rec_sem, out_sem, send_sem, recv_sem):
    steps = x_hbm.shape[0]
    rows = steps * SEQS
    half, quarter, eighth, last = steps // 2, steps // 4, steps // 8, steps // 16
    d_model = x_hbm.shape[2]
    me = lax.axis_index("tp")
    core = lax.rem(me, 2)
    px = lax.rem(lax.div(me, 2), 2)
    py = lax.div(me, 4)
    partner = me + 1 - 2 * core
    x_peer = me + 2 * (1 - 2 * px)
    y_peer = me + 4 * (1 - 2 * py)
    first, second = (x_peer, y_peer), (y_peer, x_peer)
    pos1, pos2 = (px, py), (py, px)
    base = half * core
    base1 = [base + quarter * j + eighth * pos1[j] for j in range(2)]
    base2 = [base1[j] + last * pos2[j] for j in range(2)]

    weight_pairs = ((wq_hbm, wq), (wk_hbm, wk), (wv_hbm, wv), (win_hbm, win), (wo_hbm, wo), (wout_hbm, wout))

    def weight_copy(layer, j):
        src, dst = weight_pairs[j]
        return pltpu.make_async_copy(src.at[layer], dst.at[layer], w_sem.at[layer, j])

    def x_copy(chunk):
        return pltpu.make_async_copy(x_hbm.at[:, pl.ds(pl.multiple_of(chunk * SEQS, SEQS), SEQS), :], hid.at[chunk], x_sem.at[chunk])

    def out_copy(chunk):
        return pltpu.make_async_copy(hid.at[chunk], out_hbm.at[:, pl.ds(pl.multiple_of(chunk * SEQS, SEQS), SEQS), :], out_sem.at[chunk])

    def kv_copies(stage):
        layer, chunk, slot = lax.div(stage, n_chunks), lax.rem(stage, n_chunks), lax.rem(stage, 2)
        seqs = pl.ds(chunk * SEQS, SEQS)
        return (pltpu.make_async_copy(k_hbm.at[layer, seqs], kbuf.at[slot], kv_sem.at[0, slot]),
                pltpu.make_async_copy(v_hbm.at[layer, seqs], vbuf.at[slot], kv_sem.at[1, slot]))

    def rec_copies(stage):
        layer, chunk, slot = lax.div(stage, n_chunks), lax.rem(stage, n_chunks), lax.rem(stage, 2)
        seqs = pl.ds(chunk * SEQS, SEQS)
        new = pl.ds(2 * OLD, 2 * steps)
        return (pltpu.make_async_copy(kbuf.at[slot, :, new, :], rec_k.at[layer, seqs], rec_sem.at[0, slot]),
                pltpu.make_async_copy(vbuf.at[slot, :, new, :], rec_v.at[layer, seqs], rec_sem.at[1, slot]))

    def remote(kind, stage, src, dst, peer):
        return pltpu.make_async_remote_copy(src_ref=src, dst_ref=dst, send_sem=send_sem.at[kind, lax.rem(stage, 2)],
                                            recv_sem=recv_sem.at[kind, lax.rem(stage, 4)], device_id={"tp": peer}, device_id_type=MESH)

    def phase0(stage):
        return remote(0, stage, part.at[pl.ds(half - base, half)], recv0.at[lax.rem(stage, 2)], partner)

    def phase1(stage, j):
        block = pl.ds(quarter * j + eighth * (1 - pos1[j]), eighth)
        return remote(1 + j, stage, sum0.at[lax.rem(stage, 2), block], recv1.at[lax.rem(stage, 4), pl.ds(eighth * j, eighth)], first[j])

    def phase2(stage, j):
        block = pl.ds(eighth * j + last * (1 - pos2[j]), last)
        return remote(3 + j, stage, sum1.at[lax.rem(stage, 2), block], recv2.at[lax.rem(stage, 4), pl.ds(last * j, last)], second[j])

    def gather(kind, stage, start, size, peer):
        block = hid.at[lax.rem(stage, n_chunks), pl.ds(start, size)]
        return remote(kind, stage, block, block, peer)

    def phase3(stage, j):
        return gather(5 + j, stage, base2[j], last, second[j])

    def phase4(stage, j):
        return gather(7 + j, stage, base1[j], eighth, first[j])

    def phase5(stage):
        return gather(9, stage, base, half, partner)

    barrier = pltpu.get_barrier_semaphore()
    for peer in (partner, x_peer, y_peer):
        pl.semaphore_signal(barrier, inc=1, device_id={"tp": peer}, device_id_type=MESH)
    x_copy(0).start()
    for j in range(3):
        weight_copy(0, j).start()
    for copy in kv_copies(0):
        copy.start()
    for j in range(3, 6):
        weight_copy(0, j).start()
    for chunk in range(1, n_chunks):
        x_copy(chunk).start()
    for j in range(6):
        weight_copy(1, j).start()
    for b in range(lens.shape[0]):
        lens[b:b + 1, :] = jnp.full((1, lens.shape[1]), lens_in[b], jnp.int32)
    angles = lens[:, 0:128].astype(F32) * inv_freq[...]
    odd = lax.rem(lax.broadcasted_iota(jnp.int32, angles.shape, 1), 2) == 1
    cos_c[...] = jnp.cos(angles)
    sin_c[...] = jnp.where(odd, jnp.sin(angles), -jnp.sin(angles))
    for src, dst in ((gain_in, gain), (bias_in, bias), (b_in_in, b_in), (b_out_in, b_out)):
        for layer in range(src.shape[0]):
            dst[layer] = src[layer:layer + 1, :].astype(F32)
    pl.semaphore_wait(barrier, 3)

    def norm_and_project(stage, layer, chunk):
        @pl.when(layer == 0)
        def _():
            x_copy(chunk).wait()

        group = 8

        @pl.loop(0, steps // group)
        def _(g):
            x = hid[chunk, pl.ds(g * group, group)].astype(F32)
            mean = jnp.mean(x, axis=-1, keepdims=True)
            centered = x - mean
            var = jnp.mean(centered * centered, axis=-1, keepdims=True)
            y = centered * lax.rsqrt(var + LN_EPS) * gain[layer][None] + bias[layer][None]
            normed[pl.ds(pl.multiple_of(g * group * SEQS, group * SEQS), group * SEQS), :] = y.reshape(group * SEQS, d_model).astype(BF16)

        @pl.when(chunk == 0)
        def _():
            for j in range(3):
                weight_copy(layer, j).wait()

        here = pl.ds(pl.multiple_of(chunk * SEQS, SEQS), SEQS)
        cc, sc = cos_c[here, :][None], sin_c[here, :][None]
        ct, st = cos_t[...], sin_t[...]
        cos = (cc * ct - sc * st).reshape(rows, 128)
        sin = (sc * ct + cc * st).reshape(rows, 128)
        even = lax.rem(lax.broadcasted_iota(jnp.int32, (rows, 128), 1), 2) == 0

        for weight, dst, rotate in ((wq, qf, True), (wk, kf, True), (wv, vf, False)):
            vec = jnp.dot(normed[...], weight[layer], preferred_element_type=F32)
            for h in range(2):
                piece = vec[:, h * 128:(h + 1) * 128]
                if rotate:
                    swapped = jnp.where(even, pltpu.roll(piece, 127, 1), pltpu.roll(piece, 1, 1))
                    piece = piece * cos + swapped * sin
                dst[h] = piece

    def attend(stage, layer, chunk):
        slot = lax.rem(stage, 2)
        for copy in kv_copies(stage):
            copy.wait()
        shape = (2 * steps, 2 * (OLD + steps))
        row, col = lax.broadcasted_iota(jnp.int32, shape, 0), lax.broadcasted_iota(jnp.int32, shape, 1)
        col_slot, col_head = lax.shift_right_logical(col, 1), lax.bitwise_and(col, 1)
        row_head, row_step = lax.div(row, steps), lax.rem(row, steps)
        never = 1 << 20
        fresh = jnp.where(col_slot - OLD <= row_step, -1, never)
        key = jnp.where(row_head == col_head, jnp.where(col_slot >= OLD, fresh, col_slot), never)
        here = pl.ds(pl.multiple_of(chunk * SEQS, SEQS), SEQS)
        limit = lens[here, :]
        for b in range(SEQS):
            mine = pl.ds(b, steps, stride=SEQS)
            for src, buf, j in ((kf, kbuf, 0), (vf, vbuf, 1)):
                for h in range(2):
                    inter[b, j, pl.ds(h, steps, stride=2), :] = src[h, mine, :]
                buf[slot, b, pl.ds(2 * OLD, 2 * steps), :] = inter[b, j].astype(BF16)
        for copy in rec_copies(stage):
            copy.start()
        for b in range(SEQS):
            mine = pl.ds(b, steps, stride=SEQS)
            query = jnp.concatenate([qf[0, mine, :], qf[1, mine, :]], axis=0).astype(BF16)
            s = lax.dot_general(query, kbuf[slot, b], (((1,), (1,)), ((), ())), preferred_element_type=F32) * (128 ** -0.5)
            scores[b] = jnp.where(key < limit[b:b + 1, :], s, -jnp.inf)
        for b in range(SEQS):
            s = scores[b]
            e = jnp.exp(s - jnp.max(s, axis=-1, keepdims=True))
            probs = (e * (1.0 / jnp.sum(e, axis=-1, keepdims=True))).astype(BF16)
            context = jnp.dot(probs, vbuf[slot, b], preferred_element_type=F32)
            for h in range(2):
                cf[h, pl.ds(b, steps, stride=SEQS), :] = context[h * steps:(h + 1) * steps]

    def feed_forward(layer, chunk):
        @pl.when(chunk == 0)
        def _():
            for j in range(3, 6):
                weight_copy(layer, j).wait()

        @pl.loop(0, act.shape[1] // 256, unroll=2)
        def _(n):
            cols = pl.ds(pl.multiple_of(n * 256, 256), 256)
            pre = jnp.dot(normed[...], win[layer, :, cols], preferred_element_type=F32) + b_in[layer, :, cols]
            act[:, cols] = jax.nn.gelu(pre, approximate=True).astype(BF16)

    def project_out(stage, layer):
        for h in range(2):
            ctx[:, h * 128:(h + 1) * 128] = cf[h].astype(BF16)

        @pl.loop(0, d_model // 256, unroll=2)
        def _(n):
            cols = pl.ds(pl.multiple_of(n * 256, 256), 256)
            total = jnp.dot(ctx[...], wo[layer, :, cols], preferred_element_type=F32)
            total += jnp.dot(act[...], wout[layer, :, cols], preferred_element_type=F32)
            part[:, :, cols] = total.reshape(steps, SEQS, 256).astype(BF16)

    def between(i, lag):
        return jnp.logical_and(i >= lag, i < n_stages + lag)

    @pl.loop(0, n_stages + 6)
    def _(i):
        layer, chunk = lax.div(i, n_chunks), lax.rem(i, n_chunks)
        live = i < n_stages

        @pl.when(live)
        def _():
            norm_and_project(i, layer, chunk)

            @pl.when(i >= 1)
            def _():
                for copy in rec_copies(i - 1):
                    copy.wait()

            @pl.when(i + 1 < n_stages)
            def _():
                for copy in kv_copies(i + 1):
                    copy.start()

            attend(i, layer, chunk)

        @pl.when(between(i, 1))
        def _():
            s = i - 1
            phase0(s).wait()
            for j in range(2):
                @pl.loop(0, quarter // 4)
                def _(g):
                    ts = pl.ds(quarter * j + g * 4, 4)
                    sum0[lax.rem(s, 2), ts] = part[pl.ds(base + quarter * j + g * 4, 4)] + recv0[lax.rem(s, 2), ts]

                phase1(s, j).start()

        @pl.when(between(i, 2))
        def _():
            s = i - 2
            for j in range(2):
                phase1(s, j).wait()
                mine = pl.ds(quarter * j + eighth * pos1[j], eighth)
                ts = pl.ds(eighth * j, eighth)
                sum1[lax.rem(s, 2), ts] = sum0[lax.rem(s, 2), mine] + recv1[lax.rem(s, 4), ts]
                phase2(s, j).start()

        @pl.when(between(i, 3))
        def _():
            s = i - 3
            where = lax.rem(s, n_chunks)
            for j in range(2):
                phase2(s, j).wait()
                own = pl.ds(base2[j], last)
                total = sum1[lax.rem(s, 2), pl.ds(eighth * j + last * pos2[j], last)].astype(F32) + recv2[lax.rem(s, 4), pl.ds(last * j, last)].astype(F32)
                total = total + hid[where, own].astype(F32) + b_out[lax.div(s, n_chunks)][None]
                hid[where, own] = total.astype(BF16)
                phase3(s, j).start()

        @pl.when(between(i, 4))
        def _():
            for j in range(2):
                phase3(i - 4, j).wait()
                phase4(i - 4, j).start()

        @pl.when(between(i, 5))
        def _():
            for j in range(2):
                phase4(i - 5, j).wait()
            phase5(i - 5).start()

        @pl.when(live)
        def _():
            feed_forward(layer, chunk)
            project_out(i, layer)
            phase0(i).start()

        @pl.when(between(i, 5))
        def _():
            s = i - 5
            phase5(s).wait()

            @pl.when(s >= n_stages - n_chunks)
            def _():
                out_copy(lax.rem(s, n_chunks)).start()

    for copy in rec_copies(n_stages - 1):
        copy.wait()
    for chunk in range(n_chunks):
        out_copy(chunk).wait()


def merge_kernel(n_blocks, lens, hid_in, k_hbm, v_hbm, rec_k, rec_v, hid_out, k_out, v_out, hbuf, kbuf, vbuf, rk, rv, in_sem, out_sem):
    size = kbuf.shape[0] // n_blocks
    steps = rk.shape[1]

    def block(ref, i):
        rows = ref.shape[0] // n_blocks
        return ref.at[pl.ds(i * rows, rows)]

    def loads(i):
        pairs = ((k_hbm, kbuf), (v_hbm, vbuf), (rec_k, rk), (rec_v, rv), (hid_in, hbuf))
        return [pltpu.make_async_copy(block(src, i), block(dst, i), in_sem.at[j, i]) for j, (src, dst) in enumerate(pairs)]

    def stores(i):
        pairs = ((kbuf, k_out), (vbuf, v_out), (hbuf, hid_out))
        return [pltpu.make_async_copy(block(src, i), block(dst, i), out_sem.at[j, i]) for j, (src, dst) in enumerate(pairs)]

    for i in range(n_blocks):
        for copy in loads(i):
            copy.start()

    @pl.loop(0, n_blocks)
    def _(i):
        for copy in loads(i):
            copy.wait()
        for b in range(size):
            row = i * size + b
            at = lens[lax.rem(row, lens.shape[0])]
            kbuf[row, pl.ds(at, steps)] = rk[row]
            vbuf[row, pl.ds(at, steps)] = rv[row]
        for copy in stores(i):
            copy.start()

    for i in range(n_blocks):
        for copy in stores(i):
            copy.wait()


def inverse_frequencies():
    lane = np.arange(128)
    return np.where(lane < ROT_DIM, 1.0 / (10000.0 ** ((lane // 2 * 2) / ROT_DIM)), 0.0)


def decode_shard(x_steps, cur_len, k_cache, v_cache, ln_gain, ln_bias, w_q, w_k, w_v, w_o, w_in, b_in, w_out, b_out):
    n_layers, batch, cache_len, n_heads, head_dim = k_cache.shape
    steps, _, d_model = x_steps.shape
    ff = w_in.shape[2]
    n_chunks = batch // SEQS
    n_stages = n_layers * n_chunks
    rows = steps * SEQS
    flat = (n_layers, batch, cache_len * n_heads, head_dim)
    step_angles = np.arange(steps)[:, None] * inverse_frequencies()[None, :]
    signed = np.where(np.arange(128) % 2 == 0, -1.0, 1.0)
    cos_t, sin_t = (np.repeat(tab.astype(np.float32)[:, None, :], SEQS, axis=1) for tab in (np.cos(step_angles), np.sin(step_angles) * signed))
    inv_freq = inverse_frequencies().astype(np.float32)[None, :]
    any_spec, vmem = pl.BlockSpec(memory_space=pl.ANY), pl.BlockSpec(memory_space=pltpu.VMEM)
    dma = pltpu.SemaphoreType.DMA
    block = (steps, SEQS, d_model)
    hidden, rec_k, rec_v = pl.pallas_call(
        functools.partial(decode_kernel, n_chunks, n_stages),
        out_shape=(jax.ShapeDtypeStruct(x_steps.shape, BF16),
                   jax.ShapeDtypeStruct((n_layers, batch, steps * n_heads, head_dim), BF16),
                   jax.ShapeDtypeStruct((n_layers, batch, steps * n_heads, head_dim), BF16)),
        in_specs=[any_spec] * 9 + [pl.BlockSpec(memory_space=pltpu.SMEM)] + [vmem] * 7,
        out_specs=(any_spec,) * 3,
        scratch_shapes=[
            pltpu.VMEM(w_q.shape, BF16), pltpu.VMEM(w_k.shape, BF16), pltpu.VMEM(w_v.shape, BF16), pltpu.VMEM(w_o.shape, BF16),
            pltpu.VMEM(w_in.shape, BF16), pltpu.VMEM(w_out.shape, BF16),
            pltpu.VMEM((n_chunks,) + block, BF16), pltpu.VMEM(block, BF16),
            pltpu.VMEM((2, steps // 2, SEQS, d_model), BF16), pltpu.VMEM((2, steps // 2, SEQS, d_model), BF16),
            pltpu.VMEM((4, steps // 4, SEQS, d_model), BF16), pltpu.VMEM((2, steps // 4, SEQS, d_model), BF16),
            pltpu.VMEM((4, steps // 8, SEQS, d_model), BF16),
            pltpu.VMEM((rows, d_model), BF16),
            pltpu.VMEM((2, rows, 128), F32), pltpu.VMEM((2, rows, 128), F32), pltpu.VMEM((2, rows, 128), F32), pltpu.VMEM((2, rows, 128), F32),
            pltpu.VMEM((rows, 256), BF16), pltpu.VMEM((rows, ff), BF16),
            pltpu.VMEM((SEQS, 2, 2 * steps, 128), F32), pltpu.VMEM((SEQS, 2 * steps, 256), F32),
            pltpu.VMEM((2, SEQS, 256, 128), BF16), pltpu.VMEM((2, SEQS, 256, 128), BF16),
            pltpu.VMEM((batch, cache_len * n_heads), jnp.int32), pltpu.VMEM((batch, 128), F32), pltpu.VMEM((batch, 128), F32),
            pltpu.VMEM((n_layers, 1, d_model), F32), pltpu.VMEM((n_layers, 1, d_model), F32),
            pltpu.VMEM((n_layers, 1, ff), F32), pltpu.VMEM((n_layers, 1, d_model), F32),
            dma((n_layers, 6)), dma((n_chunks,)), dma((2, 2)), dma((2, 2)), dma((n_chunks,)), dma((10, 2)), dma((10, 4)),
        ],
        compiler_params=pltpu.CompilerParams(collective_id=0, has_side_effects=True, vmem_limit_bytes=60 * 1024 * 1024),
        name="decode",
    )(x_steps, k_cache.reshape(flat), v_cache.reshape(flat), w_q, w_k, w_v, w_o, w_in, w_out,
      cur_len, inv_freq, cos_t, sin_t, ln_gain, ln_bias, b_in, b_out)

    pairs = n_layers * batch
    n_blocks = 16
    lines = (pairs, cache_len, n_heads, head_dim)
    new = (pairs, steps, n_heads, head_dim)
    hidden, k_out, v_out = pl.pallas_call(
        functools.partial(merge_kernel, n_blocks),
        out_shape=(jax.ShapeDtypeStruct(x_steps.shape, BF16),) + (jax.ShapeDtypeStruct(lines, BF16),) * 2,
        in_specs=[pl.BlockSpec(memory_space=pltpu.SMEM)] + [any_spec] * 5,
        out_specs=(any_spec,) * 3,
        scratch_shapes=[pltpu.VMEM(x_steps.shape, BF16), pltpu.VMEM(lines, BF16), pltpu.VMEM(lines, BF16),
                        pltpu.VMEM(new, BF16), pltpu.VMEM(new, BF16), dma((5, n_blocks)), dma((3, n_blocks))],
        compiler_params=pltpu.CompilerParams(vmem_limit_bytes=62 * 1024 * 1024),
        name="merge",
    )(cur_len, hidden, k_cache.reshape(lines), v_cache.reshape(lines), rec_k.reshape(new), rec_v.reshape(new))
    return hidden, k_out.reshape(k_cache.shape), v_out.reshape(v_cache.shape)


def solution(mesh):
    cache_spec = P(None, "dp", None, "tp", None)
    in_specs = (P(None, "dp", None), P("dp"), cache_spec, cache_spec, P(None, None), P(None, None),
                P(None, None, "tp"), P(None, None, "tp"), P(None, None, "tp"), P(None, "tp", None),
                P(None, None, "tp"), P(None, "tp"), P(None, "tp", None), P(None, None))
    out_specs = (P(None, "dp", None), cache_spec, cache_spec)
    return jax.shard_map(decode_shard, mesh=mesh, in_specs=in_specs, out_specs=out_specs, check_vma=False)
```

```python
import functools

import jax
import jax.numpy as jnp
import numpy as np
from jax import lax
from jax.experimental import pallas as pl
from jax.experimental.pallas import tpu as pltpu
from jax.sharding import PartitionSpec as P

ROT_DIM = 64
LN_EPS = 1e-5
MESH = pl.DeviceIdType.MESH
F32 = jnp.float32
BF16 = jnp.bfloat16
SEQS = 8
OLD = 96


def decode_kernel(n_chunks, n_stages, x_hbm, k_hbm, v_hbm, wq_hbm, wk_hbm, wv_hbm, wo_hbm, win_hbm, wout_hbm,
                  lens_in, inv_freq, cos_t, sin_t, gain_in, bias_in, b_in_in, b_out_in,
                  out_hbm, rec_k, rec_v,
                  wq, wk, wv, wo, win, wout, hid, part, recv0, sum0, recv1, sum1, recv2,
                  normed, qf, kf, vf, cf, ctx, act, inter, scores, kbuf, vbuf,
                  lens, cos_c, sin_c, gain, bias, b_in, b_out,
                  w_sem, x_sem, kv_sem, rec_sem, out_sem, send_sem, recv_sem):
    steps = x_hbm.shape[0]
    rows = steps * SEQS
    half, quarter, eighth, last = steps // 2, steps // 4, steps // 8, steps // 16
    d_model = x_hbm.shape[2]
    me = lax.axis_index("tp")
    core = lax.rem(me, 2)
    px = lax.rem(lax.div(me, 2), 2)
    py = lax.div(me, 4)
    partner = me + 1 - 2 * core
    x_peer = me + 2 * (1 - 2 * px)
    y_peer = me + 4 * (1 - 2 * py)
    first, second = (x_peer, y_peer), (y_peer, x_peer)
    pos1, pos2 = (px, py), (py, px)
    base = half * core
    base1 = [base + quarter * j + eighth * pos1[j] for j in range(2)]
    base2 = [base1[j] + last * pos2[j] for j in range(2)]

    weight_pairs = ((wq_hbm, wq), (wk_hbm, wk), (wv_hbm, wv), (win_hbm, win), (wo_hbm, wo), (wout_hbm, wout))

    def weight_copy(layer, j):
        src, dst = weight_pairs[j]
        return pltpu.make_async_copy(src.at[layer], dst.at[layer], w_sem.at[layer, j])

    def x_copy(chunk):
        return pltpu.make_async_copy(x_hbm.at[:, pl.ds(pl.multiple_of(chunk * SEQS, SEQS), SEQS), :], hid.at[chunk], x_sem.at[chunk])

    def out_copy(chunk):
        return pltpu.make_async_copy(hid.at[chunk], out_hbm.at[:, pl.ds(pl.multiple_of(chunk * SEQS, SEQS), SEQS), :], out_sem.at[chunk])

    def kv_copies(stage):
        layer, chunk, slot = lax.div(stage, n_chunks), lax.rem(stage, n_chunks), lax.rem(stage, 2)
        seqs = pl.ds(chunk * SEQS, SEQS)
        return (pltpu.make_async_copy(k_hbm.at[layer, seqs], kbuf.at[slot], kv_sem.at[0, slot]),
                pltpu.make_async_copy(v_hbm.at[layer, seqs], vbuf.at[slot], kv_sem.at[1, slot]))

    def rec_copies(stage):
        layer, chunk, slot = lax.div(stage, n_chunks), lax.rem(stage, n_chunks), lax.rem(stage, 2)
        seqs = pl.ds(chunk * SEQS, SEQS)
        new = pl.ds(2 * OLD, 2 * steps)
        return (pltpu.make_async_copy(kbuf.at[slot, :, new, :], rec_k.at[layer, seqs], rec_sem.at[0, slot]),
                pltpu.make_async_copy(vbuf.at[slot, :, new, :], rec_v.at[layer, seqs], rec_sem.at[1, slot]))

    def remote(kind, stage, src, dst, peer):
        return pltpu.make_async_remote_copy(src_ref=src, dst_ref=dst, send_sem=send_sem.at[kind, lax.rem(stage, 2)],
                                            recv_sem=recv_sem.at[kind, lax.rem(stage, 4)], device_id={"tp": peer}, device_id_type=MESH)

    def phase0(stage):
        return remote(0, stage, part.at[pl.ds(half - base, half)], recv0.at[lax.rem(stage, 2)], partner)

    def phase1(stage, j):
        block = pl.ds(quarter * j + eighth * (1 - pos1[j]), eighth)
        return remote(1 + j, stage, sum0.at[lax.rem(stage, 2), block], recv1.at[lax.rem(stage, 4), pl.ds(eighth * j, eighth)], first[j])

    def phase2(stage, j):
        block = pl.ds(eighth * j + last * (1 - pos2[j]), last)
        return remote(3 + j, stage, sum1.at[lax.rem(stage, 2), block], recv2.at[lax.rem(stage, 4), pl.ds(last * j, last)], second[j])

    def gather(kind, stage, start, size, peer):
        block = hid.at[lax.rem(stage, n_chunks), pl.ds(start, size)]
        return remote(kind, stage, block, block, peer)

    def phase3(stage, j):
        return gather(5 + j, stage, base2[j], last, second[j])

    def phase4(stage, j):
        return gather(7 + j, stage, base1[j], eighth, first[j])

    def phase5(stage):
        return gather(9, stage, base, half, partner)

    barrier = pltpu.get_barrier_semaphore()
    for peer in (partner, x_peer, y_peer):
        pl.semaphore_signal(barrier, inc=1, device_id={"tp": peer}, device_id_type=MESH)
    x_copy(0).start()
    for j in range(3):
        weight_copy(0, j).start()
    for copy in kv_copies(0):
        copy.start()
    for j in range(3, 6):
        weight_copy(0, j).start()
    for chunk in range(1, n_chunks):
        x_copy(chunk).start()
    for j in range(6):
        weight_copy(1, j).start()
    for b in range(lens.shape[0]):
        lens[b:b + 1, :] = jnp.full((1, lens.shape[1]), lens_in[b], jnp.int32)
    angles = lens[:, 0:128].astype(F32) * inv_freq[...]
    odd = lax.rem(lax.broadcasted_iota(jnp.int32, angles.shape, 1), 2) == 1
    cos_c[...] = jnp.cos(angles)
    sin_c[...] = jnp.where(odd, jnp.sin(angles), -jnp.sin(angles))
    for src, dst in ((gain_in, gain), (bias_in, bias), (b_in_in, b_in), (b_out_in, b_out)):
        for layer in range(src.shape[0]):
            dst[layer] = src[layer:layer + 1, :].astype(F32)
    pl.semaphore_wait(barrier, 3)

    def norm_and_project(stage, layer, chunk):
        @pl.when(layer == 0)
        def _():
            x_copy(chunk).wait()

        group = 8

        @pl.loop(0, steps // group)
        def _(g):
            x = hid[chunk, pl.ds(g * group, group)].astype(F32)
            mean = jnp.mean(x, axis=-1, keepdims=True)
            centered = x - mean
            var = jnp.mean(centered * centered, axis=-1, keepdims=True)
            y = centered * lax.rsqrt(var + LN_EPS) * gain[layer][None] + bias[layer][None]
            normed[pl.ds(pl.multiple_of(g * group * SEQS, group * SEQS), group * SEQS), :] = y.reshape(group * SEQS, d_model).astype(BF16)

        @pl.when(chunk == 0)
        def _():
            for j in range(3):
                weight_copy(layer, j).wait()

        here = pl.ds(pl.multiple_of(chunk * SEQS, SEQS), SEQS)
        cc, sc = cos_c[here, :][None], sin_c[here, :][None]
        ct, st = cos_t[...], sin_t[...]
        cos = (cc * ct - sc * st).reshape(rows, 128)
        sin = (sc * ct + cc * st).reshape(rows, 128)
        even = lax.rem(lax.broadcasted_iota(jnp.int32, (rows, 128), 1), 2) == 0

        for weight, dst, rotate in ((wq, qf, True), (wk, kf, True), (wv, vf, False)):
            vec = jnp.dot(normed[...], weight[layer], preferred_element_type=F32)
            for h in range(2):
                piece = vec[:, h * 128:(h + 1) * 128]
                if rotate:
                    swapped = jnp.where(even, pltpu.roll(piece, 127, 1), pltpu.roll(piece, 1, 1))
                    piece = piece * cos + swapped * sin
                dst[h] = piece

    def attend(stage, layer, chunk):
        slot = lax.rem(stage, 2)
        for copy in kv_copies(stage):
            copy.wait()
        shape = (2 * steps, 2 * (OLD + steps))
        row, col = lax.broadcasted_iota(jnp.int32, shape, 0), lax.broadcasted_iota(jnp.int32, shape, 1)
        col_slot, col_head = lax.shift_right_logical(col, 1), lax.bitwise_and(col, 1)
        row_head, row_step = lax.div(row, steps), lax.rem(row, steps)
        never = 1 << 20
        fresh = jnp.where(col_slot - OLD <= row_step, -1, never)
        key = jnp.where(row_head == col_head, jnp.where(col_slot >= OLD, fresh, col_slot), never)
        here = pl.ds(pl.multiple_of(chunk * SEQS, SEQS), SEQS)
        limit = lens[here, :]
        for b in range(SEQS):
            mine = pl.ds(b, steps, stride=SEQS)
            for src, buf, j in ((kf, kbuf, 0), (vf, vbuf, 1)):
                for h in range(2):
                    inter[b, j, pl.ds(h, steps, stride=2), :] = src[h, mine, :]
                buf[slot, b, pl.ds(2 * OLD, 2 * steps), :] = inter[b, j].astype(BF16)
        for copy in rec_copies(stage):
            copy.start()
        for b in range(SEQS):
            mine = pl.ds(b, steps, stride=SEQS)
            query = jnp.concatenate([qf[0, mine, :], qf[1, mine, :]], axis=0).astype(BF16)
            s = lax.dot_general(query, kbuf[slot, b], (((1,), (1,)), ((), ())), preferred_element_type=F32) * (128 ** -0.5)
            scores[b] = jnp.where(key < limit[b:b + 1, :], s, -jnp.inf)
        for b in range(SEQS):
            s = scores[b]
            e = jnp.exp(s - jnp.max(s, axis=-1, keepdims=True))
            probs = (e * (1.0 / jnp.sum(e, axis=-1, keepdims=True))).astype(BF16)
            context = jnp.dot(probs, vbuf[slot, b], preferred_element_type=F32)
            for h in range(2):
                cf[h, pl.ds(b, steps, stride=SEQS), :] = context[h * steps:(h + 1) * steps]

    def feed_forward(layer, chunk):
        @pl.when(chunk == 0)
        def _():
            for j in range(3, 6):
                weight_copy(layer, j).wait()

        @pl.loop(0, act.shape[1] // 256, unroll=2)
        def _(n):
            cols = pl.ds(pl.multiple_of(n * 256, 256), 256)
            pre = jnp.dot(normed[...], win[layer, :, cols], preferred_element_type=F32) + b_in[layer, :, cols]
            act[:, cols] = jax.nn.gelu(pre, approximate=True).astype(BF16)

    def project_out(stage, layer):
        for h in range(2):
            ctx[:, h * 128:(h + 1) * 128] = cf[h].astype(BF16)

        @pl.loop(0, d_model // 256, unroll=2)
        def _(n):
            cols = pl.ds(pl.multiple_of(n * 256, 256), 256)
            total = jnp.dot(ctx[...], wo[layer, :, cols], preferred_element_type=F32)
            total += jnp.dot(act[...], wout[layer, :, cols], preferred_element_type=F32)
            part[:, :, cols] = total.reshape(steps, SEQS, 256).astype(BF16)

    def between(i, lag):
        return jnp.logical_and(i >= lag, i < n_stages + lag)

    @pl.loop(0, n_stages + 6)
    def _(i):
        layer, chunk = lax.div(i, n_chunks), lax.rem(i, n_chunks)
        live = i < n_stages

        @pl.when(live)
        def _():
            norm_and_project(i, layer, chunk)

        @pl.when(between(i, 5))
        def _():
            for j in range(2):
                phase3(i - 5, j).wait()
                phase4(i - 5, j).start()

        @pl.when(between(i, 6))
        def _():
            for j in range(2):
                phase4(i - 6, j).wait()
            phase5(i - 6).start()

        @pl.when(live)
        def _():
            @pl.when(i >= 1)
            def _():
                for copy in rec_copies(i - 1):
                    copy.wait()

            @pl.when(i + 1 < n_stages)
            def _():
                for copy in kv_copies(i + 1):
                    copy.start()

            attend(i, layer, chunk)

        @pl.when(between(i, 1))
        def _():
            s = i - 1
            phase0(s).wait()
            for j in range(2):
                @pl.loop(0, quarter // 4)
                def _(g):
                    ts = pl.ds(quarter * j + g * 4, 4)
                    sum0[lax.rem(s, 2), ts] = part[pl.ds(base + quarter * j + g * 4, 4)] + recv0[lax.rem(s, 2), ts]

                phase1(s, j).start()

        @pl.when(live)
        def _():
            feed_forward(layer, chunk)

        @pl.when(between(i, 2))
        def _():
            s = i - 2
            for j in range(2):
                phase1(s, j).wait()
                mine = pl.ds(quarter * j + eighth * pos1[j], eighth)
                ts = pl.ds(eighth * j, eighth)
                sum1[lax.rem(s, 2), ts] = sum0[lax.rem(s, 2), mine] + recv1[lax.rem(s, 4), ts]
                phase2(s, j).start()

        @pl.when(live)
        def _():
            project_out(i, layer)
            phase0(i).start()

        @pl.when(between(i, 3))
        def _():
            s = i - 3
            where = lax.rem(s, n_chunks)
            for j in range(2):
                phase2(s, j).wait()
                own = pl.ds(base2[j], last)
                total = sum1[lax.rem(s, 2), pl.ds(eighth * j + last * pos2[j], last)].astype(F32) + recv2[lax.rem(s, 4), pl.ds(last * j, last)].astype(F32)
                total = total + hid[where, own].astype(F32) + b_out[lax.div(s, n_chunks)][None]
                hid[where, own] = total.astype(BF16)
                phase3(s, j).start()

        @pl.when(between(i, 6))
        def _():
            s = i - 6
            phase5(s).wait()

            @pl.when(s >= n_stages - n_chunks)
            def _():
                out_copy(lax.rem(s, n_chunks)).start()

    for copy in rec_copies(n_stages - 1):
        copy.wait()
    for chunk in range(n_chunks):
        out_copy(chunk).wait()


def merge_kernel(n_blocks, lens, hid_in, k_hbm, v_hbm, rec_k, rec_v, hid_out, k_out, v_out, hbuf, kbuf, vbuf, rk, rv, in_sem, out_sem):
    size = kbuf.shape[0] // n_blocks
    steps = rk.shape[1]

    def block(ref, i):
        rows = ref.shape[0] // n_blocks
        return ref.at[pl.ds(i * rows, rows)]

    def loads(i):
        pairs = ((k_hbm, kbuf), (v_hbm, vbuf), (rec_k, rk), (rec_v, rv), (hid_in, hbuf))
        return [pltpu.make_async_copy(block(src, i), block(dst, i), in_sem.at[j, i]) for j, (src, dst) in enumerate(pairs)]

    def stores(i):
        pairs = ((kbuf, k_out), (vbuf, v_out), (hbuf, hid_out))
        return [pltpu.make_async_copy(block(src, i), block(dst, i), out_sem.at[j, i]) for j, (src, dst) in enumerate(pairs)]

    for i in range(n_blocks):
        for copy in loads(i):
            copy.start()

    @pl.loop(0, n_blocks)
    def _(i):
        for copy in loads(i):
            copy.wait()
        for b in range(size):
            row = i * size + b
            at = lens[lax.rem(row, lens.shape[0])]
            kbuf[row, pl.ds(at, steps)] = rk[row]
            vbuf[row, pl.ds(at, steps)] = rv[row]
        for copy in stores(i):
            copy.start()

    for i in range(n_blocks):
        for copy in stores(i):
            copy.wait()


def inverse_frequencies():
    lane = np.arange(128)
    return np.where(lane < ROT_DIM, 1.0 / (10000.0 ** ((lane // 2 * 2) / ROT_DIM)), 0.0)


def decode_shard(x_steps, cur_len, k_cache, v_cache, ln_gain, ln_bias, w_q, w_k, w_v, w_o, w_in, b_in, w_out, b_out):
    n_layers, batch, cache_len, n_heads, head_dim = k_cache.shape
    steps, _, d_model = x_steps.shape
    ff = w_in.shape[2]
    n_chunks = batch // SEQS
    n_stages = n_layers * n_chunks
    rows = steps * SEQS
    flat = (n_layers, batch, cache_len * n_heads, head_dim)
    step_angles = np.arange(steps)[:, None] * inverse_frequencies()[None, :]
    signed = np.where(np.arange(128) % 2 == 0, -1.0, 1.0)
    cos_t, sin_t = (np.repeat(tab.astype(np.float32)[:, None, :], SEQS, axis=1) for tab in (np.cos(step_angles), np.sin(step_angles) * signed))
    inv_freq = inverse_frequencies().astype(np.float32)[None, :]
    any_spec, vmem = pl.BlockSpec(memory_space=pl.ANY), pl.BlockSpec(memory_space=pltpu.VMEM)
    dma = pltpu.SemaphoreType.DMA
    block = (steps, SEQS, d_model)
    hidden, rec_k, rec_v = pl.pallas_call(
        functools.partial(decode_kernel, n_chunks, n_stages),
        out_shape=(jax.ShapeDtypeStruct(x_steps.shape, BF16),
                   jax.ShapeDtypeStruct((n_layers, batch, steps * n_heads, head_dim), BF16),
                   jax.ShapeDtypeStruct((n_layers, batch, steps * n_heads, head_dim), BF16)),
        in_specs=[any_spec] * 9 + [pl.BlockSpec(memory_space=pltpu.SMEM)] + [vmem] * 7,
        out_specs=(any_spec,) * 3,
        scratch_shapes=[
            pltpu.VMEM(w_q.shape, BF16), pltpu.VMEM(w_k.shape, BF16), pltpu.VMEM(w_v.shape, BF16), pltpu.VMEM(w_o.shape, BF16),
            pltpu.VMEM(w_in.shape, BF16), pltpu.VMEM(w_out.shape, BF16),
            pltpu.VMEM((n_chunks,) + block, BF16), pltpu.VMEM(block, BF16),
            pltpu.VMEM((2, steps // 2, SEQS, d_model), BF16), pltpu.VMEM((2, steps // 2, SEQS, d_model), BF16),
            pltpu.VMEM((4, steps // 4, SEQS, d_model), BF16), pltpu.VMEM((2, steps // 4, SEQS, d_model), BF16),
            pltpu.VMEM((4, steps // 8, SEQS, d_model), BF16),
            pltpu.VMEM((rows, d_model), BF16),
            pltpu.VMEM((2, rows, 128), F32), pltpu.VMEM((2, rows, 128), F32), pltpu.VMEM((2, rows, 128), F32), pltpu.VMEM((2, rows, 128), F32),
            pltpu.VMEM((rows, 256), BF16), pltpu.VMEM((rows, ff), BF16),
            pltpu.VMEM((SEQS, 2, 2 * steps, 128), F32), pltpu.VMEM((SEQS, 2 * steps, 256), F32),
            pltpu.VMEM((2, SEQS, 256, 128), BF16), pltpu.VMEM((2, SEQS, 256, 128), BF16),
            pltpu.VMEM((batch, cache_len * n_heads), jnp.int32), pltpu.VMEM((batch, 128), F32), pltpu.VMEM((batch, 128), F32),
            pltpu.VMEM((n_layers, 1, d_model), F32), pltpu.VMEM((n_layers, 1, d_model), F32),
            pltpu.VMEM((n_layers, 1, ff), F32), pltpu.VMEM((n_layers, 1, d_model), F32),
            dma((n_layers, 6)), dma((n_chunks,)), dma((2, 2)), dma((2, 2)), dma((n_chunks,)), dma((10, 2)), dma((10, 4)),
        ],
        compiler_params=pltpu.CompilerParams(collective_id=0, has_side_effects=True, vmem_limit_bytes=60 * 1024 * 1024),
        name="decode",
    )(x_steps, k_cache.reshape(flat), v_cache.reshape(flat), w_q, w_k, w_v, w_o, w_in, w_out,
      cur_len, inv_freq, cos_t, sin_t, ln_gain, ln_bias, b_in, b_out)

    pairs = n_layers * batch
    n_blocks = 16
    lines = (pairs, cache_len, n_heads, head_dim)
    new = (pairs, steps, n_heads, head_dim)
    hidden, k_out, v_out = pl.pallas_call(
        functools.partial(merge_kernel, n_blocks),
        out_shape=(jax.ShapeDtypeStruct(x_steps.shape, BF16),) + (jax.ShapeDtypeStruct(lines, BF16),) * 2,
        in_specs=[pl.BlockSpec(memory_space=pltpu.SMEM)] + [any_spec] * 5,
        out_specs=(any_spec,) * 3,
        scratch_shapes=[pltpu.VMEM(x_steps.shape, BF16), pltpu.VMEM(lines, BF16), pltpu.VMEM(lines, BF16),
                        pltpu.VMEM(new, BF16), pltpu.VMEM(new, BF16), dma((5, n_blocks)), dma((3, n_blocks))],
        compiler_params=pltpu.CompilerParams(vmem_limit_bytes=62 * 1024 * 1024),
        name="merge",
    )(cur_len, hidden, k_cache.reshape(lines), v_cache.reshape(lines), rec_k.reshape(new), rec_v.reshape(new))
    return hidden, k_out.reshape(k_cache.shape), v_out.reshape(v_cache.shape)


def solution(mesh):
    cache_spec = P(None, "dp", None, "tp", None)
    in_specs = (P(None, "dp", None), P("dp"), cache_spec, cache_spec, P(None, None), P(None, None),
                P(None, None, "tp"), P(None, None, "tp"), P(None, None, "tp"), P(None, "tp", None),
                P(None, None, "tp"), P(None, "tp"), P(None, "tp", None), P(None, None))
    out_specs = (P(None, "dp", None), cache_spec, cache_spec)
    return jax.shard_map(decode_shard, mesh=mesh, in_specs=in_specs, out_specs=out_specs, check_vma=False)
```

```python
import functools

import jax
import jax.numpy as jnp
import numpy as np
from jax import lax
from jax.experimental import pallas as pl
from jax.experimental.pallas import tpu as pltpu
from jax.sharding import PartitionSpec as P

ROT_DIM = 64
LN_EPS = 1e-5
MESH = pl.DeviceIdType.MESH
F32 = jnp.float32
BF16 = jnp.bfloat16
SEQS = 8
OLD = 96


def decode_kernel(n_chunks, n_stages, x_hbm, k_hbm, v_hbm, wq_hbm, wk_hbm, wv_hbm, wo_hbm, win_hbm, wout_hbm,
                  lens_in, inv_freq, cos_t, sin_t, gain_in, bias_in, b_in_in, b_out_in,
                  out_hbm, rec_k, rec_v,
                  wq, wk, wv, wo, win, wout, hid, part, recv0, sum0, recv1, sum1, recv2,
                  normed, qf, kf, vf, cf, ctx, act, inter, scores, key_scr, kbuf, vbuf,
                  lens, cos_c, sin_c, gain, bias, b_in, b_out,
                  w_sem, x_sem, kv_sem, rec_sem, out_sem, send_sem, recv_sem):
    steps = x_hbm.shape[0]
    rows = steps * SEQS
    ff = win_hbm.shape[2]
    half, quarter, eighth, last = steps // 2, steps // 4, steps // 8, steps // 16
    d_model = x_hbm.shape[2]
    me = lax.axis_index("tp")
    core = lax.rem(me, 2)
    px = lax.rem(lax.div(me, 2), 2)
    py = lax.div(me, 4)
    partner = me + 1 - 2 * core
    x_peer = me + 2 * (1 - 2 * px)
    y_peer = me + 4 * (1 - 2 * py)
    first, second = (x_peer, y_peer), (y_peer, x_peer)
    pos1, pos2 = (px, py), (py, px)
    base = half * core
    base1 = [base + quarter * j + eighth * pos1[j] for j in range(2)]
    base2 = [base1[j] + last * pos2[j] for j in range(2)]

    weight_pairs = ((wq_hbm, wq), (wk_hbm, wk), (wv_hbm, wv), (win_hbm, win), (wo_hbm, wo), (wout_hbm, wout))

    def weight_copy(layer, j):
        src, dst = weight_pairs[j]
        return pltpu.make_async_copy(src.at[layer], dst.at[layer], w_sem.at[layer, j])

    def x_copy(chunk):
        return pltpu.make_async_copy(x_hbm.at[:, pl.ds(pl.multiple_of(chunk * SEQS, SEQS), SEQS), :], hid.at[chunk], x_sem.at[chunk])

    def out_copy(chunk):
        return pltpu.make_async_copy(hid.at[chunk], out_hbm.at[:, pl.ds(pl.multiple_of(chunk * SEQS, SEQS), SEQS), :], out_sem.at[chunk])

    def kv_copies(stage):
        layer, chunk, slot = lax.div(stage, n_chunks), lax.rem(stage, n_chunks), lax.rem(stage, 2)
        seqs = pl.ds(chunk * SEQS, SEQS)
        return (pltpu.make_async_copy(k_hbm.at[layer, seqs], kbuf.at[slot], kv_sem.at[0, slot]),
                pltpu.make_async_copy(v_hbm.at[layer, seqs], vbuf.at[slot], kv_sem.at[1, slot]))

    def rec_copies(stage):
        layer, chunk, slot = lax.div(stage, n_chunks), lax.rem(stage, n_chunks), lax.rem(stage, 2)
        seqs = pl.ds(chunk * SEQS, SEQS)
        new = pl.ds(2 * OLD, 2 * steps)
        return (pltpu.make_async_copy(kbuf.at[slot, :, new, :], rec_k.at[layer, seqs], rec_sem.at[0, slot]),
                pltpu.make_async_copy(vbuf.at[slot, :, new, :], rec_v.at[layer, seqs], rec_sem.at[1, slot]))

    def remote(kind, stage, src, dst, peer):
        return pltpu.make_async_remote_copy(src_ref=src, dst_ref=dst, send_sem=send_sem.at[kind, lax.rem(stage, 2)],
                                            recv_sem=recv_sem.at[kind, lax.rem(stage, 4)], device_id={"tp": peer}, device_id_type=MESH)

    def phase0(stage):
        return remote(0, stage, part.at[pl.ds(half - base, half)], recv0.at[lax.rem(stage, 2)], partner)

    def phase1(stage, j):
        block = pl.ds(quarter * j + eighth * (1 - pos1[j]), eighth)
        return remote(1 + j, stage, sum0.at[lax.rem(stage, 2), block], recv1.at[lax.rem(stage, 4), pl.ds(eighth * j, eighth)], first[j])

    def phase2(stage, j):
        block = pl.ds(eighth * j + last * (1 - pos2[j]), last)
        return remote(3 + j, stage, sum1.at[lax.rem(stage, 2), block], recv2.at[lax.rem(stage, 4), pl.ds(last * j, last)], second[j])

    def gather(kind, stage, start, size, peer):
        block = hid.at[lax.rem(stage, n_chunks), pl.ds(start, size)]
        return remote(kind, stage, block, block, peer)

    def phase3(stage, j):
        return gather(5 + j, stage, base2[j], last, second[j])

    def phase4(stage, j):
        return gather(7 + j, stage, base1[j], eighth, first[j])

    def phase5(stage):
        return gather(9, stage, base, half, partner)

    barrier = pltpu.get_barrier_semaphore()
    for peer in (partner, x_peer, y_peer):
        pl.semaphore_signal(barrier, inc=1, device_id={"tp": peer}, device_id_type=MESH)
    x_copy(0).start()
    for j in range(3):
        weight_copy(0, j).start()
    for copy in kv_copies(0):
        copy.start()
    for j in range(3, 6):
        weight_copy(0, j).start()
    for chunk in range(1, n_chunks):
        x_copy(chunk).start()
    for j in range(6):
        weight_copy(1, j).start()
    for b in range(lens.shape[0]):
        lens[b:b + 1, :] = jnp.full((1, lens.shape[1]), lens_in[b], jnp.int32)
    angles = lens[:, 0:128].astype(F32) * inv_freq[...]
    odd = lax.rem(lax.broadcasted_iota(jnp.int32, angles.shape, 1), 2) == 1
    cos_c[...] = jnp.cos(angles)
    sin_c[...] = jnp.where(odd, jnp.sin(angles), -jnp.sin(angles))
    for src, dst in ((gain_in, gain), (bias_in, bias), (b_in_in, b_in), (b_out_in, b_out)):
        for layer in range(src.shape[0]):
            dst[layer] = src[layer:layer + 1, :].astype(F32)
    pl.semaphore_wait(barrier, 3)

    def norm_rows(stage, start, count):
        layer, chunk, slot = lax.div(stage, n_chunks), lax.rem(stage, n_chunks), lax.rem(stage, 2)
        for k in range(0, count, 2):
            x = hid[chunk, pl.ds(start + k, 2)].astype(F32)
            centered = x - jnp.mean(x, axis=-1, keepdims=True)
            var = jnp.mean(centered * centered, axis=-1, keepdims=True)
            y = centered * lax.rsqrt(var + LN_EPS) * gain[layer][None] + bias[layer][None]
            normed[slot, pl.ds((start + k) * SEQS if isinstance(start, int) else pl.multiple_of((start + k) * SEQS, 2 * SEQS), 2 * SEQS), pl.ds(0, d_model)] = y.reshape(2 * SEQS, d_model).astype(BF16)

    def project_in(stage, layer, chunk):
        @pl.when(chunk == 0)
        def _():
            for j in range(3):
                weight_copy(layer, j).wait()

        here = pl.ds(pl.multiple_of(chunk * SEQS, SEQS), SEQS)
        cc, sc = cos_c[here, :][None], sin_c[here, :][None]
        ct, st = cos_t[...], sin_t[...]
        cos = (cc * ct - sc * st).reshape(rows, 128)
        sin = (sc * ct + cc * st).reshape(rows, 128)
        even = lax.rem(lax.broadcasted_iota(jnp.int32, (rows, 128), 1), 2) == 0

        for weight, dst, rotate in ((wq, qf, True), (wk, kf, True), (wv, vf, False)):
            vec = jnp.dot(normed[lax.rem(stage, 2), :, pl.ds(0, d_model)], weight[layer], preferred_element_type=F32)
            for h in range(2):
                piece = vec[:, h * 128:(h + 1) * 128]
                if rotate:
                    swapped = jnp.where(even, pltpu.roll(piece, 127, 1), pltpu.roll(piece, 1, 1))
                    piece = piece * cos + swapped * sin
                dst[h] = piece

    def attend(stage, layer, chunk):
        slot = lax.rem(stage, 2)
        for copy in kv_copies(stage):
            copy.wait()

        @pl.when(chunk == 0)
        def _():
            for j in range(3, 6):
                weight_copy(layer, j).wait()

        shape = (2 * steps, 2 * (OLD + steps))
        row, col = lax.broadcasted_iota(jnp.int32, shape, 0), lax.broadcasted_iota(jnp.int32, shape, 1)
        col_slot, col_head = lax.shift_right_logical(col, 1), lax.bitwise_and(col, 1)
        row_head, row_step = lax.div(row, steps), lax.rem(row, steps)
        never = 1 << 20
        fresh = jnp.where(col_slot - OLD <= row_step, -1, never)
        key_scr[...] = jnp.where(row_head == col_head, jnp.where(col_slot >= OLD, fresh, col_slot), never)
        limit = lens[pl.ds(pl.multiple_of(chunk * SEQS, SEQS), SEQS), :]
        for b in range(SEQS):
            mine = pl.ds(b, steps, stride=SEQS)
            for src, buf, j in ((kf, kbuf, 0), (vf, vbuf, 1)):
                for h in range(2):
                    inter[b, j, pl.ds(h, steps, stride=2), :] = src[h, mine, :]
                buf[slot, b, pl.ds(2 * OLD, 2 * steps), :] = inter[b, j].astype(BF16)
        for b in range(SEQS):
            mine = pl.ds(b, steps, stride=SEQS)
            query = jnp.concatenate([qf[0, mine, :], qf[1, mine, :]], axis=0).astype(BF16)
            s = lax.dot_general(query, kbuf[slot, b], (((1,), (1,)), ((), ())), preferred_element_type=F32) * (128 ** -0.5)
            scores[b] = jnp.where(key_scr[...] < limit[b:b + 1, :], s, -jnp.inf)
        for b in range(SEQS):
            s = scores[b]
            e = jnp.exp(s - jnp.max(s, axis=-1, keepdims=True))
            probs = (e * (1.0 / jnp.sum(e, axis=-1, keepdims=True))).astype(BF16)
            context = jnp.dot(probs, vbuf[slot, b], preferred_element_type=F32)
            for h in range(2):
                cf[h, pl.ds(b, steps, stride=SEQS), :] = context[h * steps:(h + 1) * steps]

        for copy in rec_copies(stage):
            copy.start()

    def feed_forward(stage, layer):
        slot = lax.rem(stage, 2)
        for n in range(ff // 256):
            cols = pl.ds(n * 256, 256)
            pre = jnp.dot(normed[slot, :, pl.ds(0, d_model)], win[layer, :, cols], preferred_element_type=F32) + b_in[layer, :, cols]
            act[:, cols] = jax.nn.gelu(pre, approximate=True).astype(BF16)

    def project_out(stage, layer):
        for h in range(2):
            ctx[:, h * 128:(h + 1) * 128] = cf[h].astype(BF16)

        following = jnp.minimum(stage + 1, n_stages - 1)
        group = steps // (d_model // 256)

        @pl.when(stage + 1 < n_chunks)
        def _():
            x_copy(stage + 1).wait()

        for n in range(d_model // 256):
            cols = pl.ds(n * 256, 256)
            total = jnp.dot(ctx[...], wo[layer, :, cols], preferred_element_type=F32)
            total += jnp.dot(act[:, pl.ds(0, ff)], wout[layer, :, cols], preferred_element_type=F32)
            part[:, :, cols] = total.reshape(steps, SEQS, 256).astype(BF16)
            norm_rows(following, n * group, group)

    x_copy(0).wait()

    @pl.loop(0, steps // 8)
    def _(g):
        norm_rows(0, g * 8, 8)

    def between(i, lag):
        return jnp.logical_and(i >= lag, i < n_stages + lag)

    @pl.loop(0, n_stages + 6)
    def _(i):
        layer, chunk = lax.div(i, n_chunks), lax.rem(i, n_chunks)
        live = i < n_stages

        @pl.when(live)
        def _():
            project_in(i, layer, chunk)

        @pl.when(between(i, 5))
        def _():
            for j in range(2):
                phase3(i - 5, j).wait()
                phase4(i - 5, j).start()

        @pl.when(between(i, 6))
        def _():
            for j in range(2):
                phase4(i - 6, j).wait()
            phase5(i - 6).start()

        @pl.when(live)
        def _():
            @pl.when(i >= 1)
            def _():
                for copy in rec_copies(i - 1):
                    copy.wait()

            @pl.when(i + 1 < n_stages)
            def _():
                for copy in kv_copies(i + 1):
                    copy.start()

            attend(i, layer, chunk)

        @pl.when(between(i, 1))
        def _():
            s = i - 1
            phase0(s).wait()
            for j in range(2):
                @pl.loop(0, quarter // 4)
                def _(g):
                    ts = pl.ds(quarter * j + g * 4, 4)
                    sum0[lax.rem(s, 2), ts] = part[pl.ds(base + quarter * j + g * 4, 4)] + recv0[lax.rem(s, 2), ts]

                phase1(s, j).start()

        @pl.when(live)
        def _():
            feed_forward(i, layer)

        @pl.when(between(i, 2))
        def _():
            s = i - 2
            for j in range(2):
                phase1(s, j).wait()
                mine = pl.ds(quarter * j + eighth * pos1[j], eighth)
                ts = pl.ds(eighth * j, eighth)
                sum1[lax.rem(s, 2), ts] = sum0[lax.rem(s, 2), mine] + recv1[lax.rem(s, 4), ts]
                phase2(s, j).start()

        @pl.when(live)
        def _():
            project_out(i, layer)
            phase0(i).start()

        @pl.when(between(i, 3))
        def _():
            s = i - 3
            where = lax.rem(s, n_chunks)
            for j in range(2):
                phase2(s, j).wait()
                own = pl.ds(base2[j], last)
                total = sum1[lax.rem(s, 2), pl.ds(eighth * j + last * pos2[j], last)].astype(F32) + recv2[lax.rem(s, 4), pl.ds(last * j, last)].astype(F32)
                total = total + hid[where, own].astype(F32) + b_out[lax.div(s, n_chunks)][None]
                hid[where, own] = total.astype(BF16)
                phase3(s, j).start()

        @pl.when(between(i, 6))
        def _():
            s = i - 6
            phase5(s).wait()

            @pl.when(s >= n_stages - n_chunks)
            def _():
                out_copy(lax.rem(s, n_chunks)).start()

    for copy in rec_copies(n_stages - 1):
        copy.wait()
    for chunk in range(n_chunks):
        out_copy(chunk).wait()


def merge_kernel(n_blocks, lens, hid_in, k_hbm, v_hbm, rec_k, rec_v, hid_out, k_out, v_out, hbuf, kbuf, vbuf, rk, rv, in_sem, out_sem):
    size = kbuf.shape[0] // n_blocks
    steps = rk.shape[1]

    def block(ref, i):
        rows = ref.shape[0] // n_blocks
        return ref.at[pl.ds(i * rows, rows)]

    def loads(i):
        pairs = ((k_hbm, kbuf), (v_hbm, vbuf), (rec_k, rk), (rec_v, rv), (hid_in, hbuf))
        return [pltpu.make_async_copy(block(src, i), block(dst, i), in_sem.at[j, i]) for j, (src, dst) in enumerate(pairs)]

    def stores(i):
        pairs = ((kbuf, k_out), (vbuf, v_out), (hbuf, hid_out))
        return [pltpu.make_async_copy(block(src, i), block(dst, i), out_sem.at[j, i]) for j, (src, dst) in enumerate(pairs)]

    for i in range(n_blocks):
        for copy in loads(i):
            copy.start()

    @pl.loop(0, n_blocks)
    def _(i):
        for copy in loads(i):
            copy.wait()
        for b in range(size):
            row = i * size + b
            at = lens[lax.rem(row, lens.shape[0])]
            kbuf[row, pl.ds(at, steps)] = rk[row]
            vbuf[row, pl.ds(at, steps)] = rv[row]
        for copy in stores(i):
            copy.start()

    for i in range(n_blocks):
        for copy in stores(i):
            copy.wait()


def inverse_frequencies():
    lane = np.arange(128)
    return np.where(lane < ROT_DIM, 1.0 / (10000.0 ** ((lane // 2 * 2) / ROT_DIM)), 0.0)


def decode_shard(x_steps, cur_len, k_cache, v_cache, ln_gain, ln_bias, w_q, w_k, w_v, w_o, w_in, b_in, w_out, b_out):
    n_layers, batch, cache_len, n_heads, head_dim = k_cache.shape
    steps, _, d_model = x_steps.shape
    ff = w_in.shape[2]
    n_chunks = batch // SEQS
    n_stages = n_layers * n_chunks
    rows = steps * SEQS
    flat = (n_layers, batch, cache_len * n_heads, head_dim)
    step_angles = np.arange(steps)[:, None] * inverse_frequencies()[None, :]
    signed = np.where(np.arange(128) % 2 == 0, -1.0, 1.0)
    cos_t, sin_t = (np.repeat(tab.astype(np.float32)[:, None, :], SEQS, axis=1) for tab in (np.cos(step_angles), np.sin(step_angles) * signed))
    inv_freq = inverse_frequencies().astype(np.float32)[None, :]
    any_spec, vmem = pl.BlockSpec(memory_space=pl.ANY), pl.BlockSpec(memory_space=pltpu.VMEM)
    dma = pltpu.SemaphoreType.DMA
    block = (steps, SEQS, d_model)
    hidden, rec_k, rec_v = pl.pallas_call(
        functools.partial(decode_kernel, n_chunks, n_stages),
        out_shape=(jax.ShapeDtypeStruct(x_steps.shape, BF16),
                   jax.ShapeDtypeStruct((n_layers, batch, steps * n_heads, head_dim), BF16),
                   jax.ShapeDtypeStruct((n_layers, batch, steps * n_heads, head_dim), BF16)),
        in_specs=[any_spec] * 9 + [pl.BlockSpec(memory_space=pltpu.SMEM)] + [vmem] * 7,
        out_specs=(any_spec,) * 3,
        scratch_shapes=[
            pltpu.VMEM(w_q.shape, BF16), pltpu.VMEM(w_k.shape, BF16), pltpu.VMEM(w_v.shape, BF16), pltpu.VMEM(w_o.shape, BF16),
            pltpu.VMEM(w_in.shape, BF16), pltpu.VMEM(w_out.shape, BF16),
            pltpu.VMEM((n_chunks,) + block, BF16), pltpu.VMEM(block, BF16),
            pltpu.VMEM((2, steps // 2, SEQS, d_model), BF16), pltpu.VMEM((2, steps // 2, SEQS, d_model), BF16),
            pltpu.VMEM((4, steps // 4, SEQS, d_model), BF16), pltpu.VMEM((2, steps // 4, SEQS, d_model), BF16),
            pltpu.VMEM((4, steps // 8, SEQS, d_model), BF16),
            pltpu.VMEM((2, rows, d_model + 128), BF16),
            pltpu.VMEM((2, rows, 128), F32), pltpu.VMEM((2, rows, 128), F32), pltpu.VMEM((2, rows, 128), F32), pltpu.VMEM((2, rows, 128), F32),
            pltpu.VMEM((rows, 256), BF16), pltpu.VMEM((rows, ff + 128), BF16),
            pltpu.VMEM((SEQS, 2, 2 * steps, 128), F32), pltpu.VMEM((SEQS, 2 * steps, 256), F32), pltpu.VMEM((2 * steps, 256), jnp.int32),
            pltpu.VMEM((2, SEQS, 256, 128), BF16), pltpu.VMEM((2, SEQS, 256, 128), BF16),
            pltpu.VMEM((batch, cache_len * n_heads), jnp.int32), pltpu.VMEM((batch, 128), F32), pltpu.VMEM((batch, 128), F32),
            pltpu.VMEM((n_layers, 1, d_model), F32), pltpu.VMEM((n_layers, 1, d_model), F32),
            pltpu.VMEM((n_layers, 1, ff), F32), pltpu.VMEM((n_layers, 1, d_model), F32),
            dma((n_layers, 6)), dma((n_chunks,)), dma((2, 2)), dma((2, 2)), dma((n_chunks,)), dma((10, 2)), dma((10, 4)),
        ],
        compiler_params=pltpu.CompilerParams(collective_id=0, has_side_effects=True, vmem_limit_bytes=60 * 1024 * 1024),
        name="decode",
    )(x_steps, k_cache.reshape(flat), v_cache.reshape(flat), w_q, w_k, w_v, w_o, w_in, w_out,
      cur_len, inv_freq, cos_t, sin_t, ln_gain, ln_bias, b_in, b_out)

    pairs = n_layers * batch
    n_blocks = 16
    lines = (pairs, cache_len, n_heads, head_dim)
    new = (pairs, steps, n_heads, head_dim)
    hidden, k_out, v_out = pl.pallas_call(
        functools.partial(merge_kernel, n_blocks),
        out_shape=(jax.ShapeDtypeStruct(x_steps.shape, BF16),) + (jax.ShapeDtypeStruct(lines, BF16),) * 2,
        in_specs=[pl.BlockSpec(memory_space=pltpu.SMEM)] + [any_spec] * 5,
        out_specs=(any_spec,) * 3,
        scratch_shapes=[pltpu.VMEM(x_steps.shape, BF16), pltpu.VMEM(lines, BF16), pltpu.VMEM(lines, BF16),
                        pltpu.VMEM(new, BF16), pltpu.VMEM(new, BF16), dma((5, n_blocks)), dma((3, n_blocks))],
        compiler_params=pltpu.CompilerParams(vmem_limit_bytes=62 * 1024 * 1024),
        name="merge",
    )(cur_len, hidden, k_cache.reshape(lines), v_cache.reshape(lines), rec_k.reshape(new), rec_v.reshape(new))
    return hidden, k_out.reshape(k_cache.shape), v_out.reshape(v_cache.shape)


def solution(mesh):
    cache_spec = P(None, "dp", None, "tp", None)
    in_specs = (P(None, "dp", None), P("dp"), cache_spec, cache_spec, P(None, None), P(None, None),
                P(None, None, "tp"), P(None, None, "tp"), P(None, None, "tp"), P(None, "tp", None),
                P(None, None, "tp"), P(None, "tp"), P(None, "tp", None), P(None, None))
    out_specs = (P(None, "dp", None), cache_spec, cache_spec)
    return jax.shard_map(decode_shard, mesh=mesh, in_specs=in_specs, out_specs=out_specs, check_vma=False)
```

```python
import functools

import jax
import jax.numpy as jnp
import numpy as np
from jax import lax
from jax.experimental import pallas as pl
from jax.experimental.pallas import tpu as pltpu
from jax.sharding import PartitionSpec as P

ROT_DIM = 64
LN_EPS = 1e-5
MESH = pl.DeviceIdType.MESH
F32 = jnp.float32
BF16 = jnp.bfloat16
SEQS = 8
OLD = 96


def decode_kernel(n_chunks, n_stages, x_hbm, k_hbm, v_hbm, wq_hbm, wk_hbm, wv_hbm, wo_hbm, win_hbm, wout_hbm,
                  lens_in, inv_freq, cos_t, sin_t, gain_in, bias_in, b_in_in, b_out_in,
                  out_hbm, rec_k, rec_v,
                  wq, wk, wv, wo, win, wout, hid, part, recv0, sum0, recv1, sum1, recv2,
                  normed, qf, kf, vf, cf, ctx, act, inter, scores, key_scr, kbuf, vbuf,
                  lens, cos_c, sin_c, gain, bias, b_in, b_out,
                  w_sem, x_sem, kv_sem, rec_sem, out_sem, send_sem, recv_sem):
    steps = x_hbm.shape[0]
    rows = steps * SEQS
    ff = win_hbm.shape[2]
    half, quarter, eighth, last = steps // 2, steps // 4, steps // 8, steps // 16
    d_model = x_hbm.shape[2]
    me = lax.axis_index("tp")
    core = lax.rem(me, 2)
    px = lax.rem(lax.div(me, 2), 2)
    py = lax.div(me, 4)
    partner = me + 1 - 2 * core
    x_peer = me + 2 * (1 - 2 * px)
    y_peer = me + 4 * (1 - 2 * py)
    first, second = (x_peer, y_peer), (y_peer, x_peer)
    pos1, pos2 = (px, py), (py, px)
    base = half * core
    base1 = [base + quarter * j + eighth * pos1[j] for j in range(2)]
    base2 = [base1[j] + last * pos2[j] for j in range(2)]

    weight_pairs = ((wq_hbm, wq), (wk_hbm, wk), (wv_hbm, wv), (win_hbm, win), (wo_hbm, wo), (wout_hbm, wout))

    def weight_copy(layer, j):
        src, dst = weight_pairs[j]
        return pltpu.make_async_copy(src.at[layer], dst.at[layer], w_sem.at[layer, j])

    def x_copy(chunk):
        return pltpu.make_async_copy(x_hbm.at[:, pl.ds(pl.multiple_of(chunk * SEQS, SEQS), SEQS), :], hid.at[chunk], x_sem.at[chunk])

    def out_copy(chunk):
        return pltpu.make_async_copy(hid.at[chunk], out_hbm.at[:, pl.ds(pl.multiple_of(chunk * SEQS, SEQS), SEQS), :], out_sem.at[chunk])

    def kv_copies(stage):
        layer, chunk, slot = lax.div(stage, n_chunks), lax.rem(stage, n_chunks), lax.rem(stage, 2)
        seqs = pl.ds(chunk * SEQS, SEQS)
        return (pltpu.make_async_copy(k_hbm.at[layer, seqs], kbuf.at[slot], kv_sem.at[0, slot]),
                pltpu.make_async_copy(v_hbm.at[layer, seqs], vbuf.at[slot], kv_sem.at[1, slot]))

    def rec_copies(stage):
        layer, chunk, slot = lax.div(stage, n_chunks), lax.rem(stage, n_chunks), lax.rem(stage, 2)
        seqs = pl.ds(chunk * SEQS, SEQS)
        new = pl.ds(2 * OLD, 2 * steps)
        return (pltpu.make_async_copy(kbuf.at[slot, :, new, :], rec_k.at[layer, seqs], rec_sem.at[0, slot]),
                pltpu.make_async_copy(vbuf.at[slot, :, new, :], rec_v.at[layer, seqs], rec_sem.at[1, slot]))

    def remote(kind, stage, src, dst, peer):
        return pltpu.make_async_remote_copy(src_ref=src, dst_ref=dst, send_sem=send_sem.at[kind, lax.rem(stage, 2)],
                                            recv_sem=recv_sem.at[kind, lax.rem(stage, 4)], device_id={"tp": peer}, device_id_type=MESH)

    def phase0(stage):
        return remote(0, stage, part.at[pl.ds(half - base, half)], recv0.at[lax.rem(stage, 2)], partner)

    def phase1(stage, j):
        block = pl.ds(quarter * j + eighth * (1 - pos1[j]), eighth)
        return remote(1 + j, stage, sum0.at[lax.rem(stage, 2), block], recv1.at[lax.rem(stage, 4), pl.ds(eighth * j, eighth)], first[j])

    def phase2(stage, j):
        block = pl.ds(eighth * j + last * (1 - pos2[j]), last)
        return remote(3 + j, stage, sum1.at[lax.rem(stage, 2), block], recv2.at[lax.rem(stage, 4), pl.ds(last * j, last)], second[j])

    def gather(kind, stage, start, size, peer):
        block = hid.at[lax.rem(stage, n_chunks), pl.ds(start, size)]
        return remote(kind, stage, block, block, peer)

    def phase3(stage, j):
        return gather(5 + j, stage, base2[j], last, second[j])

    def phase4(stage, j):
        return gather(7 + j, stage, base1[j], eighth, first[j])

    def phase5(stage):
        return gather(9, stage, base, half, partner)

    barrier = pltpu.get_barrier_semaphore()
    for peer in (partner, x_peer, y_peer):
        pl.semaphore_signal(barrier, inc=1, device_id={"tp": peer}, device_id_type=MESH)
    x_copy(0).start()
    for j in range(3):
        weight_copy(0, j).start()
    for copy in kv_copies(0):
        copy.start()
    for j in range(3, 6):
        weight_copy(0, j).start()
    x_copy(1).start()
    for b in range(lens.shape[0]):
        lens[b:b + 1, :] = jnp.full((1, lens.shape[1]), lens_in[b], jnp.int32)
    angles = lens[:, 0:128].astype(F32) * inv_freq[...]
    odd = lax.rem(lax.broadcasted_iota(jnp.int32, angles.shape, 1), 2) == 1
    cos_c[...] = jnp.cos(angles)
    sin_c[...] = jnp.where(odd, jnp.sin(angles), -jnp.sin(angles))
    for src, dst in ((gain_in, gain), (bias_in, bias), (b_in_in, b_in), (b_out_in, b_out)):
        for layer in range(src.shape[0]):
            dst[layer] = src[layer:layer + 1, :].astype(F32)

    def norm_rows(stage, start, count):
        layer, chunk, slot = lax.div(stage, n_chunks), lax.rem(stage, n_chunks), lax.rem(stage, 2)
        for k in range(0, count, 2):
            x = hid[chunk, pl.ds(start + k, 2)].astype(F32)
            centered = x - jnp.mean(x, axis=-1, keepdims=True)
            var = jnp.mean(centered * centered, axis=-1, keepdims=True)
            y = centered * lax.rsqrt(var + LN_EPS) * gain[layer][None] + bias[layer][None]
            normed[slot, pl.ds((start + k) * SEQS if isinstance(start, int) else pl.multiple_of((start + k) * SEQS, 2 * SEQS), 2 * SEQS), pl.ds(0, d_model)] = y.reshape(2 * SEQS, d_model).astype(BF16)

    def project_in(stage, layer, chunk):
        @pl.when(chunk == 0)
        def _():
            for j in range(3):
                weight_copy(layer, j).wait()

        here = pl.ds(pl.multiple_of(chunk * SEQS, SEQS), SEQS)
        cc, sc = cos_c[here, :][None], sin_c[here, :][None]
        ct, st = cos_t[...], sin_t[...]
        cos = (cc * ct - sc * st).reshape(rows, 128)
        sin = (sc * ct + cc * st).reshape(rows, 128)
        even = lax.rem(lax.broadcasted_iota(jnp.int32, (rows, 128), 1), 2) == 0

        for weight, dst, rotate in ((wq, qf, True), (wk, kf, True), (wv, vf, False)):
            vec = jnp.dot(normed[lax.rem(stage, 2), :, pl.ds(0, d_model)], weight[layer], preferred_element_type=F32)
            for h in range(2):
                piece = vec[:, h * 128:(h + 1) * 128]
                if rotate:
                    swapped = jnp.where(even, pltpu.roll(piece, 127, 1), pltpu.roll(piece, 1, 1))
                    piece = piece * cos + swapped * sin
                dst[h] = piece

    def attend(stage, layer, chunk):
        slot = lax.rem(stage, 2)
        for copy in kv_copies(stage):
            copy.wait()

        @pl.when(chunk == 0)
        def _():
            for j in range(3, 6):
                weight_copy(layer, j).wait()

        shape = (2 * steps, 2 * (OLD + steps))
        row, col = lax.broadcasted_iota(jnp.int32, shape, 0), lax.broadcasted_iota(jnp.int32, shape, 1)
        col_slot, col_head = lax.shift_right_logical(col, 1), lax.bitwise_and(col, 1)
        row_head, row_step = lax.div(row, steps), lax.rem(row, steps)
        never = 1 << 20
        fresh = jnp.where(col_slot - OLD <= row_step, -1, never)
        key_scr[...] = jnp.where(row_head == col_head, jnp.where(col_slot >= OLD, fresh, col_slot), never)
        limit = lens[pl.ds(pl.multiple_of(chunk * SEQS, SEQS), SEQS), :]
        for b in range(SEQS):
            mine = pl.ds(b, steps, stride=SEQS)
            for src, buf, j in ((kf, kbuf, 0), (vf, vbuf, 1)):
                for h in range(2):
                    inter[b, j, pl.ds(h, steps, stride=2), :] = src[h, mine, :]
                buf[slot, b, pl.ds(2 * OLD, 2 * steps), :] = inter[b, j].astype(BF16)
        for b in range(SEQS):
            mine = pl.ds(b, steps, stride=SEQS)
            query = jnp.concatenate([qf[0, mine, :], qf[1, mine, :]], axis=0).astype(BF16)
            s = lax.dot_general(query, kbuf[slot, b], (((1,), (1,)), ((), ())), preferred_element_type=F32) * (128 ** -0.5)
            scores[b] = jnp.where(key_scr[...] < limit[b:b + 1, :], s, -jnp.inf)
        for b in range(SEQS):
            s = scores[b]
            e = jnp.exp(s - jnp.max(s, axis=-1, keepdims=True))
            probs = (e * (1.0 / jnp.sum(e, axis=-1, keepdims=True))).astype(BF16)
            context = jnp.dot(probs, vbuf[slot, b], preferred_element_type=F32)
            for h in range(2):
                cf[h, pl.ds(b, steps, stride=SEQS), :] = context[h * steps:(h + 1) * steps]

        for copy in rec_copies(stage):
            copy.start()

    def feed_forward(stage, layer):
        slot = lax.rem(stage, 2)
        for n in range(ff // 256):
            cols = pl.ds(n * 256, 256)
            pre = jnp.dot(normed[slot, :, pl.ds(0, d_model)], win[layer, :, cols], preferred_element_type=F32) + b_in[layer, :, cols]
            act[:, cols] = jax.nn.gelu(pre, approximate=True).astype(BF16)

    def project_out(stage, layer):
        for h in range(2):
            ctx[:, h * 128:(h + 1) * 128] = cf[h].astype(BF16)

        following = jnp.minimum(stage + 1, n_stages - 1)
        group = steps // (d_model // 256)

        @pl.when(stage + 1 < n_chunks)
        def _():
            x_copy(stage + 1).wait()

        for n in range(d_model // 256):
            cols = pl.ds(n * 256, 256)
            total = jnp.dot(ctx[...], wo[layer, :, cols], preferred_element_type=F32)
            total += jnp.dot(act[:, pl.ds(0, ff)], wout[layer, :, cols], preferred_element_type=F32)
            part[:, :, cols] = total.reshape(steps, SEQS, 256).astype(BF16)
            norm_rows(following, n * group, group)

    x_copy(0).wait()

    @pl.loop(0, steps // 8)
    def _(g):
        norm_rows(0, g * 8, 8)

    pl.semaphore_wait(barrier, 3)

    def between(i, lag):
        return jnp.logical_and(i >= lag, i < n_stages + lag)

    @pl.loop(0, n_stages + 7)
    def _(i):
        layer, chunk = lax.div(i, n_chunks), lax.rem(i, n_chunks)
        live = i < n_stages

        @pl.when(i == 1)
        def _():
            for c in range(2, n_chunks):
                x_copy(c).start()
            for j in range(6):
                weight_copy(1, j).start()

        @pl.when(live)
        def _():
            project_in(i, layer, chunk)

        @pl.when(between(i, 5))
        def _():
            for j in range(2):
                phase3(i - 5, j).wait()
                phase4(i - 5, j).start()

        @pl.when(between(i, 7))
        def _():
            s = i - 7
            phase5(s).wait()

            @pl.when(s >= n_stages - n_chunks)
            def _():
                out_copy(lax.rem(s, n_chunks)).start()

        @pl.when(between(i, 6))
        def _():
            for j in range(2):
                phase4(i - 6, j).wait()
            phase5(i - 6).start()

        @pl.when(live)
        def _():
            @pl.when(i >= 1)
            def _():
                for copy in rec_copies(i - 1):
                    copy.wait()

            @pl.when(i + 1 < n_stages)
            def _():
                for copy in kv_copies(i + 1):
                    copy.start()

            attend(i, layer, chunk)

        @pl.when(between(i, 1))
        def _():
            s = i - 1
            phase0(s).wait()
            for j in range(2):
                @pl.loop(0, quarter // 4)
                def _(g):
                    ts = pl.ds(quarter * j + g * 4, 4)
                    sum0[lax.rem(s, 2), ts] = part[pl.ds(base + quarter * j + g * 4, 4)] + recv0[lax.rem(s, 2), ts]

                phase1(s, j).start()

        @pl.when(live)
        def _():
            feed_forward(i, layer)

        @pl.when(between(i, 2))
        def _():
            s = i - 2
            for j in range(2):
                phase1(s, j).wait()
                mine = pl.ds(quarter * j + eighth * pos1[j], eighth)
                ts = pl.ds(eighth * j, eighth)
                sum1[lax.rem(s, 2), ts] = sum0[lax.rem(s, 2), mine] + recv1[lax.rem(s, 4), ts]
                phase2(s, j).start()

        @pl.when(live)
        def _():
            project_out(i, layer)
            phase0(i).start()

        @pl.when(between(i, 3))
        def _():
            s = i - 3
            where = lax.rem(s, n_chunks)
            for j in range(2):
                phase2(s, j).wait()
                own = pl.ds(base2[j], last)
                total = sum1[lax.rem(s, 2), pl.ds(eighth * j + last * pos2[j], last)].astype(F32) + recv2[lax.rem(s, 4), pl.ds(last * j, last)].astype(F32)
                total = total + hid[where, own].astype(F32) + b_out[lax.div(s, n_chunks)][None]
                hid[where, own] = total.astype(BF16)
                phase3(s, j).start()

    for copy in rec_copies(n_stages - 1):
        copy.wait()
    for chunk in range(n_chunks):
        out_copy(chunk).wait()


def merge_kernel(n_blocks, lens, hid_in, k_hbm, v_hbm, rec_k, rec_v, hid_out, k_out, v_out, hbuf, kbuf, vbuf, rk, rv, in_sem, out_sem):
    size = kbuf.shape[0] // n_blocks
    steps = rk.shape[1]

    def block(ref, i):
        rows = ref.shape[0] // n_blocks
        return ref.at[pl.ds(i * rows, rows)]

    def loads(i):
        pairs = ((k_hbm, kbuf), (v_hbm, vbuf), (rec_k, rk), (rec_v, rv), (hid_in, hbuf))
        return [pltpu.make_async_copy(block(src, i), block(dst, i), in_sem.at[j, i]) for j, (src, dst) in enumerate(pairs)]

    def stores(i):
        pairs = ((kbuf, k_out), (vbuf, v_out), (hbuf, hid_out))
        return [pltpu.make_async_copy(block(src, i), block(dst, i), out_sem.at[j, i]) for j, (src, dst) in enumerate(pairs)]

    for i in range(n_blocks):
        for copy in loads(i):
            copy.start()

    @pl.loop(0, n_blocks)
    def _(i):
        for copy in loads(i):
            copy.wait()
        for b in range(size):
            row = i * size + b
            at = lens[lax.rem(row, lens.shape[0])]
            kbuf[row, pl.ds(at, steps)] = rk[row]
            vbuf[row, pl.ds(at, steps)] = rv[row]
        for copy in stores(i):
            copy.start()

    for i in range(n_blocks):
        for copy in stores(i):
            copy.wait()


def inverse_frequencies():
    lane = np.arange(128)
    return np.where(lane < ROT_DIM, 1.0 / (10000.0 ** ((lane // 2 * 2) / ROT_DIM)), 0.0)


def decode_shard(x_steps, cur_len, k_cache, v_cache, ln_gain, ln_bias, w_q, w_k, w_v, w_o, w_in, b_in, w_out, b_out):
    n_layers, batch, cache_len, n_heads, head_dim = k_cache.shape
    steps, _, d_model = x_steps.shape
    ff = w_in.shape[2]
    n_chunks = batch // SEQS
    n_stages = n_layers * n_chunks
    rows = steps * SEQS
    flat = (n_layers, batch, cache_len * n_heads, head_dim)
    step_angles = np.arange(steps)[:, None] * inverse_frequencies()[None, :]
    signed = np.where(np.arange(128) % 2 == 0, -1.0, 1.0)
    cos_t, sin_t = (np.repeat(tab.astype(np.float32)[:, None, :], SEQS, axis=1) for tab in (np.cos(step_angles), np.sin(step_angles) * signed))
    inv_freq = inverse_frequencies().astype(np.float32)[None, :]
    any_spec, vmem = pl.BlockSpec(memory_space=pl.ANY), pl.BlockSpec(memory_space=pltpu.VMEM)
    dma = pltpu.SemaphoreType.DMA
    block = (steps, SEQS, d_model)
    hidden, rec_k, rec_v = pl.pallas_call(
        functools.partial(decode_kernel, n_chunks, n_stages),
        out_shape=(jax.ShapeDtypeStruct(x_steps.shape, BF16),
                   jax.ShapeDtypeStruct((n_layers, batch, steps * n_heads, head_dim), BF16),
                   jax.ShapeDtypeStruct((n_layers, batch, steps * n_heads, head_dim), BF16)),
        in_specs=[any_spec] * 9 + [pl.BlockSpec(memory_space=pltpu.SMEM)] + [vmem] * 7,
        out_specs=(any_spec,) * 3,
        scratch_shapes=[
            pltpu.VMEM(w_q.shape, BF16), pltpu.VMEM(w_k.shape, BF16), pltpu.VMEM(w_v.shape, BF16), pltpu.VMEM(w_o.shape, BF16),
            pltpu.VMEM(w_in.shape, BF16), pltpu.VMEM(w_out.shape, BF16),
            pltpu.VMEM((n_chunks,) + block, BF16), pltpu.VMEM(block, BF16),
            pltpu.VMEM((2, steps // 2, SEQS, d_model), BF16), pltpu.VMEM((2, steps // 2, SEQS, d_model), BF16),
            pltpu.VMEM((4, steps // 4, SEQS, d_model), BF16), pltpu.VMEM((2, steps // 4, SEQS, d_model), BF16),
            pltpu.VMEM((4, steps // 8, SEQS, d_model), BF16),
            pltpu.VMEM((2, rows, d_model + 128), BF16),
            pltpu.VMEM((2, rows, 128), F32), pltpu.VMEM((2, rows, 128), F32), pltpu.VMEM((2, rows, 128), F32), pltpu.VMEM((2, rows, 128), F32),
            pltpu.VMEM((rows, 256), BF16), pltpu.VMEM((rows, ff + 128), BF16),
            pltpu.VMEM((SEQS, 2, 2 * steps, 128), F32), pltpu.VMEM((SEQS, 2 * steps, 256), F32), pltpu.VMEM((2 * steps, 256), jnp.int32),
            pltpu.VMEM((2, SEQS, 256, 128), BF16), pltpu.VMEM((2, SEQS, 256, 128), BF16),
            pltpu.VMEM((batch, cache_len * n_heads), jnp.int32), pltpu.VMEM((batch, 128), F32), pltpu.VMEM((batch, 128), F32),
            pltpu.VMEM((n_layers, 1, d_model), F32), pltpu.VMEM((n_layers, 1, d_model), F32),
            pltpu.VMEM((n_layers, 1, ff), F32), pltpu.VMEM((n_layers, 1, d_model), F32),
            dma((n_layers, 6)), dma((n_chunks,)), dma((2, 2)), dma((2, 2)), dma((n_chunks,)), dma((10, 2)), dma((10, 4)),
        ],
        compiler_params=pltpu.CompilerParams(collective_id=0, has_side_effects=True, vmem_limit_bytes=60 * 1024 * 1024),
        name="decode",
    )(x_steps, k_cache.reshape(flat), v_cache.reshape(flat), w_q, w_k, w_v, w_o, w_in, w_out,
      cur_len, inv_freq, cos_t, sin_t, ln_gain, ln_bias, b_in, b_out)

    pairs = n_layers * batch
    n_blocks = 16
    lines = (pairs, cache_len, n_heads, head_dim)
    new = (pairs, steps, n_heads, head_dim)
    hidden, k_out, v_out = pl.pallas_call(
        functools.partial(merge_kernel, n_blocks),
        out_shape=(jax.ShapeDtypeStruct(x_steps.shape, BF16),) + (jax.ShapeDtypeStruct(lines, BF16),) * 2,
        in_specs=[pl.BlockSpec(memory_space=pltpu.SMEM)] + [any_spec] * 5,
        out_specs=(any_spec,) * 3,
        scratch_shapes=[pltpu.VMEM(x_steps.shape, BF16), pltpu.VMEM(lines, BF16), pltpu.VMEM(lines, BF16),
                        pltpu.VMEM(new, BF16), pltpu.VMEM(new, BF16), dma((5, n_blocks)), dma((3, n_blocks))],
        compiler_params=pltpu.CompilerParams(vmem_limit_bytes=62 * 1024 * 1024),
        name="merge",
    )(cur_len, hidden, k_cache.reshape(lines), v_cache.reshape(lines), rec_k.reshape(new), rec_v.reshape(new))
    return hidden, k_out.reshape(k_cache.shape), v_out.reshape(v_cache.shape)


def solution(mesh):
    cache_spec = P(None, "dp", None, "tp", None)
    in_specs = (P(None, "dp", None), P("dp"), cache_spec, cache_spec, P(None, None), P(None, None),
                P(None, None, "tp"), P(None, None, "tp"), P(None, None, "tp"), P(None, "tp", None),
                P(None, None, "tp"), P(None, "tp"), P(None, "tp", None), P(None, None))
    out_specs = (P(None, "dp", None), cache_spec, cache_spec)
    return jax.shard_map(decode_shard, mesh=mesh, in_specs=in_specs, out_specs=out_specs, check_vma=False)
```

```python
import functools

import jax
import jax.numpy as jnp
import numpy as np
from jax import lax
from jax.experimental import pallas as pl
from jax.experimental.pallas import tpu as pltpu
from jax.sharding import PartitionSpec as P

ROT_DIM = 64
LN_EPS = 1e-5
MESH = pl.DeviceIdType.MESH
F32 = jnp.float32
BF16 = jnp.bfloat16
SEQS = 8
OLD = 96


def decode_kernel(n_chunks, n_stages, x_hbm, k_hbm, v_hbm, wq_hbm, wk_hbm, wv_hbm, wo_hbm, win_hbm, wout_hbm,
                  lens_in, inv_freq, cos_t, sin_t, gain_in, bias_in, b_in_in, b_out_in,
                  out_hbm, rec_k, rec_v,
                  wq, wk, wv, wo, win, wout, hid, part, recv0, sum0, recv1, sum1, recv2,
                  normed, qf, kf, vf, cf, ctx, act, inter, scores, key_scr, kbuf, vbuf,
                  lens, cos_c, sin_c, gain, bias, b_in, b_out,
                  w_sem, x_sem, kv_sem, rec_sem, out_sem, send_sem, recv_sem):
    steps = x_hbm.shape[0]
    rows = steps * SEQS
    ff = win_hbm.shape[2]
    half, quarter, eighth, last = steps // 2, steps // 4, steps // 8, steps // 16
    d_model = x_hbm.shape[2]
    me = lax.axis_index("tp")
    core = lax.rem(me, 2)
    px = lax.rem(lax.div(me, 2), 2)
    py = lax.div(me, 4)
    partner = me + 1 - 2 * core
    x_peer = me + 2 * (1 - 2 * px)
    y_peer = me + 4 * (1 - 2 * py)
    first, second = (x_peer, y_peer), (y_peer, x_peer)
    pos1, pos2 = (px, py), (py, px)
    base = half * core
    base1 = [base + quarter * j + eighth * pos1[j] for j in range(2)]
    base2 = [base1[j] + last * pos2[j] for j in range(2)]

    weight_pairs = ((wq_hbm, wq), (wk_hbm, wk), (wv_hbm, wv), (win_hbm, win), (wo_hbm, wo), (wout_hbm, wout))

    def weight_copy(layer, j):
        src, dst = weight_pairs[j]
        return pltpu.make_async_copy(src.at[layer], dst.at[layer], w_sem.at[layer, j])

    def x_copy(chunk):
        return pltpu.make_async_copy(x_hbm.at[:, pl.ds(pl.multiple_of(chunk * SEQS, SEQS), SEQS), :], hid.at[chunk], x_sem.at[chunk])

    def out_copy(chunk):
        return pltpu.make_async_copy(hid.at[chunk], out_hbm.at[:, pl.ds(pl.multiple_of(chunk * SEQS, SEQS), SEQS), :], out_sem.at[chunk])

    def kv_copies(stage):
        layer, chunk, slot = lax.div(stage, n_chunks), lax.rem(stage, n_chunks), lax.rem(stage, 2)
        seqs = pl.ds(chunk * SEQS, SEQS)
        return (pltpu.make_async_copy(k_hbm.at[layer, seqs], kbuf.at[slot], kv_sem.at[0, slot]),
                pltpu.make_async_copy(v_hbm.at[layer, seqs], vbuf.at[slot], kv_sem.at[1, slot]))

    def rec_copies(stage):
        layer, chunk, slot = lax.div(stage, n_chunks), lax.rem(stage, n_chunks), lax.rem(stage, 2)
        seqs = pl.ds(chunk * SEQS, SEQS)
        new = pl.ds(2 * OLD, 2 * steps)
        return (pltpu.make_async_copy(kbuf.at[slot, :, new, :], rec_k.at[layer, seqs], rec_sem.at[0, slot]),
                pltpu.make_async_copy(vbuf.at[slot, :, new, :], rec_v.at[layer, seqs], rec_sem.at[1, slot]))

    def remote(kind, stage, src, dst, peer):
        return pltpu.make_async_remote_copy(src_ref=src, dst_ref=dst, send_sem=send_sem.at[kind, lax.rem(stage, 2)],
                                            recv_sem=recv_sem.at[kind, lax.rem(stage, 4)], device_id={"tp": peer}, device_id_type=MESH)

    def phase0(stage):
        return remote(0, stage, part.at[pl.ds(half - base, half)], recv0.at[lax.rem(stage, 2)], partner)

    def phase1(stage, j):
        block = pl.ds(quarter * j + eighth * (1 - pos1[j]), eighth)
        return remote(1 + j, stage, sum0.at[lax.rem(stage, 2), block], recv1.at[lax.rem(stage, 4), pl.ds(eighth * j, eighth)], first[j])

    def phase2(stage, j):
        block = pl.ds(eighth * j + last * (1 - pos2[j]), last)
        return remote(3 + j, stage, sum1.at[lax.rem(stage, 2), block], recv2.at[lax.rem(stage, 4), pl.ds(last * j, last)], second[j])

    def gather(kind, stage, start, size, peer):
        block = hid.at[lax.rem(stage, n_chunks), pl.ds(start, size)]
        return remote(kind, stage, block, block, peer)

    def phase3(stage, j):
        return gather(5 + j, stage, base2[j], last, second[j])

    def phase4(stage, j):
        return gather(7 + j, stage, base1[j], eighth, first[j])

    def phase5(stage):
        return gather(9, stage, base, half, partner)

    barrier = pltpu.get_barrier_semaphore()
    for peer in (partner, x_peer, y_peer):
        pl.semaphore_signal(barrier, inc=1, device_id={"tp": peer}, device_id_type=MESH)
    x_copy(0).start()
    for j in range(3):
        weight_copy(0, j).start()
    for copy in kv_copies(0):
        copy.start()
    for j in range(3, 6):
        weight_copy(0, j).start()
    x_copy(1).start()
    for b in range(lens.shape[0]):
        lens[b:b + 1, :] = jnp.full((1, lens.shape[1]), lens_in[b], jnp.int32)
    angles = lens[:, 0:128].astype(F32) * inv_freq[...]
    odd = lax.rem(lax.broadcasted_iota(jnp.int32, angles.shape, 1), 2) == 1
    cos_c[...] = jnp.cos(angles)
    sin_c[...] = jnp.where(odd, jnp.sin(angles), -jnp.sin(angles))
    for src, dst in ((gain_in, gain), (bias_in, bias), (b_in_in, b_in), (b_out_in, b_out)):
        for layer in range(src.shape[0]):
            dst[layer] = src[layer:layer + 1, :].astype(F32)

    def norm_rows(stage, start, count):
        layer, chunk, slot = lax.div(stage, n_chunks), lax.rem(stage, n_chunks), lax.rem(stage, 2)
        for k in range(0, count, 2):
            x = hid[chunk, pl.ds(start + k, 2)].astype(F32)
            centered = x - jnp.mean(x, axis=-1, keepdims=True)
            var = jnp.mean(centered * centered, axis=-1, keepdims=True)
            y = centered * lax.rsqrt(var + LN_EPS) * gain[layer][None] + bias[layer][None]
            normed[slot, pl.ds((start + k) * SEQS if isinstance(start, int) else pl.multiple_of((start + k) * SEQS, 2 * SEQS), 2 * SEQS), pl.ds(0, d_model)] = y.reshape(2 * SEQS, d_model).astype(BF16)

    def project_in(stage, layer, chunk):
        @pl.when(chunk == 0)
        def _():
            for j in range(3):
                weight_copy(layer, j).wait()

        here = pl.ds(pl.multiple_of(chunk * SEQS, SEQS), SEQS)
        cc, sc = cos_c[here, :][None], sin_c[here, :][None]
        ct, st = cos_t[...], sin_t[...]
        cos = (cc * ct - sc * st).reshape(rows, 128)
        sin = (sc * ct + cc * st).reshape(rows, 128)
        even = lax.rem(lax.broadcasted_iota(jnp.int32, (rows, 128), 1), 2) == 0

        for weight, dst, rotate in ((wq, qf, True), (wk, kf, True), (wv, vf, False)):
            vec = jnp.dot(normed[lax.rem(stage, 2), :, pl.ds(0, d_model)], weight[layer], preferred_element_type=F32)
            for h in range(2):
                piece = vec[:, h * 128:(h + 1) * 128]
                if rotate:
                    swapped = jnp.where(even, pltpu.roll(piece, 127, 1), pltpu.roll(piece, 1, 1))
                    piece = piece * cos + swapped * sin
                dst[h] = piece

    def attend(stage, layer, chunk):
        slot = lax.rem(stage, 2)
        for copy in kv_copies(stage):
            copy.wait()

        @pl.when(chunk == 0)
        def _():
            for j in range(3, 6):
                weight_copy(layer, j).wait()

        shape = (2 * steps, 2 * (OLD + steps))
        row, col = lax.broadcasted_iota(jnp.int32, shape, 0), lax.broadcasted_iota(jnp.int32, shape, 1)
        col_slot, col_head = lax.shift_right_logical(col, 1), lax.bitwise_and(col, 1)
        row_head, row_step = lax.div(row, steps), lax.rem(row, steps)
        never = 1 << 20
        fresh = jnp.where(col_slot - OLD <= row_step, -1, never)
        key_scr[...] = jnp.where(row_head == col_head, jnp.where(col_slot >= OLD, fresh, col_slot), never)
        limit = lens[pl.ds(pl.multiple_of(chunk * SEQS, SEQS), SEQS), :]
        for b in range(SEQS):
            mine = pl.ds(b, steps, stride=SEQS)
            for src, buf, j in ((kf, kbuf, 0), (vf, vbuf, 1)):
                for h in range(2):
                    inter[b, j, pl.ds(h, steps, stride=2), :] = src[h, mine, :]
                buf[slot, b, pl.ds(2 * OLD, 2 * steps), :] = inter[b, j].astype(BF16)
        for b in range(SEQS):
            mine = pl.ds(b, steps, stride=SEQS)
            query = jnp.concatenate([qf[0, mine, :], qf[1, mine, :]], axis=0).astype(BF16)
            s = lax.dot_general(query, kbuf[slot, b], (((1,), (1,)), ((), ())), preferred_element_type=F32) * (128 ** -0.5)
            scores[b] = jnp.where(key_scr[...] < limit[b:b + 1, :], s, -jnp.inf)
        for b in range(SEQS):
            s = scores[b]
            e = jnp.exp(s - jnp.max(s, axis=-1, keepdims=True))
            probs = (e * (1.0 / jnp.sum(e, axis=-1, keepdims=True))).astype(BF16)
            context = jnp.dot(probs, vbuf[slot, b], preferred_element_type=F32)
            for h in range(2):
                cf[h, pl.ds(b, steps, stride=SEQS), :] = context[h * steps:(h + 1) * steps]

        for copy in rec_copies(stage):
            copy.start()

    def feed_forward(stage, layer):
        slot = lax.rem(stage, 2)
        for n in range(ff // 256):
            cols = pl.ds(n * 256, 256)
            pre = jnp.dot(normed[slot, :, pl.ds(0, d_model)], win[layer, :, cols], preferred_element_type=F32) + b_in[layer, :, cols]
            act[:, cols] = jax.nn.gelu(pre, approximate=True).astype(BF16)

    def project_out(stage, layer):
        for h in range(2):
            ctx[:, h * 128:(h + 1) * 128] = cf[h].astype(BF16)

        following = jnp.minimum(stage + 1, n_stages - 1)
        group = steps // (d_model // 256)

        @pl.when(stage + 1 < n_chunks)
        def _():
            x_copy(stage + 1).wait()

        for n in range(d_model // 256):
            cols = pl.ds(n * 256, 256)
            total = jnp.dot(ctx[...], wo[layer, :, cols], preferred_element_type=F32)
            total += jnp.dot(act[:, pl.ds(0, ff)], wout[layer, :, cols], preferred_element_type=F32)
            part[:, :, cols] = total.reshape(steps, SEQS, 256).astype(BF16)
            norm_rows(following, n * group, group)

    x_copy(0).wait()

    @pl.loop(0, steps // 8)
    def _(g):
        norm_rows(0, g * 8, 8)

    pl.semaphore_wait(barrier, 3)

    def between(i, lag):
        return jnp.logical_and(i >= lag, i < n_stages + lag)

    @pl.loop(0, n_stages + 5)
    def _(i):
        layer, chunk = lax.div(i, n_chunks), lax.rem(i, n_chunks)
        live = i < n_stages

        @pl.when(i == 1)
        def _():
            for c in range(2, n_chunks):
                x_copy(c).start()
            for j in range(6):
                weight_copy(1, j).start()

        @pl.when(live)
        def _():
            project_in(i, layer, chunk)

        @pl.when(between(i, 2))
        def _():
            s = i - 2
            for j in range(2):
                phase1(s, j).wait()
                mine = pl.ds(quarter * j + eighth * pos1[j], eighth)
                ts = pl.ds(eighth * j, eighth)
                sum1[lax.rem(s, 2), ts] = sum0[lax.rem(s, 2), mine] + recv1[lax.rem(s, 4), ts]
                phase2(s, j).start()

        @pl.when(between(i, 5))
        def _():
            s = i - 5
            phase5(s).wait()

            @pl.when(s >= n_stages - n_chunks)
            def _():
                out_copy(lax.rem(s, n_chunks)).start()

        @pl.when(live)
        def _():
            @pl.when(i >= 1)
            def _():
                for copy in rec_copies(i - 1):
                    copy.wait()

            @pl.when(i + 1 < n_stages)
            def _():
                for copy in kv_copies(i + 1):
                    copy.start()

            attend(i, layer, chunk)

        @pl.when(between(i, 1))
        def _():
            s = i - 1
            phase0(s).wait()
            for j in range(2):
                @pl.loop(0, quarter // 4)
                def _(g):
                    ts = pl.ds(quarter * j + g * 4, 4)
                    sum0[lax.rem(s, 2), ts] = part[pl.ds(base + quarter * j + g * 4, 4)] + recv0[lax.rem(s, 2), ts]

                phase1(s, j).start()

        @pl.when(live)
        def _():
            feed_forward(i, layer)

        @pl.when(between(i, 3))
        def _():
            for j in range(2):
                phase3(i - 3, j).wait()
                phase4(i - 3, j).start()

        @pl.when(between(i, 4))
        def _():
            for j in range(2):
                phase4(i - 4, j).wait()
            phase5(i - 4).start()

        @pl.when(live)
        def _():
            project_out(i, layer)
            phase0(i).start()

        @pl.when(between(i, 2))
        def _():
            s = i - 2
            where = lax.rem(s, n_chunks)
            for j in range(2):
                phase2(s, j).wait()
                own = pl.ds(base2[j], last)
                total = sum1[lax.rem(s, 2), pl.ds(eighth * j + last * pos2[j], last)].astype(F32) + recv2[lax.rem(s, 4), pl.ds(last * j, last)].astype(F32)
                total = total + hid[where, own].astype(F32) + b_out[lax.div(s, n_chunks)][None]
                hid[where, own] = total.astype(BF16)
                phase3(s, j).start()

    for copy in rec_copies(n_stages - 1):
        copy.wait()
    for chunk in range(n_chunks):
        out_copy(chunk).wait()


def merge_kernel(n_blocks, lens, hid_in, k_hbm, v_hbm, rec_k, rec_v, hid_out, k_out, v_out, hbuf, kbuf, vbuf, rk, rv, in_sem, out_sem):
    size = kbuf.shape[0] // n_blocks
    steps = rk.shape[1]

    def block(ref, i):
        rows = ref.shape[0] // n_blocks
        return ref.at[pl.ds(i * rows, rows)]

    def loads(i):
        pairs = ((k_hbm, kbuf), (v_hbm, vbuf), (rec_k, rk), (rec_v, rv), (hid_in, hbuf))
        return [pltpu.make_async_copy(block(src, i), block(dst, i), in_sem.at[j, i]) for j, (src, dst) in enumerate(pairs)]

    def stores(i):
        pairs = ((kbuf, k_out), (vbuf, v_out), (hbuf, hid_out))
        return [pltpu.make_async_copy(block(src, i), block(dst, i), out_sem.at[j, i]) for j, (src, dst) in enumerate(pairs)]

    for i in range(n_blocks):
        for copy in loads(i):
            copy.start()

    @pl.loop(0, n_blocks)
    def _(i):
        for copy in loads(i):
            copy.wait()
        for b in range(size):
            row = i * size + b
            at = lens[lax.rem(row, lens.shape[0])]
            kbuf[row, pl.ds(at, steps)] = rk[row]
            vbuf[row, pl.ds(at, steps)] = rv[row]
        for copy in stores(i):
            copy.start()

    for i in range(n_blocks):
        for copy in stores(i):
            copy.wait()


def inverse_frequencies():
    lane = np.arange(128)
    return np.where(lane < ROT_DIM, 1.0 / (10000.0 ** ((lane // 2 * 2) / ROT_DIM)), 0.0)


def decode_shard(x_steps, cur_len, k_cache, v_cache, ln_gain, ln_bias, w_q, w_k, w_v, w_o, w_in, b_in, w_out, b_out):
    n_layers, batch, cache_len, n_heads, head_dim = k_cache.shape
    steps, _, d_model = x_steps.shape
    ff = w_in.shape[2]
    n_chunks = batch // SEQS
    n_stages = n_layers * n_chunks
    rows = steps * SEQS
    flat = (n_layers, batch, cache_len * n_heads, head_dim)
    step_angles = np.arange(steps)[:, None] * inverse_frequencies()[None, :]
    signed = np.where(np.arange(128) % 2 == 0, -1.0, 1.0)
    cos_t, sin_t = (np.repeat(tab.astype(np.float32)[:, None, :], SEQS, axis=1) for tab in (np.cos(step_angles), np.sin(step_angles) * signed))
    inv_freq = inverse_frequencies().astype(np.float32)[None, :]
    any_spec, vmem = pl.BlockSpec(memory_space=pl.ANY), pl.BlockSpec(memory_space=pltpu.VMEM)
    dma = pltpu.SemaphoreType.DMA
    block = (steps, SEQS, d_model)
    hidden, rec_k, rec_v = pl.pallas_call(
        functools.partial(decode_kernel, n_chunks, n_stages),
        out_shape=(jax.ShapeDtypeStruct(x_steps.shape, BF16),
                   jax.ShapeDtypeStruct((n_layers, batch, steps * n_heads, head_dim), BF16),
                   jax.ShapeDtypeStruct((n_layers, batch, steps * n_heads, head_dim), BF16)),
        in_specs=[any_spec] * 9 + [pl.BlockSpec(memory_space=pltpu.SMEM)] + [vmem] * 7,
        out_specs=(any_spec,) * 3,
        scratch_shapes=[
            pltpu.VMEM(w_q.shape, BF16), pltpu.VMEM(w_k.shape, BF16), pltpu.VMEM(w_v.shape, BF16), pltpu.VMEM(w_o.shape, BF16),
            pltpu.VMEM(w_in.shape, BF16), pltpu.VMEM(w_out.shape, BF16),
            pltpu.VMEM((n_chunks,) + block, BF16), pltpu.VMEM(block, BF16),
            pltpu.VMEM((2, steps // 2, SEQS, d_model), BF16), pltpu.VMEM((2, steps // 2, SEQS, d_model), BF16),
            pltpu.VMEM((4, steps // 4, SEQS, d_model), BF16), pltpu.VMEM((2, steps // 4, SEQS, d_model), BF16),
            pltpu.VMEM((4, steps // 8, SEQS, d_model), BF16),
            pltpu.VMEM((2, rows, d_model + 128), BF16),
            pltpu.VMEM((2, rows, 128), F32), pltpu.VMEM((2, rows, 128), F32), pltpu.VMEM((2, rows, 128), F32), pltpu.VMEM((2, rows, 128), F32),
            pltpu.VMEM((rows, 256), BF16), pltpu.VMEM((rows, ff + 128), BF16),
            pltpu.VMEM((SEQS, 2, 2 * steps, 128), F32), pltpu.VMEM((SEQS, 2 * steps, 256), F32), pltpu.VMEM((2 * steps, 256), jnp.int32),
            pltpu.VMEM((2, SEQS, 256, 128), BF16), pltpu.VMEM((2, SEQS, 256, 128), BF16),
            pltpu.VMEM((batch, cache_len * n_heads), jnp.int32), pltpu.VMEM((batch, 128), F32), pltpu.VMEM((batch, 128), F32),
            pltpu.VMEM((n_layers, 1, d_model), F32), pltpu.VMEM((n_layers, 1, d_model), F32),
            pltpu.VMEM((n_layers, 1, ff), F32), pltpu.VMEM((n_layers, 1, d_model), F32),
            dma((n_layers, 6)), dma((n_chunks,)), dma((2, 2)), dma((2, 2)), dma((n_chunks,)), dma((10, 2)), dma((10, 4)),
        ],
        compiler_params=pltpu.CompilerParams(collective_id=0, has_side_effects=True, vmem_limit_bytes=60 * 1024 * 1024),
        name="decode",
    )(x_steps, k_cache.reshape(flat), v_cache.reshape(flat), w_q, w_k, w_v, w_o, w_in, w_out,
      cur_len, inv_freq, cos_t, sin_t, ln_gain, ln_bias, b_in, b_out)

    pairs = n_layers * batch
    n_blocks = 16
    lines = (pairs, cache_len, n_heads, head_dim)
    new = (pairs, steps, n_heads, head_dim)
    hidden, k_out, v_out = pl.pallas_call(
        functools.partial(merge_kernel, n_blocks),
        out_shape=(jax.ShapeDtypeStruct(x_steps.shape, BF16),) + (jax.ShapeDtypeStruct(lines, BF16),) * 2,
        in_specs=[pl.BlockSpec(memory_space=pltpu.SMEM)] + [any_spec] * 5,
        out_specs=(any_spec,) * 3,
        scratch_shapes=[pltpu.VMEM(x_steps.shape, BF16), pltpu.VMEM(lines, BF16), pltpu.VMEM(lines, BF16),
                        pltpu.VMEM(new, BF16), pltpu.VMEM(new, BF16), dma((5, n_blocks)), dma((3, n_blocks))],
        compiler_params=pltpu.CompilerParams(vmem_limit_bytes=62 * 1024 * 1024),
        name="merge",
    )(cur_len, hidden, k_cache.reshape(lines), v_cache.reshape(lines), rec_k.reshape(new), rec_v.reshape(new))
    return hidden, k_out.reshape(k_cache.shape), v_out.reshape(v_cache.shape)


def solution(mesh):
    cache_spec = P(None, "dp", None, "tp", None)
    in_specs = (P(None, "dp", None), P("dp"), cache_spec, cache_spec, P(None, None), P(None, None),
                P(None, None, "tp"), P(None, None, "tp"), P(None, None, "tp"), P(None, "tp", None),
                P(None, None, "tp"), P(None, "tp"), P(None, "tp", None), P(None, None))
    out_specs = (P(None, "dp", None), cache_spec, cache_spec)
    return jax.shard_map(decode_shard, mesh=mesh, in_specs=in_specs, out_specs=out_specs, check_vma=False)
```

```python
import functools

import jax
import jax.numpy as jnp
import numpy as np
from jax import lax
from jax.experimental import pallas as pl
from jax.experimental.pallas import tpu as pltpu
from jax.sharding import PartitionSpec as P

ROT_DIM = 64
LN_EPS = 1e-5
MESH = pl.DeviceIdType.MESH
F32 = jnp.float32
BF16 = jnp.bfloat16
SEQS = 8
OLD = 96


def decode_kernel(n_chunks, n_stages, x_hbm, k_hbm, v_hbm, wq_hbm, wk_hbm, wv_hbm, wo_hbm, win_hbm, wout_hbm,
                  lens_in, inv_freq, cos_t, sin_t, gain_in, bias_in, b_in_in, b_out_in,
                  out_hbm, rec_k, rec_v,
                  wq, wk, wv, wo, win, wout, hid, part, recv0, sum0, recv1, sum1, recv2,
                  normed, qf, kf, vf, cf, ctx, act, inter, scores, key_scr, kbuf, vbuf,
                  lens, cos_c, sin_c, gain, bias, b_in, b_out,
                  w_sem, x_sem, kv_sem, rec_sem, out_sem, send_sem, recv_sem):
    steps = x_hbm.shape[0]
    rows = steps * SEQS
    ff = win_hbm.shape[2]
    half, quarter, eighth, last = steps // 2, steps // 4, steps // 8, steps // 16
    d_model = x_hbm.shape[2]
    me = lax.axis_index("tp")
    core = lax.rem(me, 2)
    px = lax.rem(lax.div(me, 2), 2)
    py = lax.div(me, 4)
    partner = me + 1 - 2 * core
    x_peer = me + 2 * (1 - 2 * px)
    y_peer = me + 4 * (1 - 2 * py)
    first, second = (x_peer, y_peer), (y_peer, x_peer)
    pos1, pos2 = (px, py), (py, px)
    base = half * core
    base1 = [base + quarter * j + eighth * pos1[j] for j in range(2)]
    base2 = [base1[j] + last * pos2[j] for j in range(2)]

    weight_pairs = ((wq_hbm, wq), (wk_hbm, wk), (wv_hbm, wv), (win_hbm, win), (wo_hbm, wo), (wout_hbm, wout))

    def weight_copy(layer, j):
        src, dst = weight_pairs[j]
        return pltpu.make_async_copy(src.at[layer], dst.at[layer], w_sem.at[layer, j])

    def x_copy(chunk):
        return pltpu.make_async_copy(x_hbm.at[:, pl.ds(pl.multiple_of(chunk * SEQS, SEQS), SEQS), :], hid.at[chunk], x_sem.at[chunk])

    def out_copy(chunk):
        return pltpu.make_async_copy(hid.at[chunk], out_hbm.at[:, pl.ds(pl.multiple_of(chunk * SEQS, SEQS), SEQS), :], out_sem.at[chunk])

    def kv_copies(stage):
        layer, chunk, slot = lax.div(stage, n_chunks), lax.rem(stage, n_chunks), lax.rem(stage, 2)
        seqs = pl.ds(chunk * SEQS, SEQS)
        return (pltpu.make_async_copy(k_hbm.at[layer, seqs], kbuf.at[slot], kv_sem.at[0, slot]),
                pltpu.make_async_copy(v_hbm.at[layer, seqs], vbuf.at[slot], kv_sem.at[1, slot]))

    def rec_copies(stage):
        layer, chunk, slot = lax.div(stage, n_chunks), lax.rem(stage, n_chunks), lax.rem(stage, 2)
        seqs = pl.ds(chunk * SEQS, SEQS)
        new = pl.ds(2 * OLD, 2 * steps)
        return (pltpu.make_async_copy(kbuf.at[slot, :, new, :], rec_k.at[layer, seqs], rec_sem.at[0, slot]),
                pltpu.make_async_copy(vbuf.at[slot, :, new, :], rec_v.at[layer, seqs], rec_sem.at[1, slot]))

    def remote(kind, stage, src, dst, peer):
        return pltpu.make_async_remote_copy(src_ref=src, dst_ref=dst, send_sem=send_sem.at[kind, lax.rem(stage, 2)],
                                            recv_sem=recv_sem.at[kind, lax.rem(stage, 4)], device_id={"tp": peer}, device_id_type=MESH)

    def phase0(stage):
        return remote(0, stage, part.at[pl.ds(half - base, half)], recv0.at[lax.rem(stage, 2)], partner)

    def phase1(stage, j):
        block = pl.ds(quarter * j + eighth * (1 - pos1[j]), eighth)
        return remote(1 + j, stage, sum0.at[lax.rem(stage, 2), block], recv1.at[lax.rem(stage, 4), pl.ds(eighth * j, eighth)], first[j])

    def phase2(stage, j):
        block = pl.ds(eighth * j + last * (1 - pos2[j]), last)
        return remote(3 + j, stage, sum1.at[lax.rem(stage, 2), block], recv2.at[lax.rem(stage, 4), pl.ds(last * j, last)], second[j])

    def gather(kind, stage, start, size, peer):
        block = hid.at[lax.rem(stage, n_chunks), pl.ds(start, size)]
        return remote(kind, stage, block, block, peer)

    def phase3(stage, j):
        return gather(5 + j, stage, base2[j], last, second[j])

    def phase4(stage, j):
        return gather(7 + j, stage, base1[j], eighth, first[j])

    def phase5(stage):
        return gather(9, stage, base, half, partner)

    barrier = pltpu.get_barrier_semaphore()
    for peer in (partner, x_peer, y_peer):
        pl.semaphore_signal(barrier, inc=1, device_id={"tp": peer}, device_id_type=MESH)
    x_copy(0).start()
    for j in range(3):
        weight_copy(0, j).start()
    for copy in kv_copies(0):
        copy.start()
    for j in range(3, 6):
        weight_copy(0, j).start()
    x_copy(1).start()
    for b in range(lens.shape[0]):
        lens[b:b + 1, :] = jnp.full((1, lens.shape[1]), lens_in[b], jnp.int32)
    angles = lens[:, 0:128].astype(F32) * inv_freq[...]
    odd = lax.rem(lax.broadcasted_iota(jnp.int32, angles.shape, 1), 2) == 1
    cos_c[...] = jnp.cos(angles)
    sin_c[...] = jnp.where(odd, jnp.sin(angles), -jnp.sin(angles))
    for src, dst in ((gain_in, gain), (bias_in, bias), (b_in_in, b_in), (b_out_in, b_out)):
        for layer in range(src.shape[0]):
            dst[layer] = src[layer:layer + 1, :].astype(F32)

    def norm_rows(stage, start, count):
        layer, chunk, slot = lax.div(stage, n_chunks), lax.rem(stage, n_chunks), lax.rem(stage, 2)
        for k in range(0, count, 2):
            x = hid[chunk, pl.ds(start + k, 2)].astype(F32)
            centered = x - jnp.mean(x, axis=-1, keepdims=True)
            var = jnp.mean(centered * centered, axis=-1, keepdims=True)
            y = centered * lax.rsqrt(var + LN_EPS) * gain[layer][None] + bias[layer][None]
            normed[slot, pl.ds((start + k) * SEQS if isinstance(start, int) else pl.multiple_of((start + k) * SEQS, 2 * SEQS), 2 * SEQS), pl.ds(0, d_model)] = y.reshape(2 * SEQS, d_model).astype(BF16)

    def project_in(stage, layer, chunk):
        @pl.when(chunk == 0)
        def _():
            for j in range(3):
                weight_copy(layer, j).wait()

        here = pl.ds(pl.multiple_of(chunk * SEQS, SEQS), SEQS)
        cc, sc = cos_c[here, :][None], sin_c[here, :][None]
        ct, st = cos_t[...], sin_t[...]
        cos = (cc * ct - sc * st).reshape(rows, 128)
        sin = (sc * ct + cc * st).reshape(rows, 128)
        even = lax.rem(lax.broadcasted_iota(jnp.int32, (rows, 128), 1), 2) == 0

        for weight, dst, rotate in ((wq, qf, True), (wk, kf, True), (wv, vf, False)):
            vec = jnp.dot(normed[lax.rem(stage, 2), :, pl.ds(0, d_model)], weight[layer], preferred_element_type=F32)
            for h in range(2):
                piece = vec[:, h * 128:(h + 1) * 128]
                if rotate:
                    swapped = jnp.where(even, pltpu.roll(piece, 127, 1), pltpu.roll(piece, 1, 1))
                    piece = piece * cos + swapped * sin
                dst[h] = piece

    def attend(stage, layer, chunk):
        slot = lax.rem(stage, 2)
        for copy in kv_copies(stage):
            copy.wait()

        @pl.when(chunk == 0)
        def _():
            for j in range(3, 6):
                weight_copy(layer, j).wait()

        shape = (2 * steps, 2 * (OLD + steps))
        row, col = lax.broadcasted_iota(jnp.int32, shape, 0), lax.broadcasted_iota(jnp.int32, shape, 1)
        col_slot, col_head = lax.shift_right_logical(col, 1), lax.bitwise_and(col, 1)
        row_head, row_step = lax.div(row, steps), lax.rem(row, steps)
        never = 1 << 20
        fresh = jnp.where(col_slot - OLD <= row_step, -1, never)
        key_scr[...] = jnp.where(row_head == col_head, jnp.where(col_slot >= OLD, fresh, col_slot), never)
        limit = lens[pl.ds(pl.multiple_of(chunk * SEQS, SEQS), SEQS), :]
        for b in range(SEQS):
            mine = pl.ds(b, steps, stride=SEQS)
            for src, buf, j in ((kf, kbuf, 0), (vf, vbuf, 1)):
                for h in range(2):
                    inter[b, j, pl.ds(h, steps, stride=2), :] = src[h, mine, :]
                buf[slot, b, pl.ds(2 * OLD, 2 * steps), :] = inter[b, j].astype(BF16)
        for b in range(SEQS):
            mine = pl.ds(b, steps, stride=SEQS)
            query = jnp.concatenate([qf[0, mine, :], qf[1, mine, :]], axis=0).astype(BF16)
            s = lax.dot_general(query, kbuf[slot, b], (((1,), (1,)), ((), ())), preferred_element_type=F32) * (128 ** -0.5)
            scores[b] = jnp.where(key_scr[...] < limit[b:b + 1, :], s, -jnp.inf)
        for b in range(SEQS):
            s = scores[b]
            e = jnp.exp(s - jnp.max(s, axis=-1, keepdims=True))
            probs = (e * (1.0 / jnp.sum(e, axis=-1, keepdims=True))).astype(BF16)
            context = jnp.dot(probs, vbuf[slot, b], preferred_element_type=F32)
            for h in range(2):
                cf[h, pl.ds(b, steps, stride=SEQS), :] = context[h * steps:(h + 1) * steps]

        for copy in rec_copies(stage):
            copy.start()

    def feed_forward(stage, layer):
        slot = lax.rem(stage, 2)
        for n in range(ff // 256):
            cols = pl.ds(n * 256, 256)
            pre = jnp.dot(normed[slot, :, pl.ds(0, d_model)], win[layer, :, cols], preferred_element_type=F32) + b_in[layer, :, cols]
            act[:, cols] = jax.nn.gelu(pre, approximate=True).astype(BF16)

    def project_out(stage, layer):
        for h in range(2):
            ctx[:, h * 128:(h + 1) * 128] = cf[h].astype(BF16)

        following = jnp.minimum(stage + 1, n_stages - 1)
        group = steps // (d_model // 256)

        @pl.when(stage + 1 < n_chunks)
        def _():
            x_copy(stage + 1).wait()

        for n in range(d_model // 256):
            cols = pl.ds(n * 256, 256)
            total = jnp.dot(ctx[...], wo[layer, :, cols], preferred_element_type=F32)
            total += jnp.dot(act[:, pl.ds(0, ff)], wout[layer, :, cols], preferred_element_type=F32)
            part[:, :, cols] = total.reshape(steps, SEQS, 256).astype(BF16)
            norm_rows(following, n * group, group)

    x_copy(0).wait()

    @pl.loop(0, steps // 8)
    def _(g):
        norm_rows(0, g * 8, 8)

    pl.semaphore_wait(barrier, 3)

    def between(i, lag):
        return jnp.logical_and(i >= lag, i < n_stages + lag)

    @pl.loop(0, n_stages + 5)
    def _(i):
        layer, chunk = lax.div(i, n_chunks), lax.rem(i, n_chunks)
        live = i < n_stages

        @pl.when(i == 1)
        def _():
            for c in range(2, n_chunks):
                x_copy(c).start()
            for j in range(6):
                weight_copy(1, j).start()

        @pl.when(live)
        def _():
            project_in(i, layer, chunk)

        @pl.when(between(i, 3))
        def _():
            s = i - 3
            where = lax.rem(s, n_chunks)
            for j in range(2):
                phase2(s, j).wait()
                own = pl.ds(base2[j], last)
                total = sum1[lax.rem(s, 2), pl.ds(eighth * j + last * pos2[j], last)].astype(F32) + recv2[lax.rem(s, 4), pl.ds(last * j, last)].astype(F32)
                total = total + hid[where, own].astype(F32) + b_out[lax.div(s, n_chunks)][None]
                hid[where, own] = total.astype(BF16)
                phase3(s, j).start()

        @pl.when(live)
        def _():
            @pl.when(i >= 1)
            def _():
                for copy in rec_copies(i - 1):
                    copy.wait()

            @pl.when(i + 1 < n_stages)
            def _():
                for copy in kv_copies(i + 1):
                    copy.start()

            attend(i, layer, chunk)

        @pl.when(between(i, 2))
        def _():
            s = i - 2
            for j in range(2):
                phase1(s, j).wait()
                mine = pl.ds(quarter * j + eighth * pos1[j], eighth)
                ts = pl.ds(eighth * j, eighth)
                sum1[lax.rem(s, 2), ts] = sum0[lax.rem(s, 2), mine] + recv1[lax.rem(s, 4), ts]
                phase2(s, j).start()

        @pl.when(live)
        def _():
            feed_forward(i, layer)

        @pl.when(between(i, 1))
        def _():
            s = i - 1
            phase0(s).wait()
            for j in range(2):
                @pl.loop(0, quarter // 4)
                def _(g):
                    ts = pl.ds(quarter * j + g * 4, 4)
                    sum0[lax.rem(s, 2), ts] = part[pl.ds(base + quarter * j + g * 4, 4)] + recv0[lax.rem(s, 2), ts]

                phase1(s, j).start()

        @pl.when(between(i, 5))
        def _():
            s = i - 5
            phase5(s).wait()

            @pl.when(s >= n_stages - n_chunks)
            def _():
                out_copy(lax.rem(s, n_chunks)).start()

        @pl.when(live)
        def _():
            project_out(i, layer)
            phase0(i).start()

        @pl.when(between(i, 3))
        def _():
            for j in range(2):
                phase3(i - 3, j).wait()
                phase4(i - 3, j).start()

        @pl.when(between(i, 4))
        def _():
            for j in range(2):
                phase4(i - 4, j).wait()
            phase5(i - 4).start()

    for copy in rec_copies(n_stages - 1):
        copy.wait()
    for chunk in range(n_chunks):
        out_copy(chunk).wait()


def merge_kernel(n_blocks, lens, hid_in, k_hbm, v_hbm, rec_k, rec_v, hid_out, k_out, v_out, hbuf, kbuf, vbuf, rk, rv, in_sem, out_sem):
    size = kbuf.shape[0] // n_blocks
    steps = rk.shape[1]

    def block(ref, i):
        rows = ref.shape[0] // n_blocks
        return ref.at[pl.ds(i * rows, rows)]

    def loads(i):
        pairs = ((k_hbm, kbuf), (v_hbm, vbuf), (rec_k, rk), (rec_v, rv), (hid_in, hbuf))
        return [pltpu.make_async_copy(block(src, i), block(dst, i), in_sem.at[j, i]) for j, (src, dst) in enumerate(pairs)]

    def stores(i):
        pairs = ((kbuf, k_out), (vbuf, v_out), (hbuf, hid_out))
        return [pltpu.make_async_copy(block(src, i), block(dst, i), out_sem.at[j, i]) for j, (src, dst) in enumerate(pairs)]

    for i in range(n_blocks):
        for copy in loads(i):
            copy.start()

    @pl.loop(0, n_blocks)
    def _(i):
        for copy in loads(i):
            copy.wait()
        for b in range(size):
            row = i * size + b
            at = lens[lax.rem(row, lens.shape[0])]
            kbuf[row, pl.ds(at, steps)] = rk[row]
            vbuf[row, pl.ds(at, steps)] = rv[row]
        for copy in stores(i):
            copy.start()

    for i in range(n_blocks):
        for copy in stores(i):
            copy.wait()


def inverse_frequencies():
    lane = np.arange(128)
    return np.where(lane < ROT_DIM, 1.0 / (10000.0 ** ((lane // 2 * 2) / ROT_DIM)), 0.0)


def decode_shard(x_steps, cur_len, k_cache, v_cache, ln_gain, ln_bias, w_q, w_k, w_v, w_o, w_in, b_in, w_out, b_out):
    n_layers, batch, cache_len, n_heads, head_dim = k_cache.shape
    steps, _, d_model = x_steps.shape
    ff = w_in.shape[2]
    n_chunks = batch // SEQS
    n_stages = n_layers * n_chunks
    rows = steps * SEQS
    flat = (n_layers, batch, cache_len * n_heads, head_dim)
    step_angles = np.arange(steps)[:, None] * inverse_frequencies()[None, :]
    signed = np.where(np.arange(128) % 2 == 0, -1.0, 1.0)
    cos_t, sin_t = (np.repeat(tab.astype(np.float32)[:, None, :], SEQS, axis=1) for tab in (np.cos(step_angles), np.sin(step_angles) * signed))
    inv_freq = inverse_frequencies().astype(np.float32)[None, :]
    any_spec, vmem = pl.BlockSpec(memory_space=pl.ANY), pl.BlockSpec(memory_space=pltpu.VMEM)
    dma = pltpu.SemaphoreType.DMA
    block = (steps, SEQS, d_model)
    hidden, rec_k, rec_v = pl.pallas_call(
        functools.partial(decode_kernel, n_chunks, n_stages),
        out_shape=(jax.ShapeDtypeStruct(x_steps.shape, BF16),
                   jax.ShapeDtypeStruct((n_layers, batch, steps * n_heads, head_dim), BF16),
                   jax.ShapeDtypeStruct((n_layers, batch, steps * n_heads, head_dim), BF16)),
        in_specs=[any_spec] * 9 + [pl.BlockSpec(memory_space=pltpu.SMEM)] + [vmem] * 7,
        out_specs=(any_spec,) * 3,
        scratch_shapes=[
            pltpu.VMEM(w_q.shape, BF16), pltpu.VMEM(w_k.shape, BF16), pltpu.VMEM(w_v.shape, BF16), pltpu.VMEM(w_o.shape, BF16),
            pltpu.VMEM(w_in.shape, BF16), pltpu.VMEM(w_out.shape, BF16),
            pltpu.VMEM((n_chunks,) + block, BF16), pltpu.VMEM(block, BF16),
            pltpu.VMEM((2, steps // 2, SEQS, d_model), BF16), pltpu.VMEM((2, steps // 2, SEQS, d_model), BF16),
            pltpu.VMEM((4, steps // 4, SEQS, d_model), BF16), pltpu.VMEM((2, steps // 4, SEQS, d_model), BF16),
            pltpu.VMEM((4, steps // 8, SEQS, d_model), BF16),
            pltpu.VMEM((2, rows, d_model + 128), BF16),
            pltpu.VMEM((2, rows, 128), F32), pltpu.VMEM((2, rows, 128), F32), pltpu.VMEM((2, rows, 128), F32), pltpu.VMEM((2, rows, 128), F32),
            pltpu.VMEM((rows, 256), BF16), pltpu.VMEM((rows, ff + 128), BF16),
            pltpu.VMEM((SEQS, 2, 2 * steps, 128), F32), pltpu.VMEM((SEQS, 2 * steps, 256), F32), pltpu.VMEM((2 * steps, 256), jnp.int32),
            pltpu.VMEM((2, SEQS, 256, 128), BF16), pltpu.VMEM((2, SEQS, 256, 128), BF16),
            pltpu.VMEM((batch, cache_len * n_heads), jnp.int32), pltpu.VMEM((batch, 128), F32), pltpu.VMEM((batch, 128), F32),
            pltpu.VMEM((n_layers, 1, d_model), F32), pltpu.VMEM((n_layers, 1, d_model), F32),
            pltpu.VMEM((n_layers, 1, ff), F32), pltpu.VMEM((n_layers, 1, d_model), F32),
            dma((n_layers, 6)), dma((n_chunks,)), dma((2, 2)), dma((2, 2)), dma((n_chunks,)), dma((10, 2)), dma((10, 4)),
        ],
        compiler_params=pltpu.CompilerParams(collective_id=0, has_side_effects=True, vmem_limit_bytes=60 * 1024 * 1024),
        name="decode",
    )(x_steps, k_cache.reshape(flat), v_cache.reshape(flat), w_q, w_k, w_v, w_o, w_in, w_out,
      cur_len, inv_freq, cos_t, sin_t, ln_gain, ln_bias, b_in, b_out)

    pairs = n_layers * batch
    n_blocks = 16
    lines = (pairs, cache_len, n_heads, head_dim)
    new = (pairs, steps, n_heads, head_dim)
    hidden, k_out, v_out = pl.pallas_call(
        functools.partial(merge_kernel, n_blocks),
        out_shape=(jax.ShapeDtypeStruct(x_steps.shape, BF16),) + (jax.ShapeDtypeStruct(lines, BF16),) * 2,
        in_specs=[pl.BlockSpec(memory_space=pltpu.SMEM)] + [any_spec] * 5,
        out_specs=(any_spec,) * 3,
        scratch_shapes=[pltpu.VMEM(x_steps.shape, BF16), pltpu.VMEM(lines, BF16), pltpu.VMEM(lines, BF16),
                        pltpu.VMEM(new, BF16), pltpu.VMEM(new, BF16), dma((5, n_blocks)), dma((3, n_blocks))],
        compiler_params=pltpu.CompilerParams(vmem_limit_bytes=62 * 1024 * 1024),
        name="merge",
    )(cur_len, hidden, k_cache.reshape(lines), v_cache.reshape(lines), rec_k.reshape(new), rec_v.reshape(new))
    return hidden, k_out.reshape(k_cache.shape), v_out.reshape(v_cache.shape)


def solution(mesh):
    cache_spec = P(None, "dp", None, "tp", None)
    in_specs = (P(None, "dp", None), P("dp"), cache_spec, cache_spec, P(None, None), P(None, None),
                P(None, None, "tp"), P(None, None, "tp"), P(None, None, "tp"), P(None, "tp", None),
                P(None, None, "tp"), P(None, "tp"), P(None, "tp", None), P(None, None))
    out_specs = (P(None, "dp", None), cache_spec, cache_spec)
    return jax.shard_map(decode_shard, mesh=mesh, in_specs=in_specs, out_specs=out_specs, check_vma=False)
```

```python
import functools

import jax
import jax.numpy as jnp
import numpy as np
from jax import lax
from jax.experimental import pallas as pl
from jax.experimental.pallas import tpu as pltpu
from jax.sharding import PartitionSpec as P

ROT_DIM = 64
LN_EPS = 1e-5
MESH = pl.DeviceIdType.MESH
F32 = jnp.float32
BF16 = jnp.bfloat16
SEQS = 8
OLD = 96


def decode_kernel(n_chunks, n_stages, x_hbm, k_hbm, v_hbm, wq_hbm, wk_hbm, wv_hbm, wo_hbm, win_hbm, wout_hbm,
                  lens_in, inv_freq, cos_t, sin_t, gain_in, bias_in, b_in_in, b_out_in,
                  out_hbm, rec_k, rec_v,
                  wq, wk, wv, wo, win, wout, hid, part, recv0, sum0, recv1, sum1, recv2,
                  normed, qf, kf, vf, cf, ctx, act, inter, scores, key_scr, kbuf, vbuf,
                  lens, cos_c, sin_c, gain, bias, b_in, b_out,
                  w_sem, x_sem, kv_sem, rec_sem, out_sem, send_sem, recv_sem):
    steps = x_hbm.shape[0]
    rows = steps * SEQS
    ff = win_hbm.shape[2]
    half, quarter, eighth, last = steps // 2, steps // 4, steps // 8, steps // 16
    d_model = x_hbm.shape[2]
    me = lax.axis_index("tp")
    core = lax.rem(me, 2)
    px = lax.rem(lax.div(me, 2), 2)
    py = lax.div(me, 4)
    partner = me + 1 - 2 * core
    x_peer = me + 2 * (1 - 2 * px)
    y_peer = me + 4 * (1 - 2 * py)
    first, second = (x_peer, y_peer), (y_peer, x_peer)
    pos1, pos2 = (px, py), (py, px)
    base = half * core
    base1 = [base + quarter * j + eighth * pos1[j] for j in range(2)]
    base2 = [base1[j] + last * pos2[j] for j in range(2)]

    weight_pairs = ((wq_hbm, wq), (wk_hbm, wk), (wv_hbm, wv), (win_hbm, win), (wo_hbm, wo), (wout_hbm, wout))

    def weight_copy(layer, j):
        src, dst = weight_pairs[j]
        return pltpu.make_async_copy(src.at[layer], dst.at[layer], w_sem.at[layer, j])

    def x_copy(chunk):
        return pltpu.make_async_copy(x_hbm.at[:, pl.ds(pl.multiple_of(chunk * SEQS, SEQS), SEQS), :], hid.at[chunk], x_sem.at[chunk])

    def out_copy(chunk):
        return pltpu.make_async_copy(hid.at[chunk], out_hbm.at[:, pl.ds(pl.multiple_of(chunk * SEQS, SEQS), SEQS), :], out_sem.at[chunk])

    def kv_copies(stage):
        layer, chunk, slot = lax.div(stage, n_chunks), lax.rem(stage, n_chunks), lax.rem(stage, 2)
        seqs = pl.ds(chunk * SEQS, SEQS)
        return (pltpu.make_async_copy(k_hbm.at[layer, seqs], kbuf.at[slot], kv_sem.at[0, slot]),
                pltpu.make_async_copy(v_hbm.at[layer, seqs], vbuf.at[slot], kv_sem.at[1, slot]))

    def rec_copies(stage):
        layer, chunk, slot = lax.div(stage, n_chunks), lax.rem(stage, n_chunks), lax.rem(stage, 2)
        seqs = pl.ds(chunk * SEQS, SEQS)
        new = pl.ds(2 * OLD, 2 * steps)
        return (pltpu.make_async_copy(kbuf.at[slot, :, new, :], rec_k.at[layer, seqs], rec_sem.at[0, slot]),
                pltpu.make_async_copy(vbuf.at[slot, :, new, :], rec_v.at[layer, seqs], rec_sem.at[1, slot]))

    def remote(kind, stage, src, dst, peer):
        return pltpu.make_async_remote_copy(src_ref=src, dst_ref=dst, send_sem=send_sem.at[kind, lax.rem(stage, 2)],
                                            recv_sem=recv_sem.at[kind, lax.rem(stage, 4)], device_id={"tp": peer}, device_id_type=MESH)

    def phase0(stage):
        return remote(0, stage, part.at[pl.ds(half - base, half)], recv0.at[lax.rem(stage, 2)], partner)

    def phase1(stage, j):
        block = pl.ds(quarter * j + eighth * (1 - pos1[j]), eighth)
        return remote(1 + j, stage, sum0.at[lax.rem(stage, 2), block], recv1.at[lax.rem(stage, 4), pl.ds(eighth * j, eighth)], first[j])

    def phase2(stage, j):
        block = pl.ds(eighth * j + last * (1 - pos2[j]), last)
        return remote(3 + j, stage, sum1.at[lax.rem(stage, 2), block], recv2.at[lax.rem(stage, 4), pl.ds(last * j, last)], second[j])

    def gather(kind, stage, start, size, peer):
        block = hid.at[lax.rem(stage, n_chunks), pl.ds(start, size)]
        return remote(kind, stage, block, block, peer)

    def phase3(stage, j):
        return gather(5 + j, stage, base2[j], last, second[j])

    def phase4(stage, j):
        return gather(7 + j, stage, base1[j], eighth, first[j])

    def phase5(stage):
        return gather(9, stage, base, half, partner)

    barrier = pltpu.get_barrier_semaphore()
    for peer in (partner, x_peer, y_peer):
        pl.semaphore_signal(barrier, inc=1, device_id={"tp": peer}, device_id_type=MESH)
    x_copy(0).start()
    for j in range(3):
        weight_copy(0, j).start()
    for b in range(lens.shape[0]):
        lens[b:b + 1, :] = jnp.full((1, lens.shape[1]), lens_in[b], jnp.int32)
    angles = lens[:, 0:128].astype(F32) * inv_freq[...]
    odd = lax.rem(lax.broadcasted_iota(jnp.int32, angles.shape, 1), 2) == 1
    cos_c[...] = jnp.cos(angles)
    sin_c[...] = jnp.where(odd, jnp.sin(angles), -jnp.sin(angles))
    for src, dst in ((gain_in, gain), (bias_in, bias), (b_in_in, b_in), (b_out_in, b_out)):
        for layer in range(src.shape[0]):
            dst[layer] = src[layer:layer + 1, :].astype(F32)

    def norm_rows(stage, start, count):
        layer, chunk, slot = lax.div(stage, n_chunks), lax.rem(stage, n_chunks), lax.rem(stage, 2)
        for k in range(0, count, 2):
            x = hid[chunk, pl.ds(start + k, 2)].astype(F32)
            centered = x - jnp.mean(x, axis=-1, keepdims=True)
            var = jnp.mean(centered * centered, axis=-1, keepdims=True)
            y = centered * lax.rsqrt(var + LN_EPS) * gain[layer][None] + bias[layer][None]
            normed[slot, pl.ds((start + k) * SEQS if isinstance(start, int) else pl.multiple_of((start + k) * SEQS, 2 * SEQS), 2 * SEQS), pl.ds(0, d_model)] = y.reshape(2 * SEQS, d_model).astype(BF16)

    def project_in(stage, layer, chunk):
        @pl.when(chunk == 0)
        def _():
            for j in range(3):
                weight_copy(layer, j).wait()

        here = pl.ds(pl.multiple_of(chunk * SEQS, SEQS), SEQS)
        cc, sc = cos_c[here, :][None], sin_c[here, :][None]
        ct, st = cos_t[...], sin_t[...]
        cos = (cc * ct - sc * st).reshape(rows, 128)
        sin = (sc * ct + cc * st).reshape(rows, 128)
        even = lax.rem(lax.broadcasted_iota(jnp.int32, (rows, 128), 1), 2) == 0

        for weight, dst, rotate in ((wq, qf, True), (wk, kf, True), (wv, vf, False)):
            vec = jnp.dot(normed[lax.rem(stage, 2), :, pl.ds(0, d_model)], weight[layer], preferred_element_type=F32)
            for h in range(2):
                piece = vec[:, h * 128:(h + 1) * 128]
                if rotate:
                    swapped = jnp.where(even, pltpu.roll(piece, 127, 1), pltpu.roll(piece, 1, 1))
                    piece = piece * cos + swapped * sin
                dst[h] = piece

    def attend(stage, layer, chunk):
        slot = lax.rem(stage, 2)
        for copy in kv_copies(stage):
            copy.wait()

        @pl.when(chunk == 0)
        def _():
            for j in range(3, 6):
                weight_copy(layer, j).wait()

        shape = (2 * steps, 2 * (OLD + steps))
        row, col = lax.broadcasted_iota(jnp.int32, shape, 0), lax.broadcasted_iota(jnp.int32, shape, 1)
        col_slot, col_head = lax.shift_right_logical(col, 1), lax.bitwise_and(col, 1)
        row_head, row_step = lax.div(row, steps), lax.rem(row, steps)
        never = 1 << 20
        fresh = jnp.where(col_slot - OLD <= row_step, -1, never)
        key_scr[...] = jnp.where(row_head == col_head, jnp.where(col_slot >= OLD, fresh, col_slot), never)
        limit = lens[pl.ds(pl.multiple_of(chunk * SEQS, SEQS), SEQS), :]
        for b in range(SEQS):
            mine = pl.ds(b, steps, stride=SEQS)
            for src, buf, j in ((kf, kbuf, 0), (vf, vbuf, 1)):
                for h in range(2):
                    inter[b, j, pl.ds(h, steps, stride=2), :] = src[h, mine, :]
                buf[slot, b, pl.ds(2 * OLD, 2 * steps), :] = inter[b, j].astype(BF16)
        for b in range(SEQS):
            mine = pl.ds(b, steps, stride=SEQS)
            query = jnp.concatenate([qf[0, mine, :], qf[1, mine, :]], axis=0).astype(BF16)
            s = lax.dot_general(query, kbuf[slot, b], (((1,), (1,)), ((), ())), preferred_element_type=F32) * (128 ** -0.5)
            scores[b] = jnp.where(key_scr[...] < limit[b:b + 1, :], s, -jnp.inf)
        for b in range(SEQS):
            s = scores[b]
            e = jnp.exp(s - jnp.max(s, axis=-1, keepdims=True))
            probs = (e * (1.0 / jnp.sum(e, axis=-1, keepdims=True))).astype(BF16)
            context = jnp.dot(probs, vbuf[slot, b], preferred_element_type=F32)
            for h in range(2):
                cf[h, pl.ds(b, steps, stride=SEQS), :] = context[h * steps:(h + 1) * steps]

        for copy in rec_copies(stage):
            copy.start()

    def feed_forward(stage, layer):
        slot = lax.rem(stage, 2)
        for n in range(ff // 256):
            cols = pl.ds(n * 256, 256)
            pre = jnp.dot(normed[slot, :, pl.ds(0, d_model)], win[layer, :, cols], preferred_element_type=F32) + b_in[layer, :, cols]
            act[:, cols] = jax.nn.gelu(pre, approximate=True).astype(BF16)

    def project_out(stage, layer):
        for h in range(2):
            ctx[:, h * 128:(h + 1) * 128] = cf[h].astype(BF16)

        following = jnp.minimum(stage + 1, n_stages - 1)
        group = steps // (d_model // 256)

        @pl.when(stage + 1 < n_chunks)
        def _():
            x_copy(stage + 1).wait()

        for n in range(d_model // 256):
            cols = pl.ds(n * 256, 256)
            total = jnp.dot(ctx[...], wo[layer, :, cols], preferred_element_type=F32)
            total += jnp.dot(act[:, pl.ds(0, ff)], wout[layer, :, cols], preferred_element_type=F32)
            part[:, :, cols] = total.reshape(steps, SEQS, 256).astype(BF16)
            norm_rows(following, n * group, group)

    x_copy(0).wait()
    for copy in kv_copies(0):
        copy.start()
    for j in range(3, 6):
        weight_copy(0, j).start()
    x_copy(1).start()

    @pl.loop(0, steps // 8)
    def _(g):
        norm_rows(0, g * 8, 8)

    pl.semaphore_wait(barrier, 3)

    def between(i, lag):
        return jnp.logical_and(i >= lag, i < n_stages + lag)

    @pl.loop(0, n_stages + 5)
    def _(i):
        layer, chunk = lax.div(i, n_chunks), lax.rem(i, n_chunks)
        live = i < n_stages

        @pl.when(i + 2 < n_chunks)
        def _():
            x_copy(i + 2).start()

        for j in range(6):
            @pl.when(i == j + 1)
            def _():
                weight_copy(1, j).start()

        @pl.when(live)
        def _():
            project_in(i, layer, chunk)

        @pl.when(between(i, 2))
        def _():
            s = i - 2
            for j in range(2):
                phase1(s, j).wait()
                mine = pl.ds(quarter * j + eighth * pos1[j], eighth)
                ts = pl.ds(eighth * j, eighth)
                sum1[lax.rem(s, 2), ts] = sum0[lax.rem(s, 2), mine] + recv1[lax.rem(s, 4), ts]
                phase2(s, j).start()

        @pl.when(between(i, 5))
        def _():
            s = i - 5
            phase5(s).wait()

            @pl.when(s >= n_stages - n_chunks)
            def _():
                out_copy(lax.rem(s, n_chunks)).start()

        @pl.when(live)
        def _():
            @pl.when(i >= 1)
            def _():
                for copy in rec_copies(i - 1):
                    copy.wait()

            @pl.when(i + 1 < n_stages)
            def _():
                for copy in kv_copies(i + 1):
                    copy.start()

            attend(i, layer, chunk)

        @pl.when(between(i, 1))
        def _():
            s = i - 1
            phase0(s).wait()
            for j in range(2):
                @pl.loop(0, quarter // 4)
                def _(g):
                    ts = pl.ds(quarter * j + g * 4, 4)
                    sum0[lax.rem(s, 2), ts] = part[pl.ds(base + quarter * j + g * 4, 4)] + recv0[lax.rem(s, 2), ts]

                phase1(s, j).start()

        @pl.when(live)
        def _():
            feed_forward(i, layer)

        @pl.when(between(i, 3))
        def _():
            for j in range(2):
                phase3(i - 3, j).wait()
                phase4(i - 3, j).start()

        @pl.when(between(i, 4))
        def _():
            for j in range(2):
                phase4(i - 4, j).wait()
            phase5(i - 4).start()

        @pl.when(live)
        def _():
            project_out(i, layer)
            phase0(i).start()

        @pl.when(between(i, 2))
        def _():
            s = i - 2
            where = lax.rem(s, n_chunks)
            for j in range(2):
                phase2(s, j).wait()
                own = pl.ds(base2[j], last)
                total = sum1[lax.rem(s, 2), pl.ds(eighth * j + last * pos2[j], last)].astype(F32) + recv2[lax.rem(s, 4), pl.ds(last * j, last)].astype(F32)
                total = total + hid[where, own].astype(F32) + b_out[lax.div(s, n_chunks)][None]
                hid[where, own] = total.astype(BF16)
                phase3(s, j).start()

    for copy in rec_copies(n_stages - 1):
        copy.wait()
    for chunk in range(n_chunks):
        out_copy(chunk).wait()


def merge_kernel(n_blocks, lens, hid_in, k_hbm, v_hbm, rec_k, rec_v, hid_out, k_out, v_out, hbuf, kbuf, vbuf, rk, rv, in_sem, out_sem):
    size = kbuf.shape[0] // n_blocks
    steps = rk.shape[1]

    def block(ref, i):
        rows = ref.shape[0] // n_blocks
        return ref.at[pl.ds(i * rows, rows)]

    def loads(i):
        pairs = ((k_hbm, kbuf), (v_hbm, vbuf), (rec_k, rk), (rec_v, rv), (hid_in, hbuf))
        return [pltpu.make_async_copy(block(src, i), block(dst, i), in_sem.at[j, i]) for j, (src, dst) in enumerate(pairs)]

    def stores(i):
        pairs = ((kbuf, k_out), (vbuf, v_out), (hbuf, hid_out))
        return [pltpu.make_async_copy(block(src, i), block(dst, i), out_sem.at[j, i]) for j, (src, dst) in enumerate(pairs)]

    for i in range(n_blocks):
        for copy in loads(i):
            copy.start()

    @pl.loop(0, n_blocks)
    def _(i):
        for copy in loads(i):
            copy.wait()
        for b in range(size):
            row = i * size + b
            at = lens[lax.rem(row, lens.shape[0])]
            kbuf[row, pl.ds(at, steps)] = rk[row]
            vbuf[row, pl.ds(at, steps)] = rv[row]
        for copy in stores(i):
            copy.start()

    for i in range(n_blocks):
        for copy in stores(i):
            copy.wait()


def inverse_frequencies():
    lane = np.arange(128)
    return np.where(lane < ROT_DIM, 1.0 / (10000.0 ** ((lane // 2 * 2) / ROT_DIM)), 0.0)


def decode_shard(x_steps, cur_len, k_cache, v_cache, ln_gain, ln_bias, w_q, w_k, w_v, w_o, w_in, b_in, w_out, b_out):
    n_layers, batch, cache_len, n_heads, head_dim = k_cache.shape
    steps, _, d_model = x_steps.shape
    ff = w_in.shape[2]
    n_chunks = batch // SEQS
    n_stages = n_layers * n_chunks
    rows = steps * SEQS
    flat = (n_layers, batch, cache_len * n_heads, head_dim)
    step_angles = np.arange(steps)[:, None] * inverse_frequencies()[None, :]
    signed = np.where(np.arange(128) % 2 == 0, -1.0, 1.0)
    cos_t, sin_t = (np.repeat(tab.astype(np.float32)[:, None, :], SEQS, axis=1) for tab in (np.cos(step_angles), np.sin(step_angles) * signed))
    inv_freq = inverse_frequencies().astype(np.float32)[None, :]
    any_spec, vmem = pl.BlockSpec(memory_space=pl.ANY), pl.BlockSpec(memory_space=pltpu.VMEM)
    dma = pltpu.SemaphoreType.DMA
    block = (steps, SEQS, d_model)
    hidden, rec_k, rec_v = pl.pallas_call(
        functools.partial(decode_kernel, n_chunks, n_stages),
        out_shape=(jax.ShapeDtypeStruct(x_steps.shape, BF16),
                   jax.ShapeDtypeStruct((n_layers, batch, steps * n_heads, head_dim), BF16),
                   jax.ShapeDtypeStruct((n_layers, batch, steps * n_heads, head_dim), BF16)),
        in_specs=[any_spec] * 9 + [pl.BlockSpec(memory_space=pltpu.SMEM)] + [vmem] * 7,
        out_specs=(any_spec,) * 3,
        scratch_shapes=[
            pltpu.VMEM(w_q.shape, BF16), pltpu.VMEM(w_k.shape, BF16), pltpu.VMEM(w_v.shape, BF16), pltpu.VMEM(w_o.shape, BF16),
            pltpu.VMEM(w_in.shape, BF16), pltpu.VMEM(w_out.shape, BF16),
            pltpu.VMEM((n_chunks,) + block, BF16), pltpu.VMEM(block, BF16),
            pltpu.VMEM((2, steps // 2, SEQS, d_model), BF16), pltpu.VMEM((2, steps // 2, SEQS, d_model), BF16),
            pltpu.VMEM((4, steps // 4, SEQS, d_model), BF16), pltpu.VMEM((2, steps // 4, SEQS, d_model), BF16),
            pltpu.VMEM((4, steps // 8, SEQS, d_model), BF16),
            pltpu.VMEM((2, rows, d_model + 128), BF16),
            pltpu.VMEM((2, rows, 128), F32), pltpu.VMEM((2, rows, 128), F32), pltpu.VMEM((2, rows, 128), F32), pltpu.VMEM((2, rows, 128), F32),
            pltpu.VMEM((rows, 256), BF16), pltpu.VMEM((rows, ff + 128), BF16),
            pltpu.VMEM((SEQS, 2, 2 * steps, 128), F32), pltpu.VMEM((SEQS, 2 * steps, 256), F32), pltpu.VMEM((2 * steps, 256), jnp.int32),
            pltpu.VMEM((2, SEQS, 256, 128), BF16), pltpu.VMEM((2, SEQS, 256, 128), BF16),
            pltpu.VMEM((batch, cache_len * n_heads), jnp.int32), pltpu.VMEM((batch, 128), F32), pltpu.VMEM((batch, 128), F32),
            pltpu.VMEM((n_layers, 1, d_model), F32), pltpu.VMEM((n_layers, 1, d_model), F32),
            pltpu.VMEM((n_layers, 1, ff), F32), pltpu.VMEM((n_layers, 1, d_model), F32),
            dma((n_layers, 6)), dma((n_chunks,)), dma((2, 2)), dma((2, 2)), dma((n_chunks,)), dma((10, 2)), dma((10, 4)),
        ],
        compiler_params=pltpu.CompilerParams(collective_id=0, has_side_effects=True, vmem_limit_bytes=60 * 1024 * 1024),
        name="decode",
    )(x_steps, k_cache.reshape(flat), v_cache.reshape(flat), w_q, w_k, w_v, w_o, w_in, w_out,
      cur_len, inv_freq, cos_t, sin_t, ln_gain, ln_bias, b_in, b_out)

    pairs = n_layers * batch
    n_blocks = 16
    lines = (pairs, cache_len, n_heads, head_dim)
    new = (pairs, steps, n_heads, head_dim)
    hidden, k_out, v_out = pl.pallas_call(
        functools.partial(merge_kernel, n_blocks),
        out_shape=(jax.ShapeDtypeStruct(x_steps.shape, BF16),) + (jax.ShapeDtypeStruct(lines, BF16),) * 2,
        in_specs=[pl.BlockSpec(memory_space=pltpu.SMEM)] + [any_spec] * 5,
        out_specs=(any_spec,) * 3,
        scratch_shapes=[pltpu.VMEM(x_steps.shape, BF16), pltpu.VMEM(lines, BF16), pltpu.VMEM(lines, BF16),
                        pltpu.VMEM(new, BF16), pltpu.VMEM(new, BF16), dma((5, n_blocks)), dma((3, n_blocks))],
        compiler_params=pltpu.CompilerParams(vmem_limit_bytes=62 * 1024 * 1024),
        name="merge",
    )(cur_len, hidden, k_cache.reshape(lines), v_cache.reshape(lines), rec_k.reshape(new), rec_v.reshape(new))
    return hidden, k_out.reshape(k_cache.shape), v_out.reshape(v_cache.shape)


def solution(mesh):
    cache_spec = P(None, "dp", None, "tp", None)
    in_specs = (P(None, "dp", None), P("dp"), cache_spec, cache_spec, P(None, None), P(None, None),
                P(None, None, "tp"), P(None, None, "tp"), P(None, None, "tp"), P(None, "tp", None),
                P(None, None, "tp"), P(None, "tp"), P(None, "tp", None), P(None, None))
    out_specs = (P(None, "dp", None), cache_spec, cache_spec)
    return jax.shard_map(decode_shard, mesh=mesh, in_specs=in_specs, out_specs=out_specs, check_vma=False)
```

```python
import functools

import jax
import jax.numpy as jnp
import numpy as np
from jax import lax
from jax.experimental import pallas as pl
from jax.experimental.pallas import tpu as pltpu
from jax.sharding import PartitionSpec as P

ROT_DIM = 64
LN_EPS = 1e-5
MESH = pl.DeviceIdType.MESH
F32 = jnp.float32
BF16 = jnp.bfloat16
SEQS = 8
OLD = 96


def decode_kernel(n_chunks, n_stages, x_hbm, k_hbm, v_hbm, wq_hbm, wk_hbm, wv_hbm, wo_hbm, win_hbm, wout_hbm,
                  lens_in, inv_freq, cos_t, sin_t, gain_in, bias_in, b_in_in, b_out_in,
                  out_hbm, rec_k, rec_v,
                  wq, wk, wv, wo, win, wout, hid, part, recv0, sum0, recv1, sum1, recv2,
                  normed, qf, kf, vf, cf, ctx, act, inter, scores, key_scr, kbuf, vbuf,
                  lens, cos_c, sin_c, gain, bias, b_in, b_out,
                  w_sem, x_sem, kv_sem, rec_sem, out_sem, send_sem, recv_sem):
    steps = x_hbm.shape[0]
    rows = steps * SEQS
    ff = win_hbm.shape[2]
    half, quarter, eighth, last = steps // 2, steps // 4, steps // 8, steps // 16
    d_model = x_hbm.shape[2]
    me = lax.axis_index("tp")
    core = lax.rem(me, 2)
    px = lax.rem(lax.div(me, 2), 2)
    py = lax.div(me, 4)
    partner = me + 1 - 2 * core
    x_peer = me + 2 * (1 - 2 * px)
    y_peer = me + 4 * (1 - 2 * py)
    first, second = (x_peer, y_peer), (y_peer, x_peer)
    pos1, pos2 = (px, py), (py, px)
    base = half * core
    base1 = [base + quarter * j + eighth * pos1[j] for j in range(2)]
    base2 = [base1[j] + last * pos2[j] for j in range(2)]

    weight_pairs = ((wq_hbm, wq), (wk_hbm, wk), (wv_hbm, wv), (win_hbm, win), (wo_hbm, wo), (wout_hbm, wout))

    def weight_copy(layer, j):
        src, dst = weight_pairs[j]
        return pltpu.make_async_copy(src.at[layer], dst.at[layer], w_sem.at[layer, j])

    def x_copy(chunk):
        return pltpu.make_async_copy(x_hbm.at[:, pl.ds(pl.multiple_of(chunk * SEQS, SEQS), SEQS), :], hid.at[chunk], x_sem.at[chunk])

    def out_copy(chunk):
        return pltpu.make_async_copy(hid.at[chunk], out_hbm.at[:, pl.ds(pl.multiple_of(chunk * SEQS, SEQS), SEQS), :], out_sem.at[chunk])

    def kv_copies(stage):
        layer, chunk, slot = lax.div(stage, n_chunks), lax.rem(stage, n_chunks), lax.rem(stage, 2)
        seqs = pl.ds(chunk * SEQS, SEQS)
        return (pltpu.make_async_copy(k_hbm.at[layer, seqs], kbuf.at[slot], kv_sem.at[0, slot]),
                pltpu.make_async_copy(v_hbm.at[layer, seqs], vbuf.at[slot], kv_sem.at[1, slot]))

    def rec_copies(stage):
        layer, chunk, slot = lax.div(stage, n_chunks), lax.rem(stage, n_chunks), lax.rem(stage, 2)
        seqs = pl.ds(chunk * SEQS, SEQS)
        new = pl.ds(2 * OLD, 2 * steps)
        return (pltpu.make_async_copy(kbuf.at[slot, :, new, :], rec_k.at[layer, seqs], rec_sem.at[0, slot]),
                pltpu.make_async_copy(vbuf.at[slot, :, new, :], rec_v.at[layer, seqs], rec_sem.at[1, slot]))

    def remote(kind, stage, src, dst, peer):
        return pltpu.make_async_remote_copy(src_ref=src, dst_ref=dst, send_sem=send_sem.at[kind, lax.rem(stage, 2)],
                                            recv_sem=recv_sem.at[kind, lax.rem(stage, 4)], device_id={"tp": peer}, device_id_type=MESH)

    def phase0(stage):
        return remote(0, stage, part.at[pl.ds(half - base, half)], recv0.at[lax.rem(stage, 2)], partner)

    def phase1(stage, j):
        block = pl.ds(quarter * j + eighth * (1 - pos1[j]), eighth)
        return remote(1 + j, stage, sum0.at[lax.rem(stage, 2), block], recv1.at[lax.rem(stage, 4), pl.ds(eighth * j, eighth)], first[j])

    def phase2(stage, j):
        block = pl.ds(eighth * j + last * (1 - pos2[j]), last)
        return remote(3 + j, stage, sum1.at[lax.rem(stage, 2), block], recv2.at[lax.rem(stage, 4), pl.ds(last * j, last)], second[j])

    def gather(kind, stage, start, size, peer):
        block = hid.at[lax.rem(stage, n_chunks), pl.ds(start, size)]
        return remote(kind, stage, block, block, peer)

    def phase3(stage, j):
        return gather(5 + j, stage, base2[j], last, second[j])

    def phase4(stage, j):
        return gather(7 + j, stage, base1[j], eighth, first[j])

    def phase5(stage):
        return gather(9, stage, base, half, partner)

    barrier = pltpu.get_barrier_semaphore()
    for peer in (partner, x_peer, y_peer):
        pl.semaphore_signal(barrier, inc=1, device_id={"tp": peer}, device_id_type=MESH)
    x_copy(0).start()
    for j in range(3):
        weight_copy(0, j).start()
    for b in range(lens.shape[0]):
        lens[b:b + 1, :] = jnp.full((1, lens.shape[1]), lens_in[b], jnp.int32)
    angles = lens[:, 0:128].astype(F32) * inv_freq[...]
    odd = lax.rem(lax.broadcasted_iota(jnp.int32, angles.shape, 1), 2) == 1
    cos_c[...] = jnp.cos(angles)
    sin_c[...] = jnp.where(odd, jnp.sin(angles), -jnp.sin(angles))
    for src, dst in ((gain_in, gain), (bias_in, bias), (b_in_in, b_in), (b_out_in, b_out)):
        for layer in range(src.shape[0]):
            dst[layer] = src[layer:layer + 1, :].astype(F32)

    def norm_rows(stage, start, count):
        layer, chunk, slot = lax.div(stage, n_chunks), lax.rem(stage, n_chunks), lax.rem(stage, 2)
        for k in range(0, count, 2):
            x = hid[chunk, pl.ds(start + k, 2)].astype(F32)
            centered = x - jnp.mean(x, axis=-1, keepdims=True)
            var = jnp.mean(centered * centered, axis=-1, keepdims=True)
            y = centered * lax.rsqrt(var + LN_EPS) * gain[layer][None] + bias[layer][None]
            normed[slot, pl.ds((start + k) * SEQS if isinstance(start, int) else pl.multiple_of((start + k) * SEQS, 2 * SEQS), 2 * SEQS), pl.ds(0, d_model)] = y.reshape(2 * SEQS, d_model).astype(BF16)

    def project_in(stage, layer, chunk):
        @pl.when(chunk == 0)
        def _():
            for j in range(3):
                weight_copy(layer, j).wait()

        here = pl.ds(pl.multiple_of(chunk * SEQS, SEQS), SEQS)
        cc, sc = cos_c[here, :][None], sin_c[here, :][None]
        ct, st = cos_t[...], sin_t[...]
        cos = (cc * ct - sc * st).reshape(rows, 128)
        sin = (sc * ct + cc * st).reshape(rows, 128)
        even = lax.rem(lax.broadcasted_iota(jnp.int32, (rows, 128), 1), 2) == 0

        for weight, dst, rotate in ((wq, qf, True), (wk, kf, True), (wv, vf, False)):
            vec = jnp.dot(normed[lax.rem(stage, 2), :, pl.ds(0, d_model)], weight[layer], preferred_element_type=F32)
            for h in range(2):
                piece = vec[:, h * 128:(h + 1) * 128]
                if rotate:
                    swapped = jnp.where(even, pltpu.roll(piece, 127, 1), pltpu.roll(piece, 1, 1))
                    piece = piece * cos + swapped * sin
                dst[h] = piece

    def attend(stage, layer, chunk):
        slot = lax.rem(stage, 2)
        for copy in kv_copies(stage):
            copy.wait()

        @pl.when(chunk == 0)
        def _():
            for j in range(3, 6):
                weight_copy(layer, j).wait()

        shape = (2 * steps, 2 * (OLD + steps))
        row, col = lax.broadcasted_iota(jnp.int32, shape, 0), lax.broadcasted_iota(jnp.int32, shape, 1)
        col_slot, col_head = lax.shift_right_logical(col, 1), lax.bitwise_and(col, 1)
        row_head, row_step = lax.div(row, steps), lax.rem(row, steps)
        never = 1 << 20
        fresh = jnp.where(col_slot - OLD <= row_step, -1, never)
        key_scr[...] = jnp.where(row_head == col_head, jnp.where(col_slot >= OLD, fresh, col_slot), never)
        limit = lens[pl.ds(pl.multiple_of(chunk * SEQS, SEQS), SEQS), :]
        for b in range(SEQS):
            mine = pl.ds(b, steps, stride=SEQS)
            for src, buf, j in ((kf, kbuf, 0), (vf, vbuf, 1)):
                for h in range(2):
                    inter[b, j, pl.ds(h, steps, stride=2), :] = src[h, mine, :]
                buf[slot, b, pl.ds(2 * OLD, 2 * steps), :] = inter[b, j].astype(BF16)
        for b in range(SEQS):
            mine = pl.ds(b, steps, stride=SEQS)
            query = jnp.concatenate([qf[0, mine, :], qf[1, mine, :]], axis=0).astype(BF16)
            s = lax.dot_general(query, kbuf[slot, b], (((1,), (1,)), ((), ())), preferred_element_type=F32) * (128 ** -0.5)
            scores[b] = jnp.where(key_scr[...] < limit[b:b + 1, :], s, -jnp.inf)
        for b in range(SEQS):
            s = scores[b]
            e = jnp.exp(s - jnp.max(s, axis=-1, keepdims=True))
            probs = (e * (1.0 / jnp.sum(e, axis=-1, keepdims=True))).astype(BF16)
            context = jnp.dot(probs, vbuf[slot, b], preferred_element_type=F32)
            for h in range(2):
                cf[h, pl.ds(b, steps, stride=SEQS), :] = context[h * steps:(h + 1) * steps]

        for copy in rec_copies(stage):
            copy.start()

    def feed_forward(stage, layer):
        slot = lax.rem(stage, 2)
        for n in range(ff // 256):
            cols = pl.ds(n * 256, 256)
            pre = jnp.dot(normed[slot, :, pl.ds(0, d_model)], win[layer, :, cols], preferred_element_type=F32) + b_in[layer, :, cols]
            act[:, cols] = jax.nn.gelu(pre, approximate=True).astype(BF16)

    def project_out(stage, layer):
        for h in range(2):
            ctx[:, h * 128:(h + 1) * 128] = cf[h].astype(BF16)

        following = jnp.minimum(stage + 1, n_stages - 1)
        group = steps // (d_model // 256)

        @pl.when(stage + 1 < n_chunks)
        def _():
            x_copy(stage + 1).wait()

        for n in range(d_model // 256):
            cols = pl.ds(n * 256, 256)
            total = jnp.dot(ctx[...], wo[layer, :, cols], preferred_element_type=F32)
            total += jnp.dot(act[:, pl.ds(0, ff)], wout[layer, :, cols], preferred_element_type=F32)
            part[:, :, cols] = total.reshape(steps, SEQS, 256).astype(BF16)
            norm_rows(following, n * group, group)

    x_copy(0).wait()
    for copy in kv_copies(0):
        copy.start()
    for j in range(3, 6):
        weight_copy(0, j).start()
    x_copy(1).start()

    @pl.loop(0, steps // 8)
    def _(g):
        norm_rows(0, g * 8, 8)

    pl.semaphore_wait(barrier, 3)

    def between(i, lag):
        return jnp.logical_and(i >= lag, i < n_stages + lag)

    @pl.loop(0, n_stages + 5)
    def _(i):
        layer, chunk = lax.div(i, n_chunks), lax.rem(i, n_chunks)
        live = i < n_stages

        @pl.when(i + 2 < n_chunks)
        def _():
            x_copy(i + 2).start()

        for j in range(6):
            @pl.when(i == j + 1)
            def _():
                weight_copy(1, j).start()

        @pl.when(live)
        def _():
            project_in(i, layer, chunk)

        @pl.when(between(i, 1))
        def _():
            s = i - 1
            phase0(s).wait()
            for j in range(2):
                @pl.loop(0, quarter // 4)
                def _(g):
                    ts = pl.ds(quarter * j + g * 4, 4)
                    sum0[lax.rem(s, 2), ts] = part[pl.ds(base + quarter * j + g * 4, 4)] + recv0[lax.rem(s, 2), ts]

                phase1(s, j).start()

        @pl.when(between(i, 2))
        def _():
            s = i - 2
            for j in range(2):
                phase1(s, j).wait()
                mine = pl.ds(quarter * j + eighth * pos1[j], eighth)
                ts = pl.ds(eighth * j, eighth)
                sum1[lax.rem(s, 2), ts] = sum0[lax.rem(s, 2), mine] + recv1[lax.rem(s, 4), ts]
                phase2(s, j).start()

        @pl.when(between(i, 5))
        def _():
            s = i - 5
            phase5(s).wait()

            @pl.when(s >= n_stages - n_chunks)
            def _():
                out_copy(lax.rem(s, n_chunks)).start()

        @pl.when(live)
        def _():
            @pl.when(i >= 1)
            def _():
                for copy in rec_copies(i - 1):
                    copy.wait()

            @pl.when(i + 1 < n_stages)
            def _():
                for copy in kv_copies(i + 1):
                    copy.start()

            attend(i, layer, chunk)

        @pl.when(live)
        def _():
            feed_forward(i, layer)

        @pl.when(between(i, 3))
        def _():
            for j in range(2):
                phase3(i - 3, j).wait()
                phase4(i - 3, j).start()

        @pl.when(between(i, 4))
        def _():
            for j in range(2):
                phase4(i - 4, j).wait()
            phase5(i - 4).start()

        @pl.when(live)
        def _():
            project_out(i, layer)
            phase0(i).start()

        @pl.when(between(i, 2))
        def _():
            s = i - 2
            where = lax.rem(s, n_chunks)
            for j in range(2):
                phase2(s, j).wait()
                own = pl.ds(base2[j], last)
                total = sum1[lax.rem(s, 2), pl.ds(eighth * j + last * pos2[j], last)].astype(F32) + recv2[lax.rem(s, 4), pl.ds(last * j, last)].astype(F32)
                total = total + hid[where, own].astype(F32) + b_out[lax.div(s, n_chunks)][None]
                hid[where, own] = total.astype(BF16)
                phase3(s, j).start()

    for copy in rec_copies(n_stages - 1):
        copy.wait()
    for chunk in range(n_chunks):
        out_copy(chunk).wait()


def merge_kernel(n_blocks, lens, hid_in, k_hbm, v_hbm, rec_k, rec_v, hid_out, k_out, v_out, hbuf, kbuf, vbuf, rk, rv, in_sem, out_sem):
    size = kbuf.shape[0] // n_blocks
    steps = rk.shape[1]

    def block(ref, i):
        rows = ref.shape[0] // n_blocks
        return ref.at[pl.ds(i * rows, rows)]

    def loads(i):
        pairs = ((k_hbm, kbuf), (v_hbm, vbuf), (rec_k, rk), (rec_v, rv), (hid_in, hbuf))
        return [pltpu.make_async_copy(block(src, i), block(dst, i), in_sem.at[j, i]) for j, (src, dst) in enumerate(pairs)]

    def stores(i):
        pairs = ((kbuf, k_out), (vbuf, v_out), (hbuf, hid_out))
        return [pltpu.make_async_copy(block(src, i), block(dst, i), out_sem.at[j, i]) for j, (src, dst) in enumerate(pairs)]

    for i in range(n_blocks):
        for copy in loads(i):
            copy.start()

    @pl.loop(0, n_blocks)
    def _(i):
        for copy in loads(i):
            copy.wait()
        for b in range(size):
            row = i * size + b
            at = lens[lax.rem(row, lens.shape[0])]
            kbuf[row, pl.ds(at, steps)] = rk[row]
            vbuf[row, pl.ds(at, steps)] = rv[row]
        for copy in stores(i):
            copy.start()

    for i in range(n_blocks):
        for copy in stores(i):
            copy.wait()


def inverse_frequencies():
    lane = np.arange(128)
    return np.where(lane < ROT_DIM, 1.0 / (10000.0 ** ((lane // 2 * 2) / ROT_DIM)), 0.0)


def decode_shard(x_steps, cur_len, k_cache, v_cache, ln_gain, ln_bias, w_q, w_k, w_v, w_o, w_in, b_in, w_out, b_out):
    n_layers, batch, cache_len, n_heads, head_dim = k_cache.shape
    steps, _, d_model = x_steps.shape
    ff = w_in.shape[2]
    n_chunks = batch // SEQS
    n_stages = n_layers * n_chunks
    rows = steps * SEQS
    flat = (n_layers, batch, cache_len * n_heads, head_dim)
    step_angles = np.arange(steps)[:, None] * inverse_frequencies()[None, :]
    signed = np.where(np.arange(128) % 2 == 0, -1.0, 1.0)
    cos_t, sin_t = (np.repeat(tab.astype(np.float32)[:, None, :], SEQS, axis=1) for tab in (np.cos(step_angles), np.sin(step_angles) * signed))
    inv_freq = inverse_frequencies().astype(np.float32)[None, :]
    any_spec, vmem = pl.BlockSpec(memory_space=pl.ANY), pl.BlockSpec(memory_space=pltpu.VMEM)
    dma = pltpu.SemaphoreType.DMA
    block = (steps, SEQS, d_model)
    hidden, rec_k, rec_v = pl.pallas_call(
        functools.partial(decode_kernel, n_chunks, n_stages),
        out_shape=(jax.ShapeDtypeStruct(x_steps.shape, BF16),
                   jax.ShapeDtypeStruct((n_layers, batch, steps * n_heads, head_dim), BF16),
                   jax.ShapeDtypeStruct((n_layers, batch, steps * n_heads, head_dim), BF16)),
        in_specs=[any_spec] * 9 + [pl.BlockSpec(memory_space=pltpu.SMEM)] + [vmem] * 7,
        out_specs=(any_spec,) * 3,
        scratch_shapes=[
            pltpu.VMEM(w_q.shape, BF16), pltpu.VMEM(w_k.shape, BF16), pltpu.VMEM(w_v.shape, BF16), pltpu.VMEM(w_o.shape, BF16),
            pltpu.VMEM(w_in.shape, BF16), pltpu.VMEM(w_out.shape, BF16),
            pltpu.VMEM((n_chunks,) + block, BF16), pltpu.VMEM(block, BF16),
            pltpu.VMEM((2, steps // 2, SEQS, d_model), BF16), pltpu.VMEM((2, steps // 2, SEQS, d_model), BF16),
            pltpu.VMEM((4, steps // 4, SEQS, d_model), BF16), pltpu.VMEM((2, steps // 4, SEQS, d_model), BF16),
            pltpu.VMEM((4, steps // 8, SEQS, d_model), BF16),
            pltpu.VMEM((2, rows, d_model + 128), BF16),
            pltpu.VMEM((2, rows, 128), F32), pltpu.VMEM((2, rows, 128), F32), pltpu.VMEM((2, rows, 128), F32), pltpu.VMEM((2, rows, 128), F32),
            pltpu.VMEM((rows, 256), BF16), pltpu.VMEM((rows, ff + 128), BF16),
            pltpu.VMEM((SEQS, 2, 2 * steps, 128), F32), pltpu.VMEM((SEQS, 2 * steps, 256), F32), pltpu.VMEM((2 * steps, 256), jnp.int32),
            pltpu.VMEM((2, SEQS, 256, 128), BF16), pltpu.VMEM((2, SEQS, 256, 128), BF16),
            pltpu.VMEM((batch, cache_len * n_heads), jnp.int32), pltpu.VMEM((batch, 128), F32), pltpu.VMEM((batch, 128), F32),
            pltpu.VMEM((n_layers, 1, d_model), F32), pltpu.VMEM((n_layers, 1, d_model), F32),
            pltpu.VMEM((n_layers, 1, ff), F32), pltpu.VMEM((n_layers, 1, d_model), F32),
            dma((n_layers, 6)), dma((n_chunks,)), dma((2, 2)), dma((2, 2)), dma((n_chunks,)), dma((10, 2)), dma((10, 4)),
        ],
        compiler_params=pltpu.CompilerParams(collective_id=0, has_side_effects=True, vmem_limit_bytes=60 * 1024 * 1024),
        name="decode",
    )(x_steps, k_cache.reshape(flat), v_cache.reshape(flat), w_q, w_k, w_v, w_o, w_in, w_out,
      cur_len, inv_freq, cos_t, sin_t, ln_gain, ln_bias, b_in, b_out)

    pairs = n_layers * batch
    n_blocks = 16
    lines = (pairs, cache_len, n_heads, head_dim)
    new = (pairs, steps, n_heads, head_dim)
    hidden, k_out, v_out = pl.pallas_call(
        functools.partial(merge_kernel, n_blocks),
        out_shape=(jax.ShapeDtypeStruct(x_steps.shape, BF16),) + (jax.ShapeDtypeStruct(lines, BF16),) * 2,
        in_specs=[pl.BlockSpec(memory_space=pltpu.SMEM)] + [any_spec] * 5,
        out_specs=(any_spec,) * 3,
        scratch_shapes=[pltpu.VMEM(x_steps.shape, BF16), pltpu.VMEM(lines, BF16), pltpu.VMEM(lines, BF16),
                        pltpu.VMEM(new, BF16), pltpu.VMEM(new, BF16), dma((5, n_blocks)), dma((3, n_blocks))],
        compiler_params=pltpu.CompilerParams(vmem_limit_bytes=62 * 1024 * 1024),
        name="merge",
    )(cur_len, hidden, k_cache.reshape(lines), v_cache.reshape(lines), rec_k.reshape(new), rec_v.reshape(new))
    return hidden, k_out.reshape(k_cache.shape), v_out.reshape(v_cache.shape)


def solution(mesh):
    cache_spec = P(None, "dp", None, "tp", None)
    in_specs = (P(None, "dp", None), P("dp"), cache_spec, cache_spec, P(None, None), P(None, None),
                P(None, None, "tp"), P(None, None, "tp"), P(None, None, "tp"), P(None, "tp", None),
                P(None, None, "tp"), P(None, "tp"), P(None, "tp", None), P(None, None))
    out_specs = (P(None, "dp", None), cache_spec, cache_spec)
    return jax.shard_map(decode_shard, mesh=mesh, in_specs=in_specs, out_specs=out_specs, check_vma=False)
```

```python
import functools

import jax
import jax.numpy as jnp
import numpy as np
from jax import lax
from jax.experimental import pallas as pl
from jax.experimental.pallas import tpu as pltpu
from jax.sharding import PartitionSpec as P

ROT_DIM = 64
LN_EPS = 1e-5
MESH = pl.DeviceIdType.MESH
F32 = jnp.float32
BF16 = jnp.bfloat16
SEQS = 8
OLD = 96


def decode_kernel(n_chunks, n_stages, x_hbm, k_hbm, v_hbm, wq_hbm, wk_hbm, wv_hbm, wo_hbm, win_hbm, wout_hbm,
                  lens_in, inv_freq, cos_t, sin_t, gain_in, bias_in, b_in_in, b_out_in,
                  out_hbm, rec_k, rec_v,
                  wq, wk, wv, wo, win, wout, hid, part, recv0, sum0, recv1, sum1, recv2,
                  normed, qf, kf, vf, cf, ctx, act, inter, scores, key_scr, kbuf, vbuf,
                  lens, cos_c, sin_c, gain, bias, b_in, b_out,
                  w_sem, x_sem, kv_sem, rec_sem, out_sem, send_sem, recv_sem):
    steps = x_hbm.shape[0]
    rows = steps * SEQS
    ff = win_hbm.shape[2]
    half, quarter, eighth, last = steps // 2, steps // 4, steps // 8, steps // 16
    d_model = x_hbm.shape[2]
    me = lax.axis_index("tp")
    core = lax.rem(me, 2)
    px = lax.rem(lax.div(me, 2), 2)
    py = lax.div(me, 4)
    partner = me + 1 - 2 * core
    x_peer = me + 2 * (1 - 2 * px)
    y_peer = me + 4 * (1 - 2 * py)
    first, second = (x_peer, y_peer), (y_peer, x_peer)
    pos1, pos2 = (px, py), (py, px)
    base = half * core
    base1 = [base + quarter * j + eighth * pos1[j] for j in range(2)]
    base2 = [base1[j] + last * pos2[j] for j in range(2)]

    weight_pairs = ((wq_hbm, wq), (wk_hbm, wk), (wv_hbm, wv), (win_hbm, win), (wo_hbm, wo), (wout_hbm, wout))

    def weight_copy(layer, j):
        src, dst = weight_pairs[j]
        return pltpu.make_async_copy(src.at[layer], dst.at[layer], w_sem.at[layer, j])

    def x_copy(chunk):
        return pltpu.make_async_copy(x_hbm.at[:, pl.ds(pl.multiple_of(chunk * SEQS, SEQS), SEQS), :], hid.at[chunk], x_sem.at[chunk])

    def out_copy(chunk):
        return pltpu.make_async_copy(hid.at[chunk], out_hbm.at[:, pl.ds(pl.multiple_of(chunk * SEQS, SEQS), SEQS), :], out_sem.at[chunk])

    def kv_copies(stage):
        layer, chunk, slot = lax.div(stage, n_chunks), lax.rem(stage, n_chunks), lax.rem(stage, 2)
        seqs = pl.ds(chunk * SEQS, SEQS)
        return (pltpu.make_async_copy(k_hbm.at[layer, seqs], kbuf.at[slot], kv_sem.at[0, slot]),
                pltpu.make_async_copy(v_hbm.at[layer, seqs], vbuf.at[slot], kv_sem.at[1, slot]))

    def rec_copies(stage):
        layer, chunk, slot = lax.div(stage, n_chunks), lax.rem(stage, n_chunks), lax.rem(stage, 2)
        seqs = pl.ds(chunk * SEQS, SEQS)
        new = pl.ds(2 * OLD, 2 * steps)
        return (pltpu.make_async_copy(kbuf.at[slot, :, new, :], rec_k.at[layer, seqs], rec_sem.at[0, slot]),
                pltpu.make_async_copy(vbuf.at[slot, :, new, :], rec_v.at[layer, seqs], rec_sem.at[1, slot]))

    def remote(kind, stage, src, dst, peer):
        return pltpu.make_async_remote_copy(src_ref=src, dst_ref=dst, send_sem=send_sem.at[kind, lax.rem(stage, 2)],
                                            recv_sem=recv_sem.at[kind, lax.rem(stage, 4)], device_id={"tp": peer}, device_id_type=MESH)

    def phase0(stage):
        return remote(0, stage, part.at[pl.ds(half - base, half)], recv0.at[lax.rem(stage, 2)], partner)

    def phase1(stage, j):
        block = pl.ds(quarter * j + eighth * (1 - pos1[j]), eighth)
        return remote(1 + j, stage, sum0.at[lax.rem(stage, 2), block], recv1.at[lax.rem(stage, 4), pl.ds(eighth * j, eighth)], first[j])

    def phase2(stage, j):
        block = pl.ds(eighth * j + last * (1 - pos2[j]), last)
        return remote(3 + j, stage, sum1.at[lax.rem(stage, 2), block], recv2.at[lax.rem(stage, 4), pl.ds(last * j, last)], second[j])

    def gather(kind, stage, start, size, peer):
        block = hid.at[lax.rem(stage, n_chunks), pl.ds(start, size)]
        return remote(kind, stage, block, block, peer)

    def phase3(stage, j):
        return gather(5 + j, stage, base2[j], last, second[j])

    def phase4(stage, j):
        return gather(7 + j, stage, base1[j], eighth, first[j])

    def phase5(stage):
        return gather(9, stage, base, half, partner)

    barrier = pltpu.get_barrier_semaphore()
    for peer in (partner, x_peer, y_peer):
        pl.semaphore_signal(barrier, inc=1, device_id={"tp": peer}, device_id_type=MESH)
    x_copy(0).start()
    for j in range(3):
        weight_copy(0, j).start()
    for copy in kv_copies(0):
        copy.start()
    for j in range(3, 6):
        weight_copy(0, j).start()
    x_copy(1).start()
    for b in range(lens.shape[0]):
        lens[b:b + 1, :] = jnp.full((1, lens.shape[1]), lens_in[b], jnp.int32)
    angles = lens[:, 0:128].astype(F32) * inv_freq[...]
    odd = lax.rem(lax.broadcasted_iota(jnp.int32, angles.shape, 1), 2) == 1
    cos_c[...] = jnp.cos(angles)
    sin_c[...] = jnp.where(odd, jnp.sin(angles), -jnp.sin(angles))
    for src, dst in ((gain_in, gain), (bias_in, bias), (b_in_in, b_in), (b_out_in, b_out)):
        for layer in range(src.shape[0]):
            dst[layer] = src[layer:layer + 1, :].astype(F32)

    def norm_rows(stage, start, count):
        layer, chunk, slot = lax.div(stage, n_chunks), lax.rem(stage, n_chunks), lax.rem(stage, 2)
        for k in range(0, count, 2):
            x = hid[chunk, pl.ds(start + k, 2)].astype(F32)
            centered = x - jnp.mean(x, axis=-1, keepdims=True)
            var = jnp.mean(centered * centered, axis=-1, keepdims=True)
            y = centered * lax.rsqrt(var + LN_EPS) * gain[layer][None] + bias[layer][None]
            normed[slot, pl.ds((start + k) * SEQS if isinstance(start, int) else pl.multiple_of((start + k) * SEQS, 2 * SEQS), 2 * SEQS), pl.ds(0, d_model)] = y.reshape(2 * SEQS, d_model).astype(BF16)

    def project_in(stage, layer, chunk):
        @pl.when(chunk == 0)
        def _():
            for j in range(3):
                weight_copy(layer, j).wait()

        here = pl.ds(pl.multiple_of(chunk * SEQS, SEQS), SEQS)
        cc, sc = cos_c[here, :][None], sin_c[here, :][None]
        ct, st = cos_t[...], sin_t[...]
        cos = (cc * ct - sc * st).reshape(rows, 128)
        sin = (sc * ct + cc * st).reshape(rows, 128)
        even = lax.rem(lax.broadcasted_iota(jnp.int32, (rows, 128), 1), 2) == 0

        for weight, dst, rotate in ((wq, qf, True), (wk, kf, True), (wv, vf, False)):
            vec = jnp.dot(normed[lax.rem(stage, 2), :, pl.ds(0, d_model)], weight[layer], preferred_element_type=F32)
            for h in range(2):
                piece = vec[:, h * 128:(h + 1) * 128]
                if rotate:
                    swapped = jnp.where(even, pltpu.roll(piece, 127, 1), pltpu.roll(piece, 1, 1))
                    piece = piece * cos + swapped * sin
                dst[h] = piece

    def attend(stage, layer, chunk):
        slot = lax.rem(stage, 2)
        for copy in kv_copies(stage):
            copy.wait()

        @pl.when(chunk == 0)
        def _():
            for j in range(3, 6):
                weight_copy(layer, j).wait()

        shape = (2 * steps, 2 * (OLD + steps))
        row, col = lax.broadcasted_iota(jnp.int32, shape, 0), lax.broadcasted_iota(jnp.int32, shape, 1)
        col_slot, col_head = lax.shift_right_logical(col, 1), lax.bitwise_and(col, 1)
        row_head, row_step = lax.div(row, steps), lax.rem(row, steps)
        never = 1 << 20
        fresh = jnp.where(col_slot - OLD <= row_step, -1, never)
        key_scr[...] = jnp.where(row_head == col_head, jnp.where(col_slot >= OLD, fresh, col_slot), never)
        limit = lens[pl.ds(pl.multiple_of(chunk * SEQS, SEQS), SEQS), :]
        for b in range(SEQS):
            mine = pl.ds(b, steps, stride=SEQS)
            for src, buf, j in ((kf, kbuf, 0), (vf, vbuf, 1)):
                for h in range(2):
                    inter[b, j, pl.ds(h, steps, stride=2), :] = src[h, mine, :]
                buf[slot, b, pl.ds(2 * OLD, 2 * steps), :] = inter[b, j].astype(BF16)
        for b in range(SEQS):
            mine = pl.ds(b, steps, stride=SEQS)
            query = jnp.concatenate([qf[0, mine, :], qf[1, mine, :]], axis=0).astype(BF16)
            s = lax.dot_general(query, kbuf[slot, b], (((1,), (1,)), ((), ())), preferred_element_type=F32) * (128 ** -0.5)
            scores[b] = jnp.where(key_scr[...] < limit[b:b + 1, :], s, -jnp.inf)
        for b in range(SEQS):
            s = scores[b]
            e = jnp.exp(s - jnp.max(s, axis=-1, keepdims=True))
            probs = (e * (1.0 / jnp.sum(e, axis=-1, keepdims=True))).astype(BF16)
            context = jnp.dot(probs, vbuf[slot, b], preferred_element_type=F32)
            for h in range(2):
                cf[h, pl.ds(b, steps, stride=SEQS), :] = context[h * steps:(h + 1) * steps]

        for copy in rec_copies(stage):
            copy.start()

    def feed_forward(stage, layer):
        slot = lax.rem(stage, 2)
        for n in range(ff // 256):
            cols = pl.ds(n * 256, 256)
            pre = jnp.dot(normed[slot, :, pl.ds(0, d_model)], win[layer, :, cols], preferred_element_type=F32) + b_in[layer, :, cols]
            act[:, cols] = jax.nn.gelu(pre, approximate=True).astype(BF16)

    def project_out(stage, layer):
        for h in range(2):
            ctx[:, h * 128:(h + 1) * 128] = cf[h].astype(BF16)

        following = jnp.minimum(stage + 1, n_stages - 1)
        group = steps // (d_model // 256)

        @pl.when(stage + 1 < n_chunks)
        def _():
            x_copy(stage + 1).wait()

        for n in range(d_model // 256):
            cols = pl.ds(n * 256, 256)
            total = jnp.dot(ctx[...], wo[layer, :, cols], preferred_element_type=F32)
            total += jnp.dot(act[:, pl.ds(0, ff)], wout[layer, :, cols], preferred_element_type=F32)
            part[:, :, cols] = total.reshape(steps, SEQS, 256).astype(BF16)
            norm_rows(following, n * group, group)

    x_copy(0).wait()

    @pl.loop(0, steps // 8)
    def _(g):
        norm_rows(0, g * 8, 8)

    pl.semaphore_wait(barrier, 3)

    def between(i, lag):
        return jnp.logical_and(i >= lag, i < n_stages + lag)

    @pl.loop(0, n_stages + 5)
    def _(i):
        layer, chunk = lax.div(i, n_chunks), lax.rem(i, n_chunks)
        live = i < n_stages

        @pl.when(i == 1)
        def _():
            for c in range(2, n_chunks):
                x_copy(c).start()
            for j in range(6):
                weight_copy(1, j).start()

        @pl.when(live)
        def _():
            project_in(i, layer, chunk)

        @pl.when(between(i, 2))
        def _():
            s = i - 2
            for j in range(2):
                phase1(s, j).wait()
                mine = pl.ds(quarter * j + eighth * pos1[j], eighth)
                ts = pl.ds(eighth * j, eighth)
                sum1[lax.rem(s, 2), ts] = sum0[lax.rem(s, 2), mine] + recv1[lax.rem(s, 4), ts]
                phase2(s, j).start()

        @pl.when(between(i, 5))
        def _():
            s = i - 5
            phase5(s).wait()

            @pl.when(s >= n_stages - n_chunks)
            def _():
                out_copy(lax.rem(s, n_chunks)).start()

        @pl.when(live)
        def _():
            @pl.when(i >= 1)
            def _():
                for copy in rec_copies(i - 1):
                    copy.wait()

            @pl.when(i + 1 < n_stages)
            def _():
                for copy in kv_copies(i + 1):
                    copy.start()

            attend(i, layer, chunk)

        @pl.when(between(i, 1))
        def _():
            s = i - 1
            phase0(s).wait()
            for j in range(2):
                @pl.loop(0, quarter // 4)
                def _(g):
                    ts = pl.ds(quarter * j + g * 4, 4)
                    sum0[lax.rem(s, 2), ts] = part[pl.ds(base + quarter * j + g * 4, 4)] + recv0[lax.rem(s, 2), ts]

                phase1(s, j).start()

        @pl.when(live)
        def _():
            feed_forward(i, layer)

        @pl.when(between(i, 3))
        def _():
            for j in range(2):
                phase3(i - 3, j).wait()
                phase4(i - 3, j).start()

        @pl.when(between(i, 4))
        def _():
            for j in range(2):
                phase4(i - 4, j).wait()
            phase5(i - 4).start()

        @pl.when(live)
        def _():
            project_out(i, layer)
            phase0(i).start()

        @pl.when(between(i, 2))
        def _():
            s = i - 2
            where = lax.rem(s, n_chunks)
            for j in range(2):
                phase2(s, j).wait()
                own = pl.ds(base2[j], last)
                total = sum1[lax.rem(s, 2), pl.ds(eighth * j + last * pos2[j], last)].astype(F32) + recv2[lax.rem(s, 4), pl.ds(last * j, last)].astype(F32)
                total = total + hid[where, own].astype(F32) + b_out[lax.div(s, n_chunks)][None]
                hid[where, own] = total.astype(BF16)
                phase3(s, j).start()

    for copy in rec_copies(n_stages - 1):
        copy.wait()
    for chunk in range(n_chunks):
        out_copy(chunk).wait()


def merge_kernel(n_blocks, lens, hid_in, k_hbm, v_hbm, rec_k, rec_v, hid_out, k_out, v_out, hbuf, kbuf, vbuf, rk, rv, in_sem, out_sem):
    size = kbuf.shape[0] // n_blocks
    steps = rk.shape[1]

    def block(ref, i):
        rows = ref.shape[0] // n_blocks
        return ref.at[pl.ds(i * rows, rows)]

    def loads(i):
        pairs = ((k_hbm, kbuf), (v_hbm, vbuf), (rec_k, rk), (rec_v, rv), (hid_in, hbuf))
        return [pltpu.make_async_copy(block(src, i), block(dst, i), in_sem.at[j, i]) for j, (src, dst) in enumerate(pairs)]

    def stores(i):
        pairs = ((kbuf, k_out), (vbuf, v_out), (hbuf, hid_out))
        return [pltpu.make_async_copy(block(src, i), block(dst, i), out_sem.at[j, i]) for j, (src, dst) in enumerate(pairs)]

    ahead = 4
    for i in range(ahead):
        for copy in loads(i):
            copy.start()

    @pl.loop(0, n_blocks)
    def _(i):
        @pl.when(i + ahead < n_blocks)
        def _():
            for copy in loads(i + ahead):
                copy.start()

        for copy in loads(i):
            copy.wait()
        for b in range(size):
            row = i * size + b
            at = lens[lax.rem(row, lens.shape[0])]
            kbuf[row, pl.ds(at, steps)] = rk[row]
            vbuf[row, pl.ds(at, steps)] = rv[row]
        for copy in stores(i):
            copy.start()

    for i in range(n_blocks):
        for copy in stores(i):
            copy.wait()


def inverse_frequencies():
    lane = np.arange(128)
    return np.where(lane < ROT_DIM, 1.0 / (10000.0 ** ((lane // 2 * 2) / ROT_DIM)), 0.0)


def decode_shard(x_steps, cur_len, k_cache, v_cache, ln_gain, ln_bias, w_q, w_k, w_v, w_o, w_in, b_in, w_out, b_out):
    n_layers, batch, cache_len, n_heads, head_dim = k_cache.shape
    steps, _, d_model = x_steps.shape
    ff = w_in.shape[2]
    n_chunks = batch // SEQS
    n_stages = n_layers * n_chunks
    rows = steps * SEQS
    flat = (n_layers, batch, cache_len * n_heads, head_dim)
    step_angles = np.arange(steps)[:, None] * inverse_frequencies()[None, :]
    signed = np.where(np.arange(128) % 2 == 0, -1.0, 1.0)
    cos_t, sin_t = (np.repeat(tab.astype(np.float32)[:, None, :], SEQS, axis=1) for tab in (np.cos(step_angles), np.sin(step_angles) * signed))
    inv_freq = inverse_frequencies().astype(np.float32)[None, :]
    any_spec, vmem = pl.BlockSpec(memory_space=pl.ANY), pl.BlockSpec(memory_space=pltpu.VMEM)
    dma = pltpu.SemaphoreType.DMA
    block = (steps, SEQS, d_model)
    hidden, rec_k, rec_v = pl.pallas_call(
        functools.partial(decode_kernel, n_chunks, n_stages),
        out_shape=(jax.ShapeDtypeStruct(x_steps.shape, BF16),
                   jax.ShapeDtypeStruct((n_layers, batch, steps * n_heads, head_dim), BF16),
                   jax.ShapeDtypeStruct((n_layers, batch, steps * n_heads, head_dim), BF16)),
        in_specs=[any_spec] * 9 + [pl.BlockSpec(memory_space=pltpu.SMEM)] + [vmem] * 7,
        out_specs=(any_spec,) * 3,
        scratch_shapes=[
            pltpu.VMEM(w_q.shape, BF16), pltpu.VMEM(w_k.shape, BF16), pltpu.VMEM(w_v.shape, BF16), pltpu.VMEM(w_o.shape, BF16),
            pltpu.VMEM(w_in.shape, BF16), pltpu.VMEM(w_out.shape, BF16),
            pltpu.VMEM((n_chunks,) + block, BF16), pltpu.VMEM(block, BF16),
            pltpu.VMEM((2, steps // 2, SEQS, d_model), BF16), pltpu.VMEM((2, steps // 2, SEQS, d_model), BF16),
            pltpu.VMEM((4, steps // 4, SEQS, d_model), BF16), pltpu.VMEM((2, steps // 4, SEQS, d_model), BF16),
            pltpu.VMEM((4, steps // 8, SEQS, d_model), BF16),
            pltpu.VMEM((2, rows, d_model + 128), BF16),
            pltpu.VMEM((2, rows, 128), F32), pltpu.VMEM((2, rows, 128), F32), pltpu.VMEM((2, rows, 128), F32), pltpu.VMEM((2, rows, 128), F32),
            pltpu.VMEM((rows, 256), BF16), pltpu.VMEM((rows, ff + 128), BF16),
            pltpu.VMEM((SEQS, 2, 2 * steps, 128), F32), pltpu.VMEM((SEQS, 2 * steps, 256), F32), pltpu.VMEM((2 * steps, 256), jnp.int32),
            pltpu.VMEM((2, SEQS, 256, 128), BF16), pltpu.VMEM((2, SEQS, 256, 128), BF16),
            pltpu.VMEM((batch, cache_len * n_heads), jnp.int32), pltpu.VMEM((batch, 128), F32), pltpu.VMEM((batch, 128), F32),
            pltpu.VMEM((n_layers, 1, d_model), F32), pltpu.VMEM((n_layers, 1, d_model), F32),
            pltpu.VMEM((n_layers, 1, ff), F32), pltpu.VMEM((n_layers, 1, d_model), F32),
            dma((n_layers, 6)), dma((n_chunks,)), dma((2, 2)), dma((2, 2)), dma((n_chunks,)), dma((10, 2)), dma((10, 4)),
        ],
        compiler_params=pltpu.CompilerParams(collective_id=0, has_side_effects=True, vmem_limit_bytes=60 * 1024 * 1024),
        name="decode",
    )(x_steps, k_cache.reshape(flat), v_cache.reshape(flat), w_q, w_k, w_v, w_o, w_in, w_out,
      cur_len, inv_freq, cos_t, sin_t, ln_gain, ln_bias, b_in, b_out)

    pairs = n_layers * batch
    n_blocks = 16
    lines = (pairs, cache_len, n_heads, head_dim)
    new = (pairs, steps, n_heads, head_dim)
    hidden, k_out, v_out = pl.pallas_call(
        functools.partial(merge_kernel, n_blocks),
        out_shape=(jax.ShapeDtypeStruct(x_steps.shape, BF16),) + (jax.ShapeDtypeStruct(lines, BF16),) * 2,
        in_specs=[pl.BlockSpec(memory_space=pltpu.SMEM)] + [any_spec] * 5,
        out_specs=(any_spec,) * 3,
        scratch_shapes=[pltpu.VMEM(x_steps.shape, BF16), pltpu.VMEM(lines, BF16), pltpu.VMEM(lines, BF16),
                        pltpu.VMEM(new, BF16), pltpu.VMEM(new, BF16), dma((5, n_blocks)), dma((3, n_blocks))],
        compiler_params=pltpu.CompilerParams(vmem_limit_bytes=62 * 1024 * 1024),
        name="merge",
    )(cur_len, hidden, k_cache.reshape(lines), v_cache.reshape(lines), rec_k.reshape(new), rec_v.reshape(new))
    return hidden, k_out.reshape(k_cache.shape), v_out.reshape(v_cache.shape)


def solution(mesh):
    cache_spec = P(None, "dp", None, "tp", None)
    in_specs = (P(None, "dp", None), P("dp"), cache_spec, cache_spec, P(None, None), P(None, None),
                P(None, None, "tp"), P(None, None, "tp"), P(None, None, "tp"), P(None, "tp", None),
                P(None, None, "tp"), P(None, "tp"), P(None, "tp", None), P(None, None))
    out_specs = (P(None, "dp", None), cache_spec, cache_spec)
    return jax.shard_map(decode_shard, mesh=mesh, in_specs=in_specs, out_specs=out_specs, check_vma=False)
```
